32 devices in a mesh: row: 8 (over y, x, core), grp: 4 (over z).
Axes of the slice: x: 2, y: 2, z: 4, core: 2. Of those that a mesh axis runs over, the one named last changes fastest.
Arguments:
- positions: float32 [3, 1024], replicated, may hold values from -0.05 to 9.35, as said below
- detuning: float32 [1024], replicated, may hold values from -1 to 1
- populations: float32 [1024], P('row'), may hold values from 0 to 1
- base: float32 [2, 64, 1024], P(None, 'grp', 'row'), may hold values from -6 to 6
- section: float32 [2, 64, 1024], P(None, 'grp', 'row'), may hold values from -6 to 6
- accum: float32 [2, 64, 1024], P(None, 'grp', 'row'), may hold values from -3 to 3
Outputs:
- next_input: float32 [2, 64, 1024], P(None, 'grp', 'row')
- accum_out: float32 [2, 64, 1024], P(None, 'grp', 'row')
The draws below stay inside these ranges and needn't reach their ends.
Inputs may be any that keep to these rules, and one draw needn't show every extreme that they name: `positions`: emitter n sits near the lattice point 0.3 * (n % 32, (n // 32) % 32, n // 1024), displaced by at most 0.05 in each coordinate.
All inputs are finite; a program needn't handle non-finite values.
Results may differ from the reference program's by a relative error of at most 0.0003.
Values sent between devices are 32-bit elements; how exact they have to be, the bound alone decides.
A program may use at most 64 MiB of HBM per device.

```python
import math
import jax
import jax.numpy as jnp
from jax import lax

S = 64
N = 1024


def draw_positions(key, part):
    index = jnp.arange(N, dtype=jnp.int32)
    lattice = jnp.stack([index % 32, index // 32 % 32, index // 1024]).astype(jnp.float32) * 0.3
    jitter = jax.random.uniform(key, (3, N), jnp.float32, -0.05, 0.05)
    return lattice + jitter


def levels(own_key, extent, shards, low, high):
    def one(dim, shards_of):
        steps = jax.random.uniform(jax.random.fold_in(jax.random.fold_in(own_key, 6), dim), (shards_of,), jnp.float32, low / len(shards), high / len(shards))
        return jnp.repeat(jnp.exp(steps), extent[dim] // shards_of).reshape((-1,) + (1,) * (len(extent) - dim - 1))

    loudness = one(*shards[0])
    for cut in shards[1:]:
        loudness = loudness * one(*cut)
    return loudness


def centred(own_key, shape, spread, bound, cuts=(), held_as=jnp.bfloat16):
    array = jax.random.normal(own_key, shape, jnp.float32) * spread
    if len(cuts) > 0:
        array = levels(own_key, shape, cuts, -0.22, 0.18) * array
    return jnp.clip(array, min=-bound, max=bound).astype(held_as)


def setup_inputs(seed: int = 0) -> dict:
    seeds = jax.random.split(jax.random.key(seed), 7)
    positions = draw_positions(jax.random.fold_in(seeds[6], 71), 0)
    detuning = jnp.clip(jax.random.uniform(seeds[1], (N,), jnp.float32, -1.0, 1.0), -1.0, 1.0)
    populations = jnp.clip(1.0 * jax.random.uniform(seeds[2], (N,), jnp.float32) ** levels(seeds[2], (N,), ((0, 8),), -0.2, 0.2), 0.0, 1.0)
    base = centred(seeds[3], (2, S, N), 1.0, 6.0, ((1, 4), (2, 8)), jnp.float32)
    section = centred(seeds[4], (2, S, N), 1.0, 6.0, ((1, 4), (2, 8)), jnp.float32)
    accum = centred(seeds[5], (2, S, N), 0.5, 3.0, ((1, 4), (2, 8)), jnp.float32)
    return {"positions": positions, "detuning": detuning, "populations": populations, "base": base, "section": section, "accum": accum}


WAVE_NUMBER = 2.0 * math.pi
TIME_STEP = 0.2

def coupling(pos_rows, pos_cols, row_ids, col_ids):
    offsets = pos_rows[:, :, None] - pos_cols[:, None, :]
    dist_sq = lax.optimization_barrier(jnp.sum(offsets * offsets, axis=0))
    on_diag = row_ids[:, None] == col_ids[None, :]
    safe_sq = jnp.where(on_diag, 1.0, dist_sq)
    phase = WAVE_NUMBER * jnp.sqrt(safe_sq)
    inverse = 1.0 / phase
    inverse_sq = inverse * inverse
    aligned = offsets[2] * offsets[2] / safe_sq
    quad_real = 1.0 - inverse_sq - aligned * (1.0 - 3.0 * inverse_sq)
    quad_imag = inverse - 3.0 * aligned * inverse
    cosine = jnp.cos(phase)
    sine = jnp.sin(phase)
    h_real = -0.75 * inverse * (cosine * quad_real - sine * quad_imag)
    h_imag = -0.75 * inverse * (sine * quad_real + cosine * quad_imag)
    return (jnp.where(on_diag, 0.0, h_real), jnp.where(on_diag, 0.0, h_imag))

def cross_rows(slab_part, tile):
    return lax.dot_general(slab_part, tile, (((1,), (1,)), ((), ())), precision=lax.Precision.HIGHEST, preferred_element_type=jnp.float32)

def lead_rows(tile, slab_part):
    return lax.dot_general(tile, slab_part, (((0,), (0,)), ((), ())), precision=lax.Precision.HIGHEST, preferred_element_type=jnp.float32)

def slab_rate(z_real, z_imag, shift, local_slab, full_slab, local_det, slab_pos, slab_det, col_start, col_count):
    slab_ids = lax.iota(jnp.int32, slab_pos.shape[1])
    w_real, w_imag = coupling(slab_pos, slab_pos, slab_ids, slab_ids)
    eye_mask = slab_ids[:, None] == slab_ids[None, :]
    w_real = w_real + jnp.where(eye_mask, slab_det[:, None], 0.0)
    w_imag = w_imag + jnp.where(eye_mask, -0.5, 0.0)
    w_real = lax.dynamic_slice_in_dim(w_real, col_start, col_count, 1)
    w_imag = lax.dynamic_slice_in_dim(w_imag, col_start, col_count, 1)
    v_real = lead_rows(w_real, full_slab[0]) + lead_rows(w_imag, full_slab[1])
    v_imag = lead_rows(w_real, full_slab[1]) - lead_rows(w_imag, full_slab[0])
    y_real = local_slab[0]
    y_imag = local_slab[1]
    z_real = z_real + local_det * y_real + 0.5 * y_imag
    z_imag = z_imag + local_det * y_imag - 0.5 * y_real
    f_real = z_imag + shift * y_imag - v_imag
    f_imag = -z_real - shift * y_real + v_real
    return jnp.stack([f_real, f_imag])

def reference(positions, detuning, populations, base, section, accum):
    block_len = math.gcd(N, 512)
    block_total = N // block_len
    signed_pops = 2.0 * populations - 1.0
    all_ids = lax.iota(jnp.int32, N)

    def one_block(row_start):
        pos_rows = lax.dynamic_slice_in_dim(positions, row_start, block_len, 1)
        row_ids = row_start + lax.iota(jnp.int32, block_len)
        h_real, h_imag = coupling(pos_rows, positions, row_ids, all_ids)
        z_real = cross_rows(section[0], h_real) - cross_rows(section[1], h_imag)
        z_imag = cross_rows(section[0], h_imag) + cross_rows(section[1], h_real)
        shift = jnp.dot(h_real, signed_pops, precision=lax.Precision.HIGHEST)
        return (z_real, z_imag, shift)
    starts = (jnp.arange(block_total) * block_len).astype(jnp.int32)
    z_real, z_imag, shift = lax.map(one_block, starts)
    z_real = jnp.transpose(z_real, (1, 0, 2)).reshape(S, N)
    z_imag = jnp.transpose(z_imag, (1, 0, 2)).reshape(S, N)
    shift = shift.reshape(N)
    rate = slab_rate(z_real, z_imag, shift, section, section, detuning, positions[:, :S], detuning[:S], 0, S)
    return (base + 0.5 * TIME_STEP * rate, accum + TIME_STEP / 3.0 * rate)
```

```python
import functools
import math

import jax
import jax.numpy as jnp
from jax import lax
from jax.experimental import pallas as pl
from jax.experimental.pallas import tpu as pltpu
from jax.sharding import PartitionSpec as P

TIME_STEP = 0.2
PAD = 16
TILE = 128
AMPLITUDE = -0.75

HALF_SIN = (4.442882834149929, -7.308241154546326, 3.606288958225646, -0.8457635961475002, 0.10920575363724722)
HALF_COS = (1.4142134965650124, -6.97885098823893, 5.739461170681154, -1.8835629872981716, 0.31069819180355424)
MESH = pl.DeviceIdType.MESH


def horner(coeffs, t):
    total = coeffs[-1] * t + coeffs[-2]
    for value in coeffs[-3::-1]:
        total = total * t + value
    return total


def coupling(cols, rows, diag):
    dx = cols[0] - rows[0]
    dy = cols[1] - rows[1]
    dz = cols[2] - rows[2]
    dz_sq = dz * dz
    dist_sq = dx * dx + dy * dy + dz_sq
    if diag is not None:
        dist_sq = jnp.where(diag, 1.0, dist_sq)
    inv = lax.rsqrt(dist_sq)
    dist = dist_sq * inv
    frac = dist - jnp.round(dist)
    t = frac * frac
    half_sin = frac * horner(HALF_SIN, t)
    half_cos = horner(HALF_COS, t)
    sine = half_sin * half_cos
    cosine = 1.0 - half_sin * half_sin
    u = inv * (0.5 / math.pi)
    aligned = dz_sq * (inv * inv)
    amp_imag = (u * u) * (1.0 - 3.0 * aligned)
    amp_real = u * ((1.0 - aligned) - amp_imag)
    h_real = amp_real * cosine - amp_imag * sine
    h_imag = amp_real * sine + amp_imag * cosine
    if diag is not None:
        h_real = jnp.where(diag, 0.0, h_real)
        h_imag = jnp.where(diag, 0.0, h_imag)
    return h_real, h_imag


def split(x):
    hi = x.astype(jnp.bfloat16)
    return hi, (x - hi.astype(jnp.float32)).astype(jnp.bfloat16)


def bdot(a, b):
    return jnp.dot(a, b, preferred_element_type=jnp.float32)


def kernel(
    n_row,
    n_grp,
    pos_in,
    det_in,
    pop_in,
    sec_in,
    out_ref,
    pos_ref,
    det_ref,
    stage,
    wide,
    rhs_hi,
    rhs_lo,
    row_buf,
    grp_buf,
    send_sem,
    row_recv,
    grp_recv,
    row_ready,
    grp_ready,
    load_sem,
):
    cols, width = sec_in.shape[1], sec_in.shape[2]
    section_loads = [
        pltpu.make_async_copy(src, dst, load_sem.at[0])
        for src, dst in (
            (sec_in.at[0], stage.at[0:cols]),
            (sec_in.at[1], stage.at[cols : 2 * cols]),
            (pop_in, stage.at[2 * cols : 2 * cols + 1]),
        )
    ]
    pos_load = pltpu.make_async_copy(pos_in, pos_ref, load_sem.at[1])
    det_load = pltpu.make_async_copy(det_in, det_ref, load_sem.at[2])
    for load in (*section_loads, pos_load, det_load):
        load.start()
    me = lax.axis_index("row")
    mine = lax.axis_index("grp")
    slab = cols * n_grp

    barrier = pltpu.get_barrier_semaphore()

    last = n_row - 2
    pair = me // 2
    odd = lax.rem(me, 2)
    partner = me + 1 - 2 * odd
    in_first = me < 2
    in_last = me >= last
    between = jnp.logical_not(in_first | in_last)
    GO, LATE = 0, 1

    def to_row(sem, lo, hi):
        def body(p, carry):
            pl.semaphore_signal(sem, inc=1, device_id={"row": p}, device_id_type=MESH)
            return carry

        lax.fori_loop(lo, hi, body, 0)

    def to_grp(sem, lo, hi):
        def body(p, carry):
            pl.semaphore_signal(sem, inc=1, device_id={"grp": p}, device_id_type=MESH)
            return carry

        lax.fori_loop(lo, hi, body, 0)

    slab_part = stage.at[0 : 2 * cols]

    def send_row(lo, hi):
        def body(p, carry):
            pltpu.make_async_remote_copy(
                stage,
                row_buf.at[me],
                send_sem.at[0],
                row_recv.at[pair],
                device_id={"row": p},
                device_id_type=MESH,
            ).start()
            return carry

        lax.fori_loop(lo, hi, body, 0)

    def send_grp(lo, hi):
        def body(p, carry):
            pltpu.make_async_remote_copy(
                slab_part,
                grp_buf.at[mine],
                send_sem.at[1],
                grp_recv,
                device_id={"grp": p},
                device_id_type=MESH,
            ).start()
            return carry

        lax.fori_loop(lo, hi, body, 0)

    def arrived(part, sem):
        pltpu.make_async_copy(part, part, sem).wait()

    to_grp(barrier, mine + 1, n_grp)

    @pl.when(odd == 1)
    def _():
        pl.semaphore_signal(barrier, inc=1, device_id={"row": partner}, device_id_type=MESH)

    after = jnp.where(in_first, 2, jnp.where(in_last, n_row, last))
    to_row(barrier, after, n_row)

    before = jnp.where(in_first, 0, jnp.where(in_last, last, 2))
    met = before + (1 - odd) + mine

    @pl.when(met > 0)
    def _():
        with jax.named_scope("bar"):
            pl.semaphore_wait(barrier, met)

    to_grp(grp_ready.at[mine], 0, mine)

    @pl.when(between)
    def _():
        to_row(row_ready.at[GO], 0, 2)

    @pl.when(in_last)
    def _():
        to_row(row_ready.at[LATE], 0, last)

    @pl.when(odd == 0)
    def _():
        pl.semaphore_signal(row_ready.at[LATE], inc=1, device_id={"row": partner}, device_id_type=MESH)

    with jax.named_scope("load"):
        arrived(stage, load_sem.at[0])
    send_grp(0, mine)
    send_row(0, before)

    @pl.when(odd == 0)
    def _():
        send_row(partner, partner + 1)

    with jax.named_scope("loadpos"):
        pos_load.wait()
        det_load.wait()

    my_start = pl.multiple_of(me * width, width)
    rows = [pos_ref[d : d + 1, pl.ds(my_start, width)] for d in range(3)]
    tiles = width // TILE

    def spread(tile, slot):
        start = pl.multiple_of(tile * TILE, TILE)
        for d in range(3):
            line = pos_ref[d : d + 1, pl.ds(start, TILE)]
            wide[slot, d] = jnp.transpose(jnp.broadcast_to(line, (TILE, TILE)))

    def fill(tile, slot, diag):
        start = pl.multiple_of(tile * TILE, TILE)
        for part in range(tiles):
            lanes = slice(part * TILE, (part + 1) * TILE)
            h_real, h_imag = coupling(
                [wide[slot, d] for d in range(3)],
                [r[:, lanes] for r in rows],
                None if diag is None else diag[:, lanes],
            )
            for base, h in ((0, h_real), (width, h_imag)):
                hi, lo = split(h)
                at = slice(base + part * TILE, base + (part + 1) * TILE)
                rhs_hi[pl.ds(start, TILE), at] = hi
                rhs_lo[pl.ds(start, TILE), at] = lo

    first = me * tiles
    total = n_row * tiles
    lane_ids = lax.broadcasted_iota(jnp.int32, (TILE, width), 1)
    sub_ids = lax.broadcasted_iota(jnp.int32, (TILE, width), 0)

    def tile_at(j):
        return lax.rem(first + j, total)

    with jax.named_scope("couple"):
        spread(first, 0)
        for j in range(tiles):
            spread(tile_at(j + 1), (j + 1) % 2)
            fill(tile_at(j), j % 2, sub_ids + j * TILE == lane_ids)

        def step(j, carry):
            spread(tile_at(j + 1), lax.rem(j + 1, 2))
            fill(tile_at(j), lax.rem(j, 2), None)
            return carry

        UNROLL = 7 if (total - tiles) % 7 == 0 else 1
        if UNROLL == total - tiles:
            for j in range(tiles, total):
                if j + 1 < total:
                    spread(tile_at(j + 1), (j + 1) % 2)
                fill(tile_at(j), j % 2, None)
        else:
            lax.fori_loop(tiles, total, step, 0)

    def answer_grp(p, carry):
        pl.semaphore_wait(grp_ready.at[p], 1)
        send_grp(p, p + 1)
        return carry

    @pl.when(in_first & (last > 2))
    def _():
        with jax.named_scope("wmid"):
            pl.semaphore_wait(row_ready.at[GO], last - 2)

        @pl.when(odd == 1)
        def _():
            to_row(row_ready.at[GO], 2, last)

        send_row(2, last)

    @pl.when(between)
    def _():
        with jax.named_scope("wgo"):
            pl.semaphore_wait(row_ready.at[GO], 1)
        send_row(2, 2 * pair)
        send_row(2 * pair + 2, last)

    with jax.named_scope("ansgrp1"):
        lax.fori_loop(mine + 1, jnp.minimum(mine + 2, n_grp), answer_grp, 0)
    late = odd + jnp.where(in_last, 0, 2)

    @pl.when(late > 0)
    def _():
        with jax.named_scope("wlate"):
            pl.semaphore_wait(row_ready.at[LATE], late)

    @pl.when(odd == 1)
    def _():
        send_row(partner, partner + 1)

    @pl.when(jnp.logical_not(in_last))
    def _():
        send_row(last, n_row)

    with jax.named_scope("ansgrp2"):
        lax.fori_loop(mine + 2, n_grp, answer_grp, 0)

    col_start = pl.multiple_of(mine * cols, cols)
    eye = lax.broadcasted_iota(jnp.int32, (cols, TILE), 0) + col_start == lax.broadcasted_iota(
        jnp.int32, (cols, TILE), 1
    )
    slab_rows = [pos_ref[d : d + 1, :TILE] for d in range(3)]
    own_cols = [
        jnp.sum(jnp.where(eye, jnp.broadcast_to(r, (cols, TILE)), 0.0), axis=1, keepdims=True) for r in slab_rows
    ]
    w_real, w_imag = coupling(own_cols, slab_rows, eye)
    w_real = AMPLITUDE * w_real + jnp.where(eye, det_ref[:, :TILE], 0.0)
    w_imag = AMPLITUDE * w_imag + jnp.where(eye, -0.5, 0.0)
    l_hi, l_lo = split(jnp.concatenate([w_real, w_imag], axis=0)[:, :slab])

    y_local = stage[0 : 2 * cols]
    row_buf[me] = stage[...]
    grp_buf[mine] = y_local

    def left(slab_and_pop):
        signed = jnp.broadcast_to(2.0 * slab_and_pop[2 * cols :] - 1.0, (PAD, width))
        return split(jnp.concatenate([slab_and_pop[: 2 * cols], signed], axis=0))

    main = jnp.zeros((4 * cols + 2 * PAD, 2 * width), jnp.float32)
    rest = jnp.zeros((2 * cols + PAD, 2 * width), jnp.float32)
    group = 2
    for lead in range(0, n_row, group):
        his, los = [], []
        with jax.named_scope(f"wrow{lead}"):

            @pl.when(pair == lead // 2)
            def _():
                arrived(row_buf.at[0], row_recv.at[lead // 2])

            @pl.when(pair != lead // 2)
            def _():
                arrived(row_buf.at[0:2], row_recv.at[lead // 2])

        for p in range(lead, lead + group):
            hi, lo = left(row_buf[p])
            his.append(hi)
            los.append(lo)
        hi = jnp.concatenate(his, axis=1)
        lo = jnp.concatenate(los, axis=1)
        span = slice(lead * width, (lead + group) * width)
        main = main + bdot(jnp.concatenate([hi, lo], axis=0), rhs_hi[span, :])
        rest = rest + bdot(hi, rhs_lo[span, :])
    half = 2 * cols + PAD
    z = AMPLITUDE * (main[:half] + main[half:] + rest)
    z_real = z[:cols, :width] - z[cols : 2 * cols, width:]
    z_imag = z[:cols, width:] + z[cols : 2 * cols, :width]
    shift = z[2 * cols : 2 * cols + 1, :width]

    with jax.named_scope("wgrp"):
        arrived(grp_buf.at[0 : n_grp - 1], grp_recv)
    blocks = [grp_buf[g] for g in range(n_grp)]
    full = jnp.concatenate(
        [jnp.concatenate([block[:cols], block[cols:]], axis=1) for block in blocks], axis=0
    )
    f_hi, f_lo = split(full)
    v = bdot(l_hi, f_hi) + bdot(l_lo, f_hi) + bdot(l_hi, f_lo)
    v_real = v[:cols, :width] + v[cols:, width:]
    v_imag = v[:cols, width:] - v[cols:, :width]

    y_real, y_imag = y_local[:cols], y_local[cols:]
    total_shift = shift + det_ref[:, pl.ds(my_start, width)]
    z_real = z_real + total_shift * y_real + 0.5 * y_imag
    z_imag = z_imag + total_shift * y_imag - 0.5 * y_real
    out_ref[0] = z_imag - v_imag
    out_ref[1] = v_real - z_real

    with jax.named_scope("drain"):
        arrived(row_buf.at[0 : n_row - 1], send_sem.at[0])
        arrived(grp_buf.at[0 : n_grp - 1], send_sem.at[1])


def local(positions, detuning, populations, base, section, accum):
    n_row, n_grp = lax.axis_size("row"), lax.axis_size("grp")
    cols, width = section.shape[1], section.shape[2]
    total = positions.shape[1]
    block = section.shape
    rate = pl.pallas_call(
        functools.partial(kernel, n_row, n_grp),
        out_shape=pltpu.VMEM(block, jnp.float32),
        in_specs=[pl.BlockSpec(memory_space=pl.ANY)] * 4,
        out_specs=pl.BlockSpec(memory_space=pltpu.VMEM),
        scratch_shapes=[
            pltpu.VMEM((3, total), jnp.float32),
            pltpu.VMEM((1, total), jnp.float32),
            pltpu.VMEM((2 * cols + 1, width), jnp.float32),
            pltpu.VMEM((2, 3, TILE, TILE), jnp.float32),
            pltpu.VMEM((total, 2 * width), jnp.bfloat16),
            pltpu.VMEM((total, 2 * width), jnp.bfloat16),
            pltpu.VMEM((n_row, 2 * cols + 1, width), jnp.float32),
            pltpu.VMEM((n_grp, 2 * cols, width), jnp.float32),
            pltpu.SemaphoreType.DMA((2,)),
            pltpu.SemaphoreType.DMA((n_row // 2,)),
            pltpu.SemaphoreType.DMA(()),
            pltpu.SemaphoreType.REGULAR((2,)),
            pltpu.SemaphoreType.REGULAR((n_grp,)),
            pltpu.SemaphoreType.DMA((3,)),
        ],
        compiler_params=pltpu.CompilerParams(collective_id=0, has_side_effects=True),
    )(positions, detuning.reshape(1, total), populations.reshape(1, width), section)
    return (base + 0.5 * TIME_STEP * rate, accum + TIME_STEP / 3.0 * rate)


def solution(mesh):
    return jax.shard_map(
        local,
        mesh=mesh,
        in_specs=(
            P(),
            P(),
            P("row"),
            P(None, "grp", "row"),
            P(None, "grp", "row"),
            P(None, "grp", "row"),
        ),
        out_specs=(P(None, "grp", "row"), P(None, "grp", "row")),
        check_vma=False,
    )
```

```python
import functools
import math

import jax
import jax.numpy as jnp
from jax import lax
from jax.experimental import pallas as pl
from jax.experimental.pallas import tpu as pltpu
from jax.sharding import PartitionSpec as P

TIME_STEP = 0.2
PAD = 16
TILE = 128
AMPLITUDE = -0.75

HALF_SIN = (4.442882834149929, -7.308241154546326, 3.606288958225646, -0.8457635961475002, 0.10920575363724722)
HALF_COS = (1.4142134965650124, -6.97885098823893, 5.739461170681154, -1.8835629872981716, 0.31069819180355424)
MESH = pl.DeviceIdType.MESH


def horner(coeffs, t):
    total = coeffs[-1] * t + coeffs[-2]
    for value in coeffs[-3::-1]:
        total = total * t + value
    return total


def coupling(cols, rows, diag):
    dx = cols[0] - rows[0]
    dy = cols[1] - rows[1]
    dz = cols[2] - rows[2]
    dz_sq = dz * dz
    dist_sq = dx * dx + dy * dy + dz_sq
    if diag is not None:
        dist_sq = jnp.where(diag, 1.0, dist_sq)
    inv = lax.rsqrt(dist_sq)
    dist = dist_sq * inv
    frac = dist - jnp.round(dist)
    t = frac * frac
    half_sin = frac * horner(HALF_SIN, t)
    half_cos = horner(HALF_COS, t)
    sine = half_sin * half_cos
    cosine = 1.0 - half_sin * half_sin
    u = inv * (0.5 / math.pi)
    aligned = dz_sq * (inv * inv)
    amp_imag = (u * u) * (1.0 - 3.0 * aligned)
    amp_real = u * ((1.0 - aligned) - amp_imag)
    h_real = amp_real * cosine - amp_imag * sine
    h_imag = amp_real * sine + amp_imag * cosine
    if diag is not None:
        h_real = jnp.where(diag, 0.0, h_real)
        h_imag = jnp.where(diag, 0.0, h_imag)
    return h_real, h_imag


def split(x):
    hi = x.astype(jnp.bfloat16)
    return hi, (x - hi.astype(jnp.float32)).astype(jnp.bfloat16)


def bdot(a, b):
    return jnp.dot(a, b, preferred_element_type=jnp.float32)


def kernel(
    n_row,
    n_grp,
    pos_in,
    det_in,
    pop_in,
    sec_in,
    out_ref,
    pos_ref,
    det_ref,
    stage,
    wide,
    rhs_hi,
    rhs_lo,
    row_buf,
    grp_buf,
    send_sem,
    row_recv,
    grp_recv,
    row_ready,
    grp_ready,
    load_sem,
):
    cols, width = sec_in.shape[0] // 2, sec_in.shape[1]
    section_loads = [
        pltpu.make_async_copy(src, dst, load_sem.at[0])
        for src, dst in (
            (sec_in, stage.at[0 : 2 * cols]),
            (pop_in, stage.at[2 * cols : 2 * cols + 1]),
        )
    ]
    pos_load = pltpu.make_async_copy(pos_in, pos_ref, load_sem.at[1])
    det_load = pltpu.make_async_copy(det_in, det_ref, load_sem.at[2])
    for load in (*section_loads, pos_load, det_load):
        load.start()
    me = lax.axis_index("row")
    mine = lax.axis_index("grp")
    slab = cols * n_grp

    barrier = pltpu.get_barrier_semaphore()

    last = n_row - 2
    pair = me // 2
    odd = lax.rem(me, 2)
    partner = me + 1 - 2 * odd
    in_first = me < 2
    in_last = me >= last
    between = jnp.logical_not(in_first | in_last)
    even = odd == 0
    GO, LATE, WORD = 0, 1, 2

    def to_row(sem, lo, hi):
        def body(p, carry):
            pl.semaphore_signal(sem, inc=1, device_id={"row": p}, device_id_type=MESH)
            return carry

        lax.fori_loop(lo, hi, body, 0)

    def to_grp(sem, lo, hi):
        def body(p, carry):
            pl.semaphore_signal(sem, inc=1, device_id={"grp": p}, device_id_type=MESH)
            return carry

        lax.fori_loop(lo, hi, body, 0)

    slab_part = stage.at[0 : 2 * cols]

    def send_row(lo, hi):
        def body(p, carry):
            pltpu.make_async_remote_copy(
                stage,
                row_buf.at[me],
                send_sem.at[0],
                row_recv.at[me // last],
                device_id={"row": p},
                device_id_type=MESH,
            ).start()
            return carry

        lax.fori_loop(lo, hi, body, 0)

    def send_grp(lo, hi, source):
        def body(p, carry):
            pltpu.make_async_remote_copy(
                source,
                grp_buf.at[mine],
                send_sem.at[1],
                grp_recv,
                device_id={"grp": p},
                device_id_type=MESH,
            ).start()
            return carry

        lax.fori_loop(lo, hi, body, 0)

    def arrived(part, sem):
        pltpu.make_async_copy(part, part, sem).wait()

    @pl.when(even & (mine > 0))
    def _():
        def body(p, carry):
            pl.semaphore_signal(barrier, inc=1, device_id={"row": partner, "grp": p}, device_id_type=MESH)
            return carry

        lax.fori_loop(mine + 1, n_grp, body, 0)

    @pl.when(jnp.logical_not(even & (mine > 0)))
    def _():
        to_grp(barrier, mine + 1, n_grp)

    @pl.when(even)
    def _():
        pl.semaphore_signal(barrier, inc=1, device_id={"row": partner}, device_id_type=MESH)

    after = jnp.where(in_first, 2, jnp.where(in_last, n_row, last))
    to_row(barrier, after, n_row)

    before = jnp.where(in_first, 0, jnp.where(in_last, last, 2))
    low = jnp.minimum(mine, 1)
    met = before + jnp.where(even, low, 1 + mine + mine - low)

    @pl.when(met > 0)
    def _():
        with jax.named_scope("bar"):
            pl.semaphore_wait(barrier, met)

    send_grp(0, low, sec_in)
    to_grp(grp_ready.at[mine - low], 0, low)

    @pl.when(between)
    def _():
        to_row(row_ready.at[GO], 0, 2)

    @pl.when(in_last)
    def _():
        to_row(row_ready.at[LATE], 0, last)

    @pl.when(jnp.logical_not(even))
    def _():
        pl.semaphore_signal(row_ready.at[WORD], inc=1, device_id={"row": partner}, device_id_type=MESH)
        to_grp(grp_ready.at[mine - low], low, mine)

    with jax.named_scope("load"):
        arrived(stage, load_sem.at[0])
    send_row(0, before)

    @pl.when(even)
    def _():
        with jax.named_scope("word"):
            pl.semaphore_wait(row_ready.at[WORD], 1)
        to_grp(grp_ready.at[mine - low], low, mine)

    send_grp(low, mine, slab_part)
    send_row(partner, partner + 1)

    with jax.named_scope("loadpos"):
        pos_load.wait()
        det_load.wait()

    my_start = pl.multiple_of(me * width, width)
    rows = [pos_ref[d : d + 1, pl.ds(my_start, width)] for d in range(3)]
    tiles = width // TILE

    def spread(tile, slot):
        start = pl.multiple_of(tile * TILE, TILE)
        for d in range(3):
            line = pos_ref[d : d + 1, pl.ds(start, TILE)]
            wide[slot, d] = jnp.transpose(jnp.broadcast_to(line, (TILE, TILE)))

    def fill(tile, slot, diag):
        start = pl.multiple_of(tile * TILE, TILE)
        for part in range(tiles):
            lanes = slice(part * TILE, (part + 1) * TILE)
            h_real, h_imag = coupling(
                [wide[slot, d] for d in range(3)],
                [r[:, lanes] for r in rows],
                None if diag is None else diag[:, lanes],
            )
            for base, h in ((0, h_real), (width, h_imag)):
                hi, lo = split(h)
                at = slice(base + part * TILE, base + (part + 1) * TILE)
                rhs_hi[pl.ds(start, TILE), at] = hi
                rhs_lo[pl.ds(start, TILE), at] = lo

    first = me * tiles
    total = n_row * tiles
    lane_ids = lax.broadcasted_iota(jnp.int32, (TILE, width), 1)
    sub_ids = lax.broadcasted_iota(jnp.int32, (TILE, width), 0)

    def tile_at(j):
        return lax.rem(first + j, total)

    with jax.named_scope("couple"):
        spread(first, 0)
        for j in range(tiles):
            spread(tile_at(j + 1), (j + 1) % 2)
            fill(tile_at(j), j % 2, sub_ids + j * TILE == lane_ids)

        def step(j, carry):
            spread(tile_at(j + 1), lax.rem(j + 1, 2))
            fill(tile_at(j), lax.rem(j, 2), None)
            return carry

        UNROLL = 7 if (total - tiles) % 7 == 0 else 1
        if UNROLL == total - tiles:
            for j in range(tiles, total):
                if j + 1 < total:
                    spread(tile_at(j + 1), (j + 1) % 2)
                fill(tile_at(j), j % 2, None)
        else:
            lax.fori_loop(tiles, total, step, 0)

    def answer_grp(p, carry):
        pl.semaphore_wait(grp_ready.at[p - 1], 1)
        send_grp(p, p + 1, slab_part)
        return carry

    @pl.when(in_first & (last > 2))
    def _():
        with jax.named_scope("wmid"):
            pl.semaphore_wait(row_ready.at[GO], last - 2)

        @pl.when(odd == 1)
        def _():
            to_row(row_ready.at[GO], 2, last)

        send_row(2, last)

    @pl.when(between)
    def _():
        with jax.named_scope("wgo"):
            pl.semaphore_wait(row_ready.at[GO], 1)
        send_row(2, 2 * pair)
        send_row(2 * pair + 2, last)

    with jax.named_scope("ansgrp1"):
        lax.fori_loop(mine + 1, jnp.minimum(mine + 2, n_grp), answer_grp, 0)

    @pl.when(jnp.logical_not(in_last))
    def _():
        with jax.named_scope("wlate"):
            pl.semaphore_wait(row_ready.at[LATE], 2)
        send_row(last, n_row)

    with jax.named_scope("ansgrp2"):
        lax.fori_loop(mine + 2, n_grp, answer_grp, 0)

    col_start = pl.multiple_of(mine * cols, cols)
    eye = lax.broadcasted_iota(jnp.int32, (cols, TILE), 0) + col_start == lax.broadcasted_iota(
        jnp.int32, (cols, TILE), 1
    )
    slab_rows = [pos_ref[d : d + 1, :TILE] for d in range(3)]
    own_cols = [
        jnp.sum(jnp.where(eye, jnp.broadcast_to(r, (cols, TILE)), 0.0), axis=1, keepdims=True) for r in slab_rows
    ]
    w_real, w_imag = coupling(own_cols, slab_rows, eye)
    w_real = AMPLITUDE * w_real + jnp.where(eye, det_ref[:, :TILE], 0.0)
    w_imag = AMPLITUDE * w_imag + jnp.where(eye, -0.5, 0.0)
    l_hi, l_lo = split(jnp.concatenate([w_real, w_imag], axis=0)[:, :slab])

    y_local = stage[0 : 2 * cols]
    row_buf[me] = stage[...]
    grp_buf[mine] = y_local

    def left(slab_and_pop):
        signed = jnp.broadcast_to(2.0 * slab_and_pop[2 * cols :] - 1.0, (PAD, width))
        return split(jnp.concatenate([slab_and_pop[: 2 * cols], signed], axis=0))

    main = jnp.zeros((4 * cols + 2 * PAD, 2 * width), jnp.float32)
    rest = jnp.zeros((2 * cols + PAD, 2 * width), jnp.float32)
    group = 2
    for lead in range(0, n_row, group):
        his, los = [], []
        for at, count in ((0, last), (last, 2)):
            if lead == at:
                with jax.named_scope(f"wrow{lead}"):

                    @pl.when(in_last == (at == last))
                    def _():
                        arrived(row_buf.at[0 : count - 1], row_recv.at[at // last])

                    @pl.when(in_last != (at == last))
                    def _():
                        arrived(row_buf.at[0:count], row_recv.at[at // last])

        for p in range(lead, lead + group):
            hi, lo = left(row_buf[p])
            his.append(hi)
            los.append(lo)
        hi = jnp.concatenate(his, axis=1)
        lo = jnp.concatenate(los, axis=1)
        span = slice(lead * width, (lead + group) * width)
        main = main + bdot(jnp.concatenate([hi, lo], axis=0), rhs_hi[span, :])
        rest = rest + bdot(hi, rhs_lo[span, :])
    half = 2 * cols + PAD
    z = AMPLITUDE * (main[:half] + main[half:] + rest)
    z_real = z[:cols, :width] - z[cols : 2 * cols, width:]
    z_imag = z[:cols, width:] + z[cols : 2 * cols, :width]
    shift = z[2 * cols : 2 * cols + 1, :width]

    with jax.named_scope("wgrp"):
        arrived(grp_buf.at[0 : n_grp - 1], grp_recv)
    blocks = [grp_buf[g] for g in range(n_grp)]
    full = jnp.concatenate(
        [jnp.concatenate([block[:cols], block[cols:]], axis=1) for block in blocks], axis=0
    )
    f_hi, f_lo = split(full)
    v = bdot(l_hi, f_hi) + bdot(l_lo, f_hi) + bdot(l_hi, f_lo)
    v_real = v[:cols, :width] + v[cols:, width:]
    v_imag = v[:cols, width:] - v[cols:, :width]

    y_real, y_imag = y_local[:cols], y_local[cols:]
    total_shift = shift + det_ref[:, pl.ds(my_start, width)]
    z_real = z_real + total_shift * y_real + 0.5 * y_imag
    z_imag = z_imag + total_shift * y_imag - 0.5 * y_real
    out_ref[0] = z_imag - v_imag
    out_ref[1] = v_real - z_real

    with jax.named_scope("drain"):
        arrived(row_buf.at[0 : n_row - 1], send_sem.at[0])
        arrived(grp_buf.at[0 : n_grp - 1], send_sem.at[1])


def local(positions, detuning, populations, base, section, accum):
    n_row, n_grp = lax.axis_size("row"), lax.axis_size("grp")
    cols, width = section.shape[1], section.shape[2]
    total = positions.shape[1]
    block = section.shape
    rate = pl.pallas_call(
        functools.partial(kernel, n_row, n_grp),
        out_shape=pltpu.VMEM(block, jnp.float32),
        in_specs=[pl.BlockSpec(memory_space=pl.ANY)] * 4,
        out_specs=pl.BlockSpec(memory_space=pltpu.VMEM),
        scratch_shapes=[
            pltpu.VMEM((3, total), jnp.float32),
            pltpu.VMEM((1, total), jnp.float32),
            pltpu.VMEM((2 * cols + 1, width), jnp.float32),
            pltpu.VMEM((2, 3, TILE, TILE), jnp.float32),
            pltpu.VMEM((total, 2 * width), jnp.bfloat16),
            pltpu.VMEM((total, 2 * width), jnp.bfloat16),
            pltpu.VMEM((n_row, 2 * cols + 1, width), jnp.float32),
            pltpu.VMEM((n_grp, 2 * cols, width), jnp.float32),
            pltpu.SemaphoreType.DMA((2,)),
            pltpu.SemaphoreType.DMA((2,)),
            pltpu.SemaphoreType.DMA(()),
            pltpu.SemaphoreType.REGULAR((3,)),
            pltpu.SemaphoreType.REGULAR((n_grp - 1,)),
            pltpu.SemaphoreType.DMA((3,)),
        ],
        compiler_params=pltpu.CompilerParams(collective_id=0, has_side_effects=True),
    )(positions, detuning.reshape(1, total), populations.reshape(1, width), section.reshape(2 * cols, width))
    return (base + 0.5 * TIME_STEP * rate, accum + TIME_STEP / 3.0 * rate)


def solution(mesh):
    return jax.shard_map(
        local,
        mesh=mesh,
        in_specs=(
            P(),
            P(),
            P("row"),
            P(None, "grp", "row"),
            P(None, "grp", "row"),
            P(None, "grp", "row"),
        ),
        out_specs=(P(None, "grp", "row"), P(None, "grp", "row")),
        check_vma=False,
    )
```

```python
import functools
import math

import jax
import jax.numpy as jnp
from jax import lax
from jax.experimental import pallas as pl
from jax.experimental.pallas import tpu as pltpu
from jax.sharding import PartitionSpec as P

TIME_STEP = 0.2
PAD = 16
TILE = 128
AMPLITUDE = -0.75
PAUSE = 1

HALF_SIN = (4.442882834149929, -7.308241154546326, 3.606288958225646, -0.8457635961475002, 0.10920575363724722)
HALF_COS = (1.4142134965650124, -6.97885098823893, 5.739461170681154, -1.8835629872981716, 0.31069819180355424)
MESH = pl.DeviceIdType.MESH


def horner(coeffs, t):
    total = coeffs[-1] * t + coeffs[-2]
    for value in coeffs[-3::-1]:
        total = total * t + value
    return total


def coupling(cols, rows, diag):
    dx = cols[0] - rows[0]
    dy = cols[1] - rows[1]
    dz = cols[2] - rows[2]
    dz_sq = dz * dz
    dist_sq = dx * dx + dy * dy + dz_sq
    if diag is not None:
        dist_sq = jnp.where(diag, 1.0, dist_sq)
    inv = lax.rsqrt(dist_sq)
    dist = dist_sq * inv
    frac = dist - jnp.round(dist)
    t = frac * frac
    half_sin = frac * horner(HALF_SIN, t)
    half_cos = horner(HALF_COS, t)
    sine = half_sin * half_cos
    cosine = 1.0 - half_sin * half_sin
    u = inv * (0.5 / math.pi)
    aligned = dz_sq * (inv * inv)
    amp_imag = (u * u) * (1.0 - 3.0 * aligned)
    amp_real = u * ((1.0 - aligned) - amp_imag)
    h_real = amp_real * cosine - amp_imag * sine
    h_imag = amp_real * sine + amp_imag * cosine
    if diag is not None:
        h_real = jnp.where(diag, 0.0, h_real)
        h_imag = jnp.where(diag, 0.0, h_imag)
    return h_real, h_imag


def split(x):
    hi = x.astype(jnp.bfloat16)
    return hi, (x - hi.astype(jnp.float32)).astype(jnp.bfloat16)


def bdot(a, b):
    return jnp.dot(a, b, preferred_element_type=jnp.float32)


def kernel(
    n_row,
    n_grp,
    pos_in,
    det_in,
    pop_in,
    sec_in,
    out_ref,
    pos_ref,
    det_ref,
    stage,
    wide,
    rhs_hi,
    rhs_lo,
    row_buf,
    grp_buf,
    coef,
    send_sem,
    row_recv,
    grp_recv,
    row_ready,
    grp_ready,
    load_sem,
):
    cols, width = sec_in.shape[0] // 2, sec_in.shape[1]
    me = lax.axis_index("row")
    mine = lax.axis_index("grp")
    slab = cols * n_grp
    barrier = pltpu.get_barrier_semaphore()

    last = n_row - 2
    pair = me // 2
    odd = lax.rem(me, 2)
    partner = me + 1 - 2 * odd
    in_first = me < 2
    in_last = me >= last
    between = jnp.logical_not(in_first | in_last)
    even = odd == 0
    low = jnp.minimum(mine, 1)
    ahead = in_first & even & (mine > 0)
    GO, LATE, WORD = 0, 1, 2
    NEXT, REST = 0, 1

    def to_row(sem, lo, hi):
        def body(p, carry):
            pl.semaphore_signal(sem, inc=1, device_id={"row": p}, device_id_type=MESH)
            return carry

        lax.fori_loop(lo, hi, body, 0)

    def to_grp(sem, lo, hi):
        def body(p, carry):
            pl.semaphore_signal(sem, inc=1, device_id={"grp": p}, device_id_type=MESH)
            return carry

        lax.fori_loop(lo, hi, body, 0)

    slab_part = stage.at[0 : 2 * cols]

    def send_row(lo, hi):
        def body(p, carry):
            pltpu.make_async_remote_copy(
                stage,
                row_buf.at[me],
                send_sem.at[0],
                row_recv.at[me // last],
                device_id={"row": p},
                device_id_type=MESH,
            ).start()
            return carry

        lax.fori_loop(lo, hi, body, 0)

    def send_grp(lo, hi, source):
        def body(p, carry):
            pltpu.make_async_remote_copy(
                source,
                grp_buf.at[mine],
                send_sem.at[1],
                grp_recv.at[mine // (n_grp - 1)],
                device_id={"grp": p},
                device_id_type=MESH,
            ).start()
            return carry

        lax.fori_loop(lo, hi, body, 0)

    def arrived(part, sem):
        pltpu.make_async_copy(part, part, sem).wait()

    @pl.when(ahead)
    def _():
        pl.semaphore_wait(barrier, 1)
        send_grp(0, 1, sec_in)

    section_loads = [
        pltpu.make_async_copy(src, dst, load_sem.at[0])
        for src, dst in (
            (sec_in, stage.at[0 : 2 * cols]),
            (pop_in, stage.at[2 * cols : 2 * cols + 1]),
        )
    ]
    pos_load = pltpu.make_async_copy(pos_in, pos_ref, load_sem.at[1])
    det_load = pltpu.make_async_copy(det_in, det_ref, load_sem.at[2])
    for load in (*section_loads, pos_load, det_load):
        load.start()

    @pl.when(even & (mine > 0))
    def _():
        def body(p, carry):
            pl.semaphore_signal(barrier, inc=1, device_id={"row": partner, "grp": p}, device_id_type=MESH)
            return carry

        lax.fori_loop(mine + 1, n_grp, body, 0)

    @pl.when(jnp.logical_not(even & (mine > 0)))
    def _():
        to_grp(barrier, mine + 1, n_grp)

    @pl.when(even)
    def _():
        pl.semaphore_signal(barrier, inc=1, device_id={"row": partner}, device_id_type=MESH)

    after = jnp.where(in_first, 2, jnp.where(in_last, n_row, last))
    to_row(barrier, after, n_row)

    before = jnp.where(in_first, 0, jnp.where(in_last, last, 2))
    met = before + jnp.where(even, low, 1 + mine + mine - low)

    @pl.when((met > 0) & jnp.logical_not(ahead))
    def _():
        with jax.named_scope("bar"):
            pl.semaphore_wait(barrier, met)

    send_grp(0, jnp.where(even & jnp.logical_not(ahead), low, 0), sec_in)

    def answer_lower(lo, hi):
        to_grp(grp_ready.at[REST], lo, jnp.minimum(hi, mine - 1))
        to_grp(grp_ready.at[NEXT], jnp.maximum(lo, mine - 1), hi)

    answer_lower(0, low)

    @pl.when(between)
    def _():
        to_row(row_ready.at[GO], 0, 2)

    @pl.when(in_last)
    def _():
        to_row(row_ready.at[LATE], 0, last)

    @pl.when(jnp.logical_not(even))
    def _():
        pl.semaphore_signal(row_ready.at[WORD], inc=1, device_id={"row": partner}, device_id_type=MESH)
        answer_lower(low, mine)

    with jax.named_scope("load"):
        arrived(stage, load_sem.at[0])
    send_row(0, before)

    @pl.when(even)
    def _():
        with jax.named_scope("word"):
            pl.semaphore_wait(row_ready.at[WORD], 1)
        answer_lower(low, mine)
        send_grp(low, mine, slab_part)

    send_row(partner, partner + 1)

    with jax.named_scope("loadpos"):
        pos_load.wait()
        det_load.wait()

    my_start = pl.multiple_of(me * width, width)
    rows = [pos_ref[d : d + 1, pl.ds(my_start, width)] for d in range(3)]
    tiles = width // TILE

    def spread(tile, slot):
        start = pl.multiple_of(tile * TILE, TILE)
        for d in range(3):
            line = pos_ref[d : d + 1, pl.ds(start, TILE)]
            wide[slot, d] = jnp.transpose(jnp.broadcast_to(line, (TILE, TILE)))

    def fill(tile, slot, diag):
        start = pl.multiple_of(tile * TILE, TILE)
        for part in range(tiles):
            lanes = slice(part * TILE, (part + 1) * TILE)
            h_real, h_imag = coupling(
                [wide[slot, d] for d in range(3)],
                [r[:, lanes] for r in rows],
                None if diag is None else diag[:, lanes],
            )
            for base, h in ((0, h_real), (width, h_imag)):
                hi, lo = split(h)
                at = slice(base + part * TILE, base + (part + 1) * TILE)
                rhs_hi[pl.ds(start, TILE), at] = hi
                rhs_lo[pl.ds(start, TILE), at] = lo

    first = me * tiles
    total = n_row * tiles
    lane_ids = lax.broadcasted_iota(jnp.int32, (TILE, width), 1)
    sub_ids = lax.broadcasted_iota(jnp.int32, (TILE, width), 0)

    def tile_at(j):
        return lax.rem(first + j, total)

    with jax.named_scope("couple"):
        def lower_from_odd():
            @pl.when(jnp.logical_not(even))
            def _():
                send_grp(0, mine, slab_part)

        def step(j, carry):
            spread(tile_at(j + 1), lax.rem(j + 1, 2))
            fill(tile_at(j), lax.rem(j, 2), None)
            return carry

        flat = total <= 16
        spread(first, 0)
        for j in range(total if flat else tiles):
            if j == tiles + PAUSE:
                lower_from_odd()
            if j + 1 < total:
                spread(tile_at(j + 1), (j + 1) % 2)
            fill(tile_at(j), j % 2, sub_ids + j * TILE == lane_ids if j < tiles else None)
        if not flat:
            lower_from_odd()
            lax.fori_loop(tiles, total, step, 0)

    @pl.when(in_first & (last > 2))
    def _():
        with jax.named_scope("wmid"):
            pl.semaphore_wait(row_ready.at[GO], last - 2)

        @pl.when(odd == 1)
        def _():
            to_row(row_ready.at[GO], 2, last)

        send_row(2, last)

    @pl.when(between)
    def _():
        with jax.named_scope("wgo"):
            pl.semaphore_wait(row_ready.at[GO], 1)
        send_row(2, 2 * pair)
        send_row(2 * pair + 2, last)

    @pl.when(mine < n_grp - 1)
    def _():
        with jax.named_scope("ansnext"):
            pl.semaphore_wait(grp_ready.at[NEXT], 1)
        send_grp(mine + 1, mine + 2, slab_part)

    @pl.when(jnp.logical_not(in_last))
    def _():
        with jax.named_scope("wlate"):
            pl.semaphore_wait(row_ready.at[LATE], 2)
        send_row(last, n_row)

    @pl.when(mine < n_grp - 2)
    def _():
        with jax.named_scope("ansrest"):
            pl.semaphore_wait(grp_ready.at[REST], n_grp - 2 - mine)
        send_grp(mine + 2, n_grp, slab_part)

    col_start = pl.multiple_of(mine * cols, cols)
    eye = lax.broadcasted_iota(jnp.int32, (cols, TILE), 0) + col_start == lax.broadcasted_iota(
        jnp.int32, (cols, TILE), 1
    )
    slab_rows = [pos_ref[d : d + 1, :TILE] for d in range(3)]
    own_cols = [
        jnp.sum(jnp.where(eye, jnp.broadcast_to(r, (cols, TILE)), 0.0), axis=1, keepdims=True) for r in slab_rows
    ]
    w_real, w_imag = coupling(own_cols, slab_rows, eye)
    w_real = AMPLITUDE * w_real + jnp.where(eye, det_ref[:, :TILE], 0.0)
    w_imag = AMPLITUDE * w_imag + jnp.where(eye, -0.5, 0.0)
    most = slab - cols
    l_hi, l_lo = split(jnp.concatenate([w_real, w_imag], axis=0)[:, :most])
    for j in range(cols):
        for lead, w in ((0, w_real), (cols, w_imag)):
            coef[j, lead : lead + cols] = jnp.broadcast_to(w[:, most + j : most + j + 1], (cols, width))

    y_local = stage[0 : 2 * cols]
    row_buf[me] = stage[...]
    grp_buf[mine] = y_local

    def left(slab_and_pop):
        signed = jnp.broadcast_to(2.0 * slab_and_pop[2 * cols :] - 1.0, (PAD, width))
        return split(jnp.concatenate([slab_and_pop[: 2 * cols], signed], axis=0))

    main = jnp.zeros((4 * cols + 2 * PAD, 2 * width), jnp.float32)
    rest = jnp.zeros((2 * cols + PAD, 2 * width), jnp.float32)
    group = 2
    for lead in range(0, n_row, group):
        his, los = [], []
        for at, count in ((0, last), (last, 2)):
            if lead == at:
                with jax.named_scope(f"wrow{lead}"):

                    @pl.when(in_last == (at == last))
                    def _():
                        arrived(row_buf.at[0 : count - 1], row_recv.at[at // last])

                    @pl.when(in_last != (at == last))
                    def _():
                        arrived(row_buf.at[0:count], row_recv.at[at // last])

        for p in range(lead, lead + group):
            hi, lo = left(row_buf[p])
            his.append(hi)
            los.append(lo)
        hi = jnp.concatenate(his, axis=1)
        lo = jnp.concatenate(los, axis=1)
        span = slice(lead * width, (lead + group) * width)
        main = main + bdot(jnp.concatenate([hi, lo], axis=0), rhs_hi[span, :])
        rest = rest + bdot(hi, rhs_lo[span, :])
    half = 2 * cols + PAD
    z = AMPLITUDE * (main[:half] + main[half:] + rest)
    z_real = z[:cols, :width] - z[cols : 2 * cols, width:]
    z_imag = z[:cols, width:] + z[cols : 2 * cols, :width]
    shift = z[2 * cols : 2 * cols + 1, :width]

    y_real, y_imag = y_local[:cols], y_local[cols:]
    total_shift = shift + det_ref[:, pl.ds(my_start, width)]
    z_real = z_real + total_shift * y_real + 0.5 * y_imag
    z_imag = z_imag + total_shift * y_imag - 0.5 * y_real

    top = n_grp - 1
    if n_grp > 2:
        with jax.named_scope("wgrp"):

            @pl.when(mine < top)
            def _():
                arrived(grp_buf.at[0 : top - 1], grp_recv.at[0])

            @pl.when(mine == top)
            def _():
                arrived(grp_buf.at[0:top], grp_recv.at[0])

    elif n_grp == 2:

        @pl.when(mine == top)
        def _():
            arrived(grp_buf.at[0:top], grp_recv.at[0])

    blocks = [grp_buf[g] for g in range(top)]
    full = jnp.concatenate(
        [jnp.concatenate([block[:cols], block[cols:]], axis=1) for block in blocks], axis=0
    )
    f_hi, f_lo = split(full)
    v = bdot(l_hi, f_hi) + bdot(l_lo, f_hi) + bdot(l_hi, f_lo)
    z_imag = z_imag - (v[:cols, width:] - v[cols:, :width])
    z_real = z_real - (v[:cols, :width] + v[cols:, width:])

    with jax.named_scope("wtop"):

        @pl.when(mine < top)
        def _():
            arrived(grp_buf.at[0], grp_recv.at[1])

    sums = [[jnp.zeros((cols, width), jnp.float32)] * 4 for _ in range(2)]
    for j in range(cols):
        fr = grp_buf[top, j : j + 1]
        fi = grp_buf[top, cols + j : cols + j + 1]
        wr, wi = coef[j, :cols], coef[j, cols:]
        k = 2 * (j % 2)
        sums[0][k] = sums[0][k] + wr * fr
        sums[0][k + 1] = sums[0][k + 1] + wi * fi
        sums[1][k] = sums[1][k] + wr * fi
        sums[1][k + 1] = sums[1][k + 1] + wi * fr
    v_real = (sums[0][0] + sums[0][1]) + (sums[0][2] + sums[0][3])
    v_imag = (sums[1][0] + sums[1][2]) - (sums[1][1] + sums[1][3])
    out_ref[0] = z_imag - v_imag
    out_ref[1] = v_real - z_real

    with jax.named_scope("drain"):
        arrived(row_buf.at[0 : n_row - 1], send_sem.at[0])
        arrived(grp_buf.at[0 : n_grp - 1], send_sem.at[1])


def local(positions, detuning, populations, base, section, accum):
    n_row, n_grp = lax.axis_size("row"), lax.axis_size("grp")
    cols, width = section.shape[1], section.shape[2]
    total = positions.shape[1]
    block = section.shape
    rate = pl.pallas_call(
        functools.partial(kernel, n_row, n_grp),
        out_shape=pltpu.VMEM(block, jnp.float32),
        in_specs=[pl.BlockSpec(memory_space=pl.ANY)] * 4,
        out_specs=pl.BlockSpec(memory_space=pltpu.VMEM),
        scratch_shapes=[
            pltpu.VMEM((3, total), jnp.float32),
            pltpu.VMEM((1, total), jnp.float32),
            pltpu.VMEM((2 * cols + 1, width), jnp.float32),
            pltpu.VMEM((2, 3, TILE, TILE), jnp.float32),
            pltpu.VMEM((total, 2 * width), jnp.bfloat16),
            pltpu.VMEM((total, 2 * width), jnp.bfloat16),
            pltpu.VMEM((n_row, 2 * cols + 1, width), jnp.float32),
            pltpu.VMEM((n_grp, 2 * cols, width), jnp.float32),
            pltpu.VMEM((cols, 2 * cols, width), jnp.float32),
            pltpu.SemaphoreType.DMA((2,)),
            pltpu.SemaphoreType.DMA((2,)),
            pltpu.SemaphoreType.DMA((2,)),
            pltpu.SemaphoreType.REGULAR((3,)),
            pltpu.SemaphoreType.REGULAR((2,)),
            pltpu.SemaphoreType.DMA((3,)),
        ],
        compiler_params=pltpu.CompilerParams(collective_id=0, has_side_effects=True),
    )(positions, detuning.reshape(1, total), populations.reshape(1, width), section.reshape(2 * cols, width))
    return (base + 0.5 * TIME_STEP * rate, accum + TIME_STEP / 3.0 * rate)


def solution(mesh):
    return jax.shard_map(
        local,
        mesh=mesh,
        in_specs=(
            P(),
            P(),
            P("row"),
            P(None, "grp", "row"),
            P(None, "grp", "row"),
            P(None, "grp", "row"),
        ),
        out_specs=(P(None, "grp", "row"), P(None, "grp", "row")),
        check_vma=False,
    )
```

```python
import functools
import math

import jax
import jax.numpy as jnp
from jax import lax
from jax.experimental import pallas as pl
from jax.experimental.pallas import tpu as pltpu
from jax.sharding import PartitionSpec as P

TIME_STEP = 0.2
PAD = 16
TILE = 128
AMPLITUDE = -0.75
PAUSE = 1

HALF_SIN = (4.442882834149929, -7.308241154546326, 3.606288958225646, -0.8457635961475002, 0.10920575363724722)
HALF_COS = (1.4142134965650124, -6.97885098823893, 5.739461170681154, -1.8835629872981716, 0.31069819180355424)
MESH = pl.DeviceIdType.MESH


def horner(coeffs, t):
    total = coeffs[-1] * t + coeffs[-2]
    for value in coeffs[-3::-1]:
        total = total * t + value
    return total


def coupling(cols, rows, diag):
    dx = cols[0] - rows[0]
    dy = cols[1] - rows[1]
    dz = cols[2] - rows[2]
    dz_sq = dz * dz
    dist_sq = dx * dx + dy * dy + dz_sq
    if diag is not None:
        dist_sq = jnp.where(diag, 1.0, dist_sq)
    inv = lax.rsqrt(dist_sq)
    dist = dist_sq * inv
    frac = dist - jnp.round(dist)
    t = frac * frac
    half_sin = frac * horner(HALF_SIN, t)
    half_cos = horner(HALF_COS, t)
    sine = half_sin * half_cos
    cosine = 1.0 - half_sin * half_sin
    u = inv * (0.5 / math.pi)
    aligned = dz_sq * (inv * inv)
    amp_imag = (u * u) * (1.0 - 3.0 * aligned)
    amp_real = u * ((1.0 - aligned) - amp_imag)
    h_real = amp_real * cosine - amp_imag * sine
    h_imag = amp_real * sine + amp_imag * cosine
    if diag is not None:
        h_real = jnp.where(diag, 0.0, h_real)
        h_imag = jnp.where(diag, 0.0, h_imag)
    return h_real, h_imag


def split(x):
    hi = x.astype(jnp.bfloat16)
    return hi, (x - hi.astype(jnp.float32)).astype(jnp.bfloat16)


def bdot(a, b):
    return jnp.dot(a, b, preferred_element_type=jnp.float32)


def exchange(
    n_row,
    n_grp,
    pos_in,
    det_in,
    pop_in,
    sec_in,
    base_in,
    accum_in,
    next_ref,
    accum_ref,
    olds,
    pos_ref,
    det_ref,
    stage,
    wide,
    rhs_hi,
    rhs_lo,
    row_buf,
    grp_buf,
    coef,
    send_sem,
    row_recv,
    grp_recv,
    row_ready,
    grp_ready,
    load_sem,
):
    cols, width = sec_in.shape[0] // 2, sec_in.shape[1]
    me = lax.axis_index("row")
    mine = lax.axis_index("grp")
    slab = cols * n_grp
    barrier = pltpu.get_barrier_semaphore()

    last = n_row - 2
    pair = me // 2
    odd = lax.rem(me, 2)
    partner = me + 1 - 2 * odd
    in_first = me < 2
    in_last = me >= last
    between = jnp.logical_not(in_first | in_last)
    even = odd == 0
    low = jnp.minimum(mine, 1)
    ahead = in_first & even & (mine > 0)
    GO, LATE, WORD = 0, 1, 2
    NEXT, REST = 0, 1

    def to_row(sem, lo, hi):
        def body(p, carry):
            pl.semaphore_signal(sem, inc=1, device_id={"row": p}, device_id_type=MESH)
            return carry

        lax.fori_loop(lo, hi, body, 0)

    def to_grp(sem, lo, hi):
        def body(p, carry):
            pl.semaphore_signal(sem, inc=1, device_id={"grp": p}, device_id_type=MESH)
            return carry

        lax.fori_loop(lo, hi, body, 0)

    slab_part = stage.at[0 : 2 * cols]

    def send_row(lo, hi):
        def body(p, carry):
            pltpu.make_async_remote_copy(
                stage,
                row_buf.at[me],
                send_sem.at[0],
                row_recv.at[me // last],
                device_id={"row": p},
                device_id_type=MESH,
            ).start()
            return carry

        lax.fori_loop(lo, hi, body, 0)

    def send_grp(lo, hi, source):
        def body(p, carry):
            pltpu.make_async_remote_copy(
                source,
                grp_buf.at[mine],
                send_sem.at[1],
                grp_recv.at[mine // (n_grp - 1)],
                device_id={"grp": p},
                device_id_type=MESH,
            ).start()
            return carry

        lax.fori_loop(lo, hi, body, 0)

    def arrived(part, sem):
        pltpu.make_async_copy(part, part, sem).wait()

    @pl.when(ahead)
    def _():
        pl.semaphore_wait(barrier, 1)
        send_grp(0, 1, sec_in)

    section_loads = [
        pltpu.make_async_copy(src, dst, load_sem.at[0])
        for src, dst in (
            (sec_in, stage.at[0 : 2 * cols]),
            (pop_in, stage.at[2 * cols : 2 * cols + 1]),
        )
    ]
    pos_load = pltpu.make_async_copy(pos_in, pos_ref, load_sem.at[1])
    det_load = pltpu.make_async_copy(det_in, det_ref, load_sem.at[2])
    old_loads = [
        pltpu.make_async_copy(src, olds.at[i], load_sem.at[3]) for i, src in enumerate((base_in, accum_in))
    ]
    for load in (*section_loads, pos_load, det_load, *old_loads):
        load.start()

    @pl.when(even & (mine > 0))
    def _():
        def body(p, carry):
            pl.semaphore_signal(barrier, inc=1, device_id={"row": partner, "grp": p}, device_id_type=MESH)
            return carry

        lax.fori_loop(mine + 1, n_grp, body, 0)

    @pl.when(jnp.logical_not(even & (mine > 0)))
    def _():
        to_grp(barrier, mine + 1, n_grp)

    @pl.when(even)
    def _():
        pl.semaphore_signal(barrier, inc=1, device_id={"row": partner}, device_id_type=MESH)

    after = jnp.where(in_first, 2, jnp.where(in_last, n_row, last))
    to_row(barrier, after, n_row)

    before = jnp.where(in_first, 0, jnp.where(in_last, last, 2))
    met = before + jnp.where(even, low, 1 + mine + mine - low)

    @pl.when((met > 0) & jnp.logical_not(ahead))
    def _():
        with jax.named_scope("bar"):
            pl.semaphore_wait(barrier, met)

    send_grp(0, jnp.where(even & jnp.logical_not(ahead), low, 0), sec_in)

    def answer_lower(lo, hi):
        to_grp(grp_ready.at[REST], lo, jnp.minimum(hi, mine - 1))
        to_grp(grp_ready.at[NEXT], jnp.maximum(lo, mine - 1), hi)

    answer_lower(0, low)

    @pl.when(between)
    def _():
        to_row(row_ready.at[GO], 0, 2)

    @pl.when(in_last)
    def _():
        to_row(row_ready.at[LATE], 0, last)

    @pl.when(jnp.logical_not(even))
    def _():
        pl.semaphore_signal(row_ready.at[WORD], inc=1, device_id={"row": partner}, device_id_type=MESH)
        answer_lower(low, mine)

    with jax.named_scope("load"):
        arrived(stage, load_sem.at[0])
    send_row(0, before)

    @pl.when(even)
    def _():
        with jax.named_scope("word"):
            pl.semaphore_wait(row_ready.at[WORD], 1)
        answer_lower(low, mine)
        send_grp(low, mine, slab_part)

    send_row(partner, partner + 1)

    with jax.named_scope("loadpos"):
        pos_load.wait()
        det_load.wait()
        arrived(olds, load_sem.at[3])

    my_start = pl.multiple_of(me * width, width)
    rows = [pos_ref[d : d + 1, pl.ds(my_start, width)] for d in range(3)]
    tiles = width // TILE

    def spread(tile, slot):
        start = pl.multiple_of(tile * TILE, TILE)
        for d in range(3):
            line = pos_ref[d : d + 1, pl.ds(start, TILE)]
            wide[slot, d] = jnp.transpose(jnp.broadcast_to(line, (TILE, TILE)))

    def fill(tile, slot, diag):
        start = pl.multiple_of(tile * TILE, TILE)
        for part in range(tiles):
            lanes = slice(part * TILE, (part + 1) * TILE)
            h_real, h_imag = coupling(
                [wide[slot, d] for d in range(3)],
                [r[:, lanes] for r in rows],
                None if diag is None else diag[:, lanes],
            )
            for base, h in ((0, h_real), (width, h_imag)):
                hi, lo = split(h)
                at = slice(base + part * TILE, base + (part + 1) * TILE)
                rhs_hi[pl.ds(start, TILE), at] = hi
                rhs_lo[pl.ds(start, TILE), at] = lo

    first = me * tiles
    total = n_row * tiles
    lane_ids = lax.broadcasted_iota(jnp.int32, (TILE, width), 1)
    sub_ids = lax.broadcasted_iota(jnp.int32, (TILE, width), 0)

    def tile_at(j):
        return lax.rem(first + j, total)

    with jax.named_scope("couple"):
        def lower_from_odd():
            @pl.when(jnp.logical_not(even))
            def _():
                send_grp(0, mine, slab_part)

        def step(j, carry):
            spread(tile_at(j + 1), lax.rem(j + 1, 2))
            fill(tile_at(j), lax.rem(j, 2), None)
            return carry

        flat = total <= 16
        spread(first, 0)
        for j in range(total if flat else tiles):
            if j == tiles + PAUSE:
                lower_from_odd()
            if j + 1 < total:
                spread(tile_at(j + 1), (j + 1) % 2)
            fill(tile_at(j), j % 2, sub_ids + j * TILE == lane_ids if j < tiles else None)
        if not flat:
            lower_from_odd()
            lax.fori_loop(tiles, total, step, 0)

    @pl.when(in_first & (last > 2))
    def _():
        with jax.named_scope("wmid"):
            pl.semaphore_wait(row_ready.at[GO], last - 2)

        @pl.when(odd == 1)
        def _():
            to_row(row_ready.at[GO], 2, last)

        send_row(2, last)

    @pl.when(between)
    def _():
        with jax.named_scope("wgo"):
            pl.semaphore_wait(row_ready.at[GO], 1)
        send_row(2, 2 * pair)
        send_row(2 * pair + 2, last)

    @pl.when(mine < n_grp - 1)
    def _():
        with jax.named_scope("ansnext"):
            pl.semaphore_wait(grp_ready.at[NEXT], 1)
        send_grp(mine + 1, mine + 2, slab_part)

    @pl.when(jnp.logical_not(in_last))
    def _():
        with jax.named_scope("wlate"):
            pl.semaphore_wait(row_ready.at[LATE], 2)
        send_row(last, n_row)

    @pl.when(mine < n_grp - 2)
    def _():
        with jax.named_scope("ansrest"):
            pl.semaphore_wait(grp_ready.at[REST], n_grp - 2 - mine)
        send_grp(mine + 2, n_grp, slab_part)

    col_start = pl.multiple_of(mine * cols, cols)
    eye = lax.broadcasted_iota(jnp.int32, (cols, TILE), 0) + col_start == lax.broadcasted_iota(
        jnp.int32, (cols, TILE), 1
    )
    slab_rows = [pos_ref[d : d + 1, :TILE] for d in range(3)]
    own_cols = [
        jnp.sum(jnp.where(eye, jnp.broadcast_to(r, (cols, TILE)), 0.0), axis=1, keepdims=True) for r in slab_rows
    ]
    w_real, w_imag = coupling(own_cols, slab_rows, eye)
    w_real = AMPLITUDE * w_real + jnp.where(eye, det_ref[:, :TILE], 0.0)
    w_imag = AMPLITUDE * w_imag + jnp.where(eye, -0.5, 0.0)
    most = slab - cols
    l_hi, l_lo = split(jnp.concatenate([w_real, w_imag], axis=0)[:, :most])
    for j in range(cols):
        for lead, w in ((0, w_real), (cols, w_imag)):
            coef[j, lead : lead + cols] = jnp.broadcast_to(w[:, most + j : most + j + 1], (cols, width))

    y_local = stage[0 : 2 * cols]
    row_buf[me] = stage[...]
    grp_buf[mine] = y_local

    def left(slab_and_pop):
        signed = jnp.broadcast_to(2.0 * slab_and_pop[2 * cols :] - 1.0, (PAD, width))
        return split(jnp.concatenate([slab_and_pop[: 2 * cols], signed], axis=0))

    main = jnp.zeros((4 * cols + 2 * PAD, 2 * width), jnp.float32)
    rest = jnp.zeros((2 * cols + PAD, 2 * width), jnp.float32)
    group = 2
    for lead in range(0, n_row, group):
        his, los = [], []
        for at, count in ((0, last), (last, 2)):
            if lead == at:
                with jax.named_scope(f"wrow{lead}"):

                    @pl.when(in_last == (at == last))
                    def _():
                        arrived(row_buf.at[0 : count - 1], row_recv.at[at // last])

                    @pl.when(in_last != (at == last))
                    def _():
                        arrived(row_buf.at[0:count], row_recv.at[at // last])

        for p in range(lead, lead + group):
            hi, lo = left(row_buf[p])
            his.append(hi)
            los.append(lo)
        hi = jnp.concatenate(his, axis=1)
        lo = jnp.concatenate(los, axis=1)
        span = slice(lead * width, (lead + group) * width)
        main = main + bdot(jnp.concatenate([hi, lo], axis=0), rhs_hi[span, :])
        rest = rest + bdot(hi, rhs_lo[span, :])
    half = 2 * cols + PAD
    z = AMPLITUDE * (main[:half] + main[half:] + rest)
    z_real = z[:cols, :width] - z[cols : 2 * cols, width:]
    z_imag = z[:cols, width:] + z[cols : 2 * cols, :width]
    shift = z[2 * cols : 2 * cols + 1, :width]

    y_real, y_imag = y_local[:cols], y_local[cols:]
    total_shift = shift + det_ref[:, pl.ds(my_start, width)]
    z_real = z_real + total_shift * y_real + 0.5 * y_imag
    z_imag = z_imag + total_shift * y_imag - 0.5 * y_real

    top = n_grp - 1
    if n_grp > 2:
        with jax.named_scope("wgrp"):

            @pl.when(mine < top)
            def _():
                arrived(grp_buf.at[0 : top - 1], grp_recv.at[0])

            @pl.when(mine == top)
            def _():
                arrived(grp_buf.at[0:top], grp_recv.at[0])

    elif n_grp == 2:

        @pl.when(mine == top)
        def _():
            arrived(grp_buf.at[0:top], grp_recv.at[0])

    blocks = [grp_buf[g] for g in range(top)]
    full = jnp.concatenate(
        [jnp.concatenate([block[:cols], block[cols:]], axis=1) for block in blocks], axis=0
    )
    f_hi, f_lo = split(full)
    v = bdot(l_hi, f_hi) + bdot(l_lo, f_hi) + bdot(l_hi, f_lo)
    z_imag = z_imag - (v[:cols, width:] - v[cols:, :width])
    z_real = z_real - (v[:cols, :width] + v[cols:, width:])

    for i, rate in enumerate((z_imag, -z_real)):
        next_ref[i] = olds[0, i] + 0.5 * TIME_STEP * rate
        accum_ref[i] = olds[1, i] + TIME_STEP / 3.0 * rate

    with jax.named_scope("drain"):
        arrived(row_buf.at[0 : n_row - 1], send_sem.at[0])
        arrived(grp_buf.at[0 : n_grp - 1], send_sem.at[1])


def finish(n_grp, next_ref, accum_ref, grp_buf, coef, grp_recv):
    cols, width = coef.shape[0], coef.shape[2]
    mine, top = lax.axis_index("grp"), n_grp - 1

    with jax.named_scope("wtop"):

        @pl.when(mine < top)
        def _():
            pltpu.make_async_copy(grp_buf.at[0], grp_buf.at[0], grp_recv.at[1]).wait()

    sums = [[jnp.zeros((cols, width), jnp.float32)] * 4 for _ in range(2)]
    for j in range(cols):
        fr = grp_buf[top, j : j + 1]
        fi = grp_buf[top, cols + j : cols + j + 1]
        wr, wi = coef[j, :cols], coef[j, cols:]
        k = 2 * (j % 2)
        sums[0][k] = sums[0][k] + wr * fr
        sums[0][k + 1] = sums[0][k + 1] + wi * fi
        sums[1][k] = sums[1][k] + wr * fi
        sums[1][k + 1] = sums[1][k + 1] + wi * fr
    v_real = (sums[0][0] + sums[0][1]) + (sums[0][2] + sums[0][3])
    v_imag = (sums[1][0] + sums[1][2]) - (sums[1][1] + sums[1][3])
    for i, rate in enumerate((-v_imag, v_real)):
        next_ref[i] = next_ref[i] + 0.5 * TIME_STEP * rate
        accum_ref[i] = accum_ref[i] + TIME_STEP / 3.0 * rate


def kernel(n_row, n_grp, pos_in, det_in, pop_in, sec_in, base_in, accum_in, next_ref, accum_ref, olds, pos_ref, det_ref, stage, wide, rhs_hi, rhs_lo, row_buf, grp_buf, coef, row_recv, grp_recv, row_ready, grp_ready):
    def scope(load_sem, send_sem):
        exchange(n_row=n_row, n_grp=n_grp, pos_in=pos_in, det_in=det_in, pop_in=pop_in, sec_in=sec_in, base_in=base_in, accum_in=accum_in, next_ref=next_ref, accum_ref=accum_ref, olds=olds, pos_ref=pos_ref, det_ref=det_ref, stage=stage, wide=wide, rhs_hi=rhs_hi, rhs_lo=rhs_lo, row_buf=row_buf, grp_buf=grp_buf, coef=coef, row_recv=row_recv, grp_recv=grp_recv, row_ready=row_ready, grp_ready=grp_ready, load_sem=load_sem, send_sem=send_sem)

    pl.run_scoped(scope, load_sem=pltpu.SemaphoreType.DMA((4,)), send_sem=pltpu.SemaphoreType.DMA((2,)))
    finish(n_grp, next_ref, accum_ref, grp_buf, coef, grp_recv)


def store(next_ref, accum_ref, next_out, accum_out, sem):
    copies = [
        pltpu.make_async_copy(next_ref, next_out, sem.at[0]),
        pltpu.make_async_copy(accum_ref, accum_out, sem.at[1]),
    ]
    for copy in copies:
        copy.start()
    for copy in copies:
        copy.wait()


def local(positions, detuning, populations, base, section, accum):
    n_row, n_grp = lax.axis_size("row"), lax.axis_size("grp")
    cols, width = section.shape[1], section.shape[2]
    total = positions.shape[1]
    block = section.shape
    results = pl.pallas_call(
        functools.partial(kernel, n_row, n_grp),
        out_shape=(pltpu.VMEM(block, jnp.float32), pltpu.VMEM(block, jnp.float32)),
        in_specs=[pl.BlockSpec(memory_space=pl.ANY)] * 6,
        out_specs=(pl.BlockSpec(memory_space=pltpu.VMEM), pl.BlockSpec(memory_space=pltpu.VMEM)),
        scratch_shapes=[
            pltpu.VMEM((2, *block), jnp.float32),
            pltpu.VMEM((3, total), jnp.float32),
            pltpu.VMEM((1, total), jnp.float32),
            pltpu.VMEM((2 * cols + 1, width), jnp.float32),
            pltpu.VMEM((2, 3, TILE, TILE), jnp.float32),
            pltpu.VMEM((total, 2 * width), jnp.bfloat16),
            pltpu.VMEM((total, 2 * width), jnp.bfloat16),
            pltpu.VMEM((n_row, 2 * cols + 1, width), jnp.float32),
            pltpu.VMEM((n_grp, 2 * cols, width), jnp.float32),
            pltpu.VMEM((cols, 2 * cols, width), jnp.float32),
            pltpu.SemaphoreType.DMA((2,)),
            pltpu.SemaphoreType.DMA((2,)),
            pltpu.SemaphoreType.REGULAR((3,)),
            pltpu.SemaphoreType.REGULAR((2,)),
        ],
        compiler_params=pltpu.CompilerParams(collective_id=0, has_side_effects=True),
    )(positions, detuning.reshape(1, total), populations.reshape(1, width), section.reshape(2 * cols, width), base, accum)
    return pl.pallas_call(
        store,
        out_shape=(jax.ShapeDtypeStruct(block, jnp.float32),) * 2,
        in_specs=[pl.BlockSpec(memory_space=pltpu.VMEM)] * 2,
        out_specs=(pl.BlockSpec(memory_space=pltpu.HBM),) * 2,
        scratch_shapes=[pltpu.SemaphoreType.DMA((2,))],
    )(*[pltpu.with_memory_space_constraint(r, pltpu.VMEM) for r in results])


def solution(mesh):
    return jax.shard_map(
        local,
        mesh=mesh,
        in_specs=(
            P(),
            P(),
            P("row"),
            P(None, "grp", "row"),
            P(None, "grp", "row"),
            P(None, "grp", "row"),
        ),
        out_specs=(P(None, "grp", "row"), P(None, "grp", "row")),
        check_vma=False,
    )
```

```python
import functools
import math

import jax
import jax.numpy as jnp
from jax import lax
from jax.experimental import pallas as pl
from jax.experimental.pallas import tpu as pltpu
from jax.sharding import PartitionSpec as P

TIME_STEP = 0.2
PAD = 16
TILE = 128
AMPLITUDE = -0.75
PAUSE = 1

HALF_SIN = (4.442882834149929, -7.308241154546326, 3.606288958225646, -0.8457635961475002, 0.10920575363724722)
HALF_COS = (1.4142134965650124, -6.97885098823893, 5.739461170681154, -1.8835629872981716, 0.31069819180355424)
MESH = pl.DeviceIdType.MESH


def horner(coeffs, t):
    total = coeffs[-1] * t + coeffs[-2]
    for value in coeffs[-3::-1]:
        total = total * t + value
    return total


def coupling(cols, rows, diag):
    dx = cols[0] - rows[0]
    dy = cols[1] - rows[1]
    dz = cols[2] - rows[2]
    dz_sq = dz * dz
    dist_sq = dx * dx + dy * dy + dz_sq
    if diag is not None:
        dist_sq = jnp.where(diag, 1.0, dist_sq)
    inv = lax.rsqrt(dist_sq)
    dist = dist_sq * inv
    frac = dist - jnp.round(dist)
    t = frac * frac
    half_sin = frac * horner(HALF_SIN, t)
    half_cos = horner(HALF_COS, t)
    sine = half_sin * half_cos
    cosine = 1.0 - half_sin * half_sin
    u = inv * (0.5 / math.pi)
    aligned = dz_sq * (inv * inv)
    amp_imag = (u * u) * (1.0 - 3.0 * aligned)
    amp_real = u * ((1.0 - aligned) - amp_imag)
    h_real = amp_real * cosine - amp_imag * sine
    h_imag = amp_real * sine + amp_imag * cosine
    if diag is not None:
        h_real = jnp.where(diag, 0.0, h_real)
        h_imag = jnp.where(diag, 0.0, h_imag)
    return h_real, h_imag


def split(x):
    hi = x.astype(jnp.bfloat16)
    return hi, (x - hi.astype(jnp.float32)).astype(jnp.bfloat16)


def bdot(a, b):
    return jnp.dot(a, b, preferred_element_type=jnp.float32)


def exchange(
    n_row,
    n_grp,
    pos_in,
    det_in,
    pop_in,
    sec_in,
    base_in,
    accum_in,
    next_ref,
    accum_ref,
    olds,
    pos_ref,
    det_ref,
    stage,
    wide,
    rhs_hi,
    rhs_lo,
    row_buf,
    grp_buf,
    coef,
    send_sem,
    row_recv,
    grp_recv,
    row_ready,
    grp_ready,
    load_sem,
):
    cols, width = sec_in.shape[0] // 2, sec_in.shape[1]
    me = lax.axis_index("row")
    mine = lax.axis_index("grp")
    slab = cols * n_grp
    barrier = pltpu.get_barrier_semaphore()

    last = n_row - 2
    pair = me // 2
    odd = lax.rem(me, 2)
    partner = me + 1 - 2 * odd
    in_first = me < 2
    in_last = me >= last
    between = jnp.logical_not(in_first | in_last)
    even = odd == 0
    low = jnp.minimum(mine, 1)
    ahead = in_first & even & (mine > 0)
    GO, LATE, WORD = 0, 1, 2
    NEXT, REST = 0, 1

    def to_row(sem, lo, hi):
        def body(p, carry):
            pl.semaphore_signal(sem, inc=1, device_id={"row": p}, device_id_type=MESH)
            return carry

        lax.fori_loop(lo, hi, body, 0)

    def to_grp(sem, lo, hi):
        def body(p, carry):
            pl.semaphore_signal(sem, inc=1, device_id={"grp": p}, device_id_type=MESH)
            return carry

        lax.fori_loop(lo, hi, body, 0)

    slab_part = stage.at[0 : 2 * cols]

    def send_row(lo, hi):
        def body(p, carry):
            pltpu.make_async_remote_copy(
                stage,
                row_buf.at[me],
                send_sem.at[0],
                row_recv.at[jnp.where(me < last, 0, 1)],
                device_id={"row": p},
                device_id_type=MESH,
            ).start()
            return carry

        lax.fori_loop(lo, hi, body, 0)

    def send_grp(lo, hi, source):
        def body(p, carry):
            pltpu.make_async_remote_copy(
                source,
                grp_buf.at[mine],
                send_sem.at[1],
                grp_recv.at[jnp.where(mine < n_grp - 1, 0, 1)],
                device_id={"grp": p},
                device_id_type=MESH,
            ).start()
            return carry

        lax.fori_loop(lo, hi, body, 0)

    def arrived(part, sem):
        pltpu.make_async_copy(part, part, sem).wait()

    @pl.when(ahead)
    def _():
        pl.semaphore_wait(barrier, 1)
        send_grp(0, 1, sec_in)

    section_loads = [
        pltpu.make_async_copy(src, dst, load_sem.at[0])
        for src, dst in (
            (sec_in, stage.at[0 : 2 * cols]),
            (pop_in, stage.at[2 * cols : 2 * cols + 1]),
        )
    ]
    pos_load = pltpu.make_async_copy(pos_in, pos_ref, load_sem.at[1])
    det_load = pltpu.make_async_copy(det_in, det_ref, load_sem.at[2])
    old_loads = [
        pltpu.make_async_copy(src, olds.at[i], load_sem.at[3]) for i, src in enumerate((base_in, accum_in))
    ]
    for load in (*section_loads, pos_load, det_load, *old_loads):
        load.start()

    @pl.when(even & (mine > 0))
    def _():
        def body(p, carry):
            pl.semaphore_signal(barrier, inc=1, device_id={"row": partner, "grp": p}, device_id_type=MESH)
            return carry

        lax.fori_loop(mine + 1, n_grp, body, 0)

    @pl.when(jnp.logical_not(even & (mine > 0)))
    def _():
        to_grp(barrier, mine + 1, n_grp)

    @pl.when(even)
    def _():
        pl.semaphore_signal(barrier, inc=1, device_id={"row": partner}, device_id_type=MESH)

    after = jnp.where(in_first, 2, jnp.where(in_last, n_row, last))
    to_row(barrier, after, n_row)

    before = jnp.where(in_first, 0, jnp.where(in_last, last, 2))
    met = before + jnp.where(even, low, 1 + mine + mine - low)

    @pl.when((met > 0) & jnp.logical_not(ahead))
    def _():
        with jax.named_scope("bar"):
            pl.semaphore_wait(barrier, met)

    send_grp(0, jnp.where(even & jnp.logical_not(ahead), low, 0), sec_in)

    def answer_lower(lo, hi):
        to_grp(grp_ready.at[REST], lo, jnp.minimum(hi, mine - 1))
        to_grp(grp_ready.at[NEXT], jnp.maximum(lo, mine - 1), hi)

    answer_lower(0, low)

    @pl.when(between)
    def _():
        to_row(row_ready.at[GO], 0, 2)

    @pl.when(in_last)
    def _():
        to_row(row_ready.at[LATE], 0, last)

    @pl.when(jnp.logical_not(even))
    def _():
        pl.semaphore_signal(row_ready.at[WORD], inc=1, device_id={"row": partner}, device_id_type=MESH)
        answer_lower(low, mine)

    with jax.named_scope("load"):
        arrived(stage, load_sem.at[0])
    send_row(0, before)

    @pl.when(even)
    def _():
        with jax.named_scope("word"):
            pl.semaphore_wait(row_ready.at[WORD], 1)
        answer_lower(low, mine)
        send_grp(low, mine, slab_part)

    send_row(partner, partner + 1)

    with jax.named_scope("loadpos"):
        pos_load.wait()

    my_start = pl.multiple_of(me * width, width)
    rows = [pos_ref[d : d + 1, pl.ds(my_start, width)] for d in range(3)]
    tiles = width // TILE

    def spread(tile, slot):
        start = pl.multiple_of(tile * TILE, TILE)
        for d in range(3):
            line = pos_ref[d : d + 1, pl.ds(start, TILE)]
            wide[slot, d] = jnp.transpose(jnp.broadcast_to(line, (TILE, TILE)))

    def fill(tile, slot, diag):
        start = pl.multiple_of(tile * TILE, TILE)
        for part in range(tiles):
            lanes = slice(part * TILE, (part + 1) * TILE)
            h_real, h_imag = coupling(
                [wide[slot, d] for d in range(3)],
                [r[:, lanes] for r in rows],
                None if diag is None else diag[:, lanes],
            )
            for base, h in ((0, h_real), (width, h_imag)):
                hi, lo = split(h)
                at = slice(base + part * TILE, base + (part + 1) * TILE)
                rhs_hi[pl.ds(start, TILE), at] = hi
                rhs_lo[pl.ds(start, TILE), at] = lo

    first = me * tiles
    total = n_row * tiles
    lane_ids = lax.broadcasted_iota(jnp.int32, (TILE, width), 1)
    sub_ids = lax.broadcasted_iota(jnp.int32, (TILE, width), 0)

    def tile_at(j):
        return lax.rem(first + j, total)

    with jax.named_scope("couple"):
        def lower_from_odd():
            @pl.when(jnp.logical_not(even))
            def _():
                send_grp(0, mine, slab_part)

        def step(j, carry):
            spread(tile_at(j + 1), lax.rem(j + 1, 2))
            fill(tile_at(j), lax.rem(j, 2), None)
            return carry

        flat = total <= 16
        spread(first, 0)
        for j in range(total if flat else tiles):
            if j == tiles + PAUSE:
                lower_from_odd()
            if j + 1 < total:
                spread(tile_at(j + 1), (j + 1) % 2)
            fill(tile_at(j), j % 2, sub_ids + j * TILE == lane_ids if j < tiles else None)
        if not flat:
            lower_from_odd()
            lax.fori_loop(tiles, total, step, 0)

    @pl.when(in_first & (last > 2))
    def _():
        with jax.named_scope("wmid"):
            pl.semaphore_wait(row_ready.at[GO], last - 2)

        @pl.when(odd == 1)
        def _():
            to_row(row_ready.at[GO], 2, last)

        send_row(2, last)

    @pl.when(between)
    def _():
        with jax.named_scope("wgo"):
            pl.semaphore_wait(row_ready.at[GO], 1)
        send_row(2, 2 * pair)
        send_row(2 * pair + 2, last)

    @pl.when(mine < n_grp - 1)
    def _():
        with jax.named_scope("ansnext"):
            pl.semaphore_wait(grp_ready.at[NEXT], 1)
        send_grp(mine + 1, mine + 2, slab_part)

    @pl.when(jnp.logical_not(in_last))
    def _():
        with jax.named_scope("wlate"):
            pl.semaphore_wait(row_ready.at[LATE], 2)
        send_row(last, n_row)

    @pl.when(mine < n_grp - 2)
    def _():
        with jax.named_scope("ansrest"):
            pl.semaphore_wait(grp_ready.at[REST], n_grp - 2 - mine)
        send_grp(mine + 2, n_grp, slab_part)

    det_load.wait()
    arrived(olds, load_sem.at[3])

    col_start = pl.multiple_of(mine * cols, cols)
    eye = lax.broadcasted_iota(jnp.int32, (cols, TILE), 0) + col_start == lax.broadcasted_iota(
        jnp.int32, (cols, TILE), 1
    )
    slab_rows = [pos_ref[d : d + 1, :TILE] for d in range(3)]
    own_cols = [
        jnp.sum(jnp.where(eye, jnp.broadcast_to(r, (cols, TILE)), 0.0), axis=1, keepdims=True) for r in slab_rows
    ]
    w_real, w_imag = coupling(own_cols, slab_rows, eye)
    w_real = AMPLITUDE * w_real + jnp.where(eye, det_ref[:, :TILE], 0.0)
    w_imag = AMPLITUDE * w_imag + jnp.where(eye, -0.5, 0.0)
    most = slab - cols
    l_hi, l_lo = split(jnp.concatenate([w_real, w_imag], axis=0)[:, :most])
    for j in range(cols):
        for lead, w in ((0, w_real), (cols, w_imag)):
            coef[j, lead : lead + cols] = jnp.broadcast_to(w[:, most + j : most + j + 1], (cols, width))

    y_local = stage[0 : 2 * cols]
    row_buf[me] = stage[...]
    grp_buf[mine] = y_local

    def left(slab_and_pop):
        signed = jnp.broadcast_to(2.0 * slab_and_pop[2 * cols :] - 1.0, (PAD, width))
        return split(jnp.concatenate([slab_and_pop[: 2 * cols], signed], axis=0))

    main = jnp.zeros((4 * cols + 2 * PAD, 2 * width), jnp.float32)
    rest = jnp.zeros((2 * cols + PAD, 2 * width), jnp.float32)
    group = 2
    for lead in range(0, n_row, group):
        his, los = [], []
        for at, count in ((0, last), (last, 2)):
            if lead == at:
                with jax.named_scope(f"wrow{lead}"):

                    @pl.when(in_last == (at == last))
                    def _():
                        arrived(row_buf.at[0 : count - 1], row_recv.at[at // last])

                    @pl.when(in_last != (at == last))
                    def _():
                        arrived(row_buf.at[0:count], row_recv.at[at // last])

        for p in range(lead, lead + group):
            hi, lo = left(row_buf[p])
            his.append(hi)
            los.append(lo)
        hi = jnp.concatenate(his, axis=1)
        lo = jnp.concatenate(los, axis=1)
        span = slice(lead * width, (lead + group) * width)
        main = main + bdot(jnp.concatenate([hi, lo], axis=0), rhs_hi[span, :])
        rest = rest + bdot(hi, rhs_lo[span, :])
    half = 2 * cols + PAD
    z = AMPLITUDE * (main[:half] + main[half:] + rest)
    z_real = z[:cols, :width] - z[cols : 2 * cols, width:]
    z_imag = z[:cols, width:] + z[cols : 2 * cols, :width]
    shift = z[2 * cols : 2 * cols + 1, :width]

    y_real, y_imag = y_local[:cols], y_local[cols:]
    total_shift = shift + det_ref[:, pl.ds(my_start, width)]
    z_real = z_real + total_shift * y_real + 0.5 * y_imag
    z_imag = z_imag + total_shift * y_imag - 0.5 * y_real

    top = n_grp - 1
    if n_grp > 2:
        with jax.named_scope("wgrp"):

            @pl.when(mine < top)
            def _():
                arrived(grp_buf.at[0 : top - 1], grp_recv.at[0])

            @pl.when(mine == top)
            def _():
                arrived(grp_buf.at[0:top], grp_recv.at[0])

    elif n_grp == 2:

        @pl.when(mine == top)
        def _():
            arrived(grp_buf.at[0:top], grp_recv.at[0])

    blocks = [grp_buf[g] for g in range(top)]
    full = jnp.concatenate(
        [jnp.concatenate([block[:cols], block[cols:]], axis=1) for block in blocks], axis=0
    )
    f_hi, f_lo = split(full)
    v = bdot(l_hi, f_hi) + bdot(l_lo, f_hi) + bdot(l_hi, f_lo)
    z_imag = z_imag - (v[:cols, width:] - v[cols:, :width])
    z_real = z_real - (v[:cols, :width] + v[cols:, width:])

    for i, rate in enumerate((z_imag, -z_real)):
        next_ref[i] = olds[0, i] + 0.5 * TIME_STEP * rate
        accum_ref[i] = olds[1, i] + TIME_STEP / 3.0 * rate

    with jax.named_scope("drain"):
        arrived(row_buf.at[0 : n_row - 1], send_sem.at[0])
        arrived(grp_buf.at[0 : n_grp - 1], send_sem.at[1])


def finish(n_grp, next_ref, accum_ref, grp_buf, coef, grp_recv):
    cols, width = coef.shape[0], coef.shape[2]
    mine, top = lax.axis_index("grp"), n_grp - 1

    with jax.named_scope("wtop"):

        @pl.when(mine < top)
        def _():
            pltpu.make_async_copy(grp_buf.at[0], grp_buf.at[0], grp_recv.at[1]).wait()

    sums = [[jnp.zeros((cols, width), jnp.float32)] * 4 for _ in range(2)]
    for j in range(cols):
        fr = grp_buf[top, j : j + 1]
        fi = grp_buf[top, cols + j : cols + j + 1]
        wr, wi = coef[j, :cols], coef[j, cols:]
        k = 2 * (j % 2)
        sums[0][k] = sums[0][k] + wr * fr
        sums[0][k + 1] = sums[0][k + 1] + wi * fi
        sums[1][k] = sums[1][k] + wr * fi
        sums[1][k + 1] = sums[1][k + 1] + wi * fr
    v_real = (sums[0][0] + sums[0][1]) + (sums[0][2] + sums[0][3])
    v_imag = (sums[1][0] + sums[1][2]) - (sums[1][1] + sums[1][3])
    for i, rate in enumerate((-v_imag, v_real)):
        next_ref[i] = next_ref[i] + 0.5 * TIME_STEP * rate
        accum_ref[i] = accum_ref[i] + TIME_STEP / 3.0 * rate


def kernel(n_row, n_grp, pos_in, det_in, pop_in, sec_in, base_in, accum_in, next_ref, accum_ref, olds, pos_ref, det_ref, stage, wide, rhs_hi, rhs_lo, row_buf, grp_buf, coef, row_recv, grp_recv, row_ready, grp_ready):
    def scope(load_sem, send_sem):
        exchange(n_row=n_row, n_grp=n_grp, pos_in=pos_in, det_in=det_in, pop_in=pop_in, sec_in=sec_in, base_in=base_in, accum_in=accum_in, next_ref=next_ref, accum_ref=accum_ref, olds=olds, pos_ref=pos_ref, det_ref=det_ref, stage=stage, wide=wide, rhs_hi=rhs_hi, rhs_lo=rhs_lo, row_buf=row_buf, grp_buf=grp_buf, coef=coef, row_recv=row_recv, grp_recv=grp_recv, row_ready=row_ready, grp_ready=grp_ready, load_sem=load_sem, send_sem=send_sem)

    pl.run_scoped(scope, load_sem=pltpu.SemaphoreType.DMA((4,)), send_sem=pltpu.SemaphoreType.DMA((2,)))
    finish(n_grp, next_ref, accum_ref, grp_buf, coef, grp_recv)


def store(next_ref, accum_ref, next_out, accum_out):
    def scope(sem):
        copies = [
            pltpu.make_async_copy(next_ref, next_out, sem.at[0]),
            pltpu.make_async_copy(accum_ref, accum_out, sem.at[1]),
        ]
        for copy in copies:
            copy.start()
        for copy in copies:
            copy.wait()

    pl.run_scoped(scope, pltpu.SemaphoreType.DMA((2,)))


def local(positions, detuning, populations, base, section, accum):
    n_row, n_grp = lax.axis_size("row"), lax.axis_size("grp")
    cols, width = section.shape[1], section.shape[2]
    total = positions.shape[1]
    block = section.shape
    results = pl.pallas_call(
        functools.partial(kernel, n_row, n_grp),
        out_shape=(pltpu.VMEM(block, jnp.float32), pltpu.VMEM(block, jnp.float32)),
        in_specs=[pl.BlockSpec(memory_space=pl.ANY)] * 6,
        out_specs=(pl.BlockSpec(memory_space=pltpu.VMEM), pl.BlockSpec(memory_space=pltpu.VMEM)),
        scratch_shapes=[
            pltpu.VMEM((2, *block), jnp.float32),
            pltpu.VMEM((3, total), jnp.float32),
            pltpu.VMEM((1, total), jnp.float32),
            pltpu.VMEM((2 * cols + 1, width), jnp.float32),
            pltpu.VMEM((2, 3, TILE, TILE), jnp.float32),
            pltpu.VMEM((total, 2 * width), jnp.bfloat16),
            pltpu.VMEM((total, 2 * width), jnp.bfloat16),
            pltpu.VMEM((n_row, 2 * cols + 1, width), jnp.float32),
            pltpu.VMEM((n_grp, 2 * cols, width), jnp.float32),
            pltpu.VMEM((cols, 2 * cols, width), jnp.float32),
            pltpu.SemaphoreType.DMA((2,)),
            pltpu.SemaphoreType.DMA((2,)),
            pltpu.SemaphoreType.REGULAR((3,)),
            pltpu.SemaphoreType.REGULAR((2,)),
        ],
        compiler_params=pltpu.CompilerParams(collective_id=0, has_side_effects=True),
    )(positions, detuning.reshape(1, total), populations.reshape(1, width), section.reshape(2 * cols, width), base, accum)
    return pl.pallas_call(
        store,
        out_shape=(jax.ShapeDtypeStruct(block, jnp.float32),) * 2,
        in_specs=[pl.BlockSpec(memory_space=pltpu.VMEM)] * 2,
        out_specs=(pl.BlockSpec(memory_space=pltpu.HBM),) * 2,
    )(*[pltpu.with_memory_space_constraint(r, pltpu.VMEM) for r in results])


def solution(mesh):
    return jax.shard_map(
        local,
        mesh=mesh,
        in_specs=(
            P(),
            P(),
            P("row"),
            P(None, "grp", "row"),
            P(None, "grp", "row"),
            P(None, "grp", "row"),
        ),
        out_specs=(P(None, "grp", "row"), P(None, "grp", "row")),
        check_vma=False,
    )
```

```python
import functools
import math

import jax
import jax.numpy as jnp
from jax import lax
from jax.experimental import pallas as pl
from jax.experimental.pallas import tpu as pltpu
from jax.sharding import PartitionSpec as P

TIME_STEP = 0.2
PAD = 16
TILE = 128
AMPLITUDE = -0.75
PAUSE = 1

HALF_SIN = (4.442882834149929, -7.308241154546326, 3.606288958225646, -0.8457635961475002, 0.10920575363724722)
HALF_COS = (1.4142134965650124, -6.97885098823893, 5.739461170681154, -1.8835629872981716, 0.31069819180355424)
MESH = pl.DeviceIdType.MESH


def horner(coeffs, t):
    total = coeffs[-1] * t + coeffs[-2]
    for value in coeffs[-3::-1]:
        total = total * t + value
    return total


def coupling(cols, rows, diag):
    dx = cols[0] - rows[0]
    dy = cols[1] - rows[1]
    dz = cols[2] - rows[2]
    dz_sq = dz * dz
    dist_sq = dx * dx + dy * dy + dz_sq
    if diag is not None:
        dist_sq = jnp.where(diag, 1.0, dist_sq)
    inv = lax.rsqrt(dist_sq)
    dist = dist_sq * inv
    frac = dist - jnp.round(dist)
    t = frac * frac
    half_sin = frac * horner(HALF_SIN, t)
    half_cos = horner(HALF_COS, t)
    sine = half_sin * half_cos
    cosine = 1.0 - half_sin * half_sin
    u = inv * (0.5 / math.pi)
    aligned = dz_sq * (inv * inv)
    amp_imag = (u * u) * (1.0 - 3.0 * aligned)
    amp_real = u * ((1.0 - aligned) - amp_imag)
    h_real = amp_real * cosine - amp_imag * sine
    h_imag = amp_real * sine + amp_imag * cosine
    if diag is not None:
        h_real = jnp.where(diag, 0.0, h_real)
        h_imag = jnp.where(diag, 0.0, h_imag)
    return h_real, h_imag


def split(x):
    hi = x.astype(jnp.bfloat16)
    return hi, (x - hi.astype(jnp.float32)).astype(jnp.bfloat16)


def bdot(a, b):
    return jnp.dot(a, b, preferred_element_type=jnp.float32)


def exchange(
    n_row,
    n_grp,
    pos_in,
    det_in,
    pop_in,
    sec_in,
    base_in,
    accum_in,
    next_ref,
    accum_ref,
    olds,
    pos_ref,
    det_ref,
    stage,
    wide,
    rhs_hi,
    rhs_lo,
    row_buf,
    grp_buf,
    coef,
    send_sem,
    row_recv,
    grp_recv,
    row_ready,
    grp_ready,
    load_sem,
):
    cols, width = sec_in.shape[0] // 2, sec_in.shape[1]
    me = lax.axis_index("row")
    mine = lax.axis_index("grp")
    slab = cols * n_grp
    barrier = pltpu.get_barrier_semaphore()

    last = n_row - 2
    pair = me // 2
    odd = lax.rem(me, 2)
    partner = me + 1 - 2 * odd
    in_first = me < 2
    in_last = me >= last
    between = jnp.logical_not(in_first | in_last)
    even = odd == 0
    low = jnp.minimum(mine, 1)
    ahead = in_first & even & (mine > 0)
    GO, LATE, WORD = 0, 1, 2
    NEXT, REST = 0, 1

    def to_row(sem, lo, hi):
        def body(p, carry):
            pl.semaphore_signal(sem, inc=1, device_id={"row": p}, device_id_type=MESH)
            return carry

        lax.fori_loop(lo, hi, body, 0)

    def to_grp(sem, lo, hi):
        def body(p, carry):
            pl.semaphore_signal(sem, inc=1, device_id={"grp": p}, device_id_type=MESH)
            return carry

        lax.fori_loop(lo, hi, body, 0)

    slab_part = stage.at[0 : 2 * cols]

    def send_row(lo, hi):
        def body(p, carry):
            pltpu.make_async_remote_copy(
                stage,
                row_buf.at[me],
                send_sem.at[0],
                row_recv.at[jnp.where(me < last, 0, 1)],
                device_id={"row": p},
                device_id_type=MESH,
            ).start()
            return carry

        lax.fori_loop(lo, hi, body, 0)

    def send_grp(lo, hi, source):
        def body(p, carry):
            pltpu.make_async_remote_copy(
                source,
                grp_buf.at[mine],
                send_sem.at[1],
                grp_recv.at[jnp.where(mine < n_grp - 1, 0, 1)],
                device_id={"grp": p},
                device_id_type=MESH,
            ).start()
            return carry

        lax.fori_loop(lo, hi, body, 0)

    def arrived(part, sem):
        pltpu.make_async_copy(part, part, sem).wait()

    @pl.when(ahead)
    def _():
        pl.semaphore_wait(barrier, 1)
        send_grp(0, 1, sec_in)

    section_loads = [
        pltpu.make_async_copy(src, dst, load_sem.at[0])
        for src, dst in (
            (sec_in, stage.at[0 : 2 * cols]),
            (pop_in, stage.at[2 * cols : 2 * cols + 1]),
        )
    ]
    pos_load = pltpu.make_async_copy(pos_in, pos_ref, load_sem.at[1])
    det_load = pltpu.make_async_copy(det_in, det_ref, load_sem.at[2])
    old_loads = [
        pltpu.make_async_copy(src, olds.at[i], load_sem.at[3]) for i, src in enumerate((base_in, accum_in))
    ]
    for load in (*section_loads, pos_load, det_load, *old_loads):
        load.start()

    @pl.when(even & (mine > 0))
    def _():
        def body(p, carry):
            pl.semaphore_signal(barrier, inc=1, device_id={"row": partner, "grp": p}, device_id_type=MESH)
            return carry

        lax.fori_loop(mine + 1, n_grp, body, 0)

    @pl.when(jnp.logical_not(even & (mine > 0)))
    def _():
        to_grp(barrier, mine + 1, n_grp)

    @pl.when(even)
    def _():
        pl.semaphore_signal(barrier, inc=1, device_id={"row": partner}, device_id_type=MESH)

    after = jnp.where(in_first, 2, jnp.where(in_last, n_row, last))
    to_row(barrier, after, n_row)

    before = jnp.where(in_first, 0, jnp.where(in_last, last, 2))
    met = before + jnp.where(even, low, 1 + mine + mine - low)

    @pl.when((met > 0) & jnp.logical_not(ahead))
    def _():
        with jax.named_scope("bar"):
            pl.semaphore_wait(barrier, met)

    send_grp(0, jnp.where(even & jnp.logical_not(ahead), low, 0), sec_in)

    def answer_lower(lo, hi):
        to_grp(grp_ready.at[REST], lo, jnp.minimum(hi, mine - 1))
        to_grp(grp_ready.at[NEXT], jnp.maximum(lo, mine - 1), hi)

    answer_lower(0, low)

    @pl.when(between)
    def _():
        to_row(row_ready.at[GO], 0, 2)

    @pl.when(in_last)
    def _():
        to_row(row_ready.at[LATE], 0, last)

    @pl.when(jnp.logical_not(even))
    def _():
        pl.semaphore_signal(row_ready.at[WORD], inc=1, device_id={"row": partner}, device_id_type=MESH)
        answer_lower(low, mine)

    with jax.named_scope("load"):
        pos_load.wait()
        arrived(stage, load_sem.at[0])
    send_row(0, before)

    @pl.when(even)
    def _():
        with jax.named_scope("word"):
            pl.semaphore_wait(row_ready.at[WORD], 1)
        answer_lower(low, mine)
        send_grp(low, mine, slab_part)

    send_row(partner, partner + 1)

    my_start = pl.multiple_of(me * width, width)
    rows = [pos_ref[d : d + 1, pl.ds(my_start, width)] for d in range(3)]
    tiles = width // TILE

    def spread(tile, slot):
        start = pl.multiple_of(tile * TILE, TILE)
        for d in range(3):
            line = pos_ref[d : d + 1, pl.ds(start, TILE)]
            wide[slot, d] = jnp.transpose(jnp.broadcast_to(line, (TILE, TILE)))

    def fill(tile, slot, diag):
        start = pl.multiple_of(tile * TILE, TILE)
        for part in range(tiles):
            lanes = slice(part * TILE, (part + 1) * TILE)
            h_real, h_imag = coupling(
                [wide[slot, d] for d in range(3)],
                [r[:, lanes] for r in rows],
                None if diag is None else diag[:, lanes],
            )
            for base, h in ((0, h_real), (width, h_imag)):
                hi, lo = split(h)
                at = slice(base + part * TILE, base + (part + 1) * TILE)
                rhs_hi[pl.ds(start, TILE), at] = hi
                rhs_lo[pl.ds(start, TILE), at] = lo

    first = me * tiles
    total = n_row * tiles
    lane_ids = lax.broadcasted_iota(jnp.int32, (TILE, width), 1)
    sub_ids = lax.broadcasted_iota(jnp.int32, (TILE, width), 0)

    def tile_at(j):
        return lax.rem(first + j, total)

    with jax.named_scope("couple"):
        def lower_from_odd():
            @pl.when(jnp.logical_not(even))
            def _():
                send_grp(0, mine, slab_part)

        def step(j, carry):
            spread(tile_at(j + 1), lax.rem(j + 1, 2))
            fill(tile_at(j), lax.rem(j, 2), None)
            return carry

        spread(first, 0)
        for j in range(tiles):
            spread(tile_at(j + 1), (j + 1) % 2)
            fill(tile_at(j), j % 2, sub_ids + j * TILE == lane_ids)
        pause = tiles + PAUSE
        lax.fori_loop(tiles, pause, step, 0)
        lower_from_odd()
        lax.fori_loop(pause, total, step, 0, unroll=2)

    @pl.when(in_first & (last > 2))
    def _():
        with jax.named_scope("wmid"):
            pl.semaphore_wait(row_ready.at[GO], last - 2)

        @pl.when(odd == 1)
        def _():
            to_row(row_ready.at[GO], 2, last)

        send_row(2, last)

    @pl.when(between)
    def _():
        with jax.named_scope("wgo"):
            pl.semaphore_wait(row_ready.at[GO], 1)
        send_row(2, 2 * pair)
        send_row(2 * pair + 2, last)

    @pl.when(mine < n_grp - 1)
    def _():
        with jax.named_scope("ansnext"):
            pl.semaphore_wait(grp_ready.at[NEXT], 1)
        send_grp(mine + 1, mine + 2, slab_part)

    @pl.when(jnp.logical_not(in_last))
    def _():
        with jax.named_scope("wlate"):
            pl.semaphore_wait(row_ready.at[LATE], 2)
        send_row(last, n_row)

    @pl.when(mine < n_grp - 2)
    def _():
        with jax.named_scope("ansrest"):
            pl.semaphore_wait(grp_ready.at[REST], n_grp - 2 - mine)
        send_grp(mine + 2, n_grp, slab_part)

    det_load.wait()
    arrived(olds, load_sem.at[3])

    col_start = pl.multiple_of(mine * cols, cols)
    eye = lax.broadcasted_iota(jnp.int32, (cols, TILE), 0) + col_start == lax.broadcasted_iota(
        jnp.int32, (cols, TILE), 1
    )
    slab_rows = [pos_ref[d : d + 1, :TILE] for d in range(3)]
    own_cols = [
        jnp.sum(jnp.where(eye, jnp.broadcast_to(r, (cols, TILE)), 0.0), axis=1, keepdims=True) for r in slab_rows
    ]
    w_real, w_imag = coupling(own_cols, slab_rows, eye)
    w_real = AMPLITUDE * w_real + jnp.where(eye, det_ref[:, :TILE], 0.0)
    w_imag = AMPLITUDE * w_imag + jnp.where(eye, -0.5, 0.0)
    most = slab - cols
    l_hi, l_lo = split(jnp.concatenate([w_real, w_imag], axis=0)[:, :most])
    for j in range(cols):
        for lead, w in ((0, w_real), (cols, w_imag)):
            coef[j, lead : lead + cols] = jnp.broadcast_to(w[:, most + j : most + j + 1], (cols, width))

    y_local = stage[0 : 2 * cols]
    row_buf[me] = stage[...]
    grp_buf[mine] = y_local

    def left(slab_and_pop):
        signed = jnp.broadcast_to(2.0 * slab_and_pop[2 * cols :] - 1.0, (PAD, width))
        return split(jnp.concatenate([slab_and_pop[: 2 * cols], signed], axis=0))

    main = jnp.zeros((4 * cols + 2 * PAD, 2 * width), jnp.float32)
    rest = jnp.zeros((2 * cols + PAD, 2 * width), jnp.float32)
    group = 2
    for lead in range(0, n_row, group):
        his, los = [], []
        for at, count in ((0, last), (last, 2)):
            if lead == at:
                with jax.named_scope(f"wrow{lead}"):

                    @pl.when(in_last == (at == last))
                    def _():
                        arrived(row_buf.at[0 : count - 1], row_recv.at[at // last])

                    @pl.when(in_last != (at == last))
                    def _():
                        arrived(row_buf.at[0:count], row_recv.at[at // last])

        for p in range(lead, lead + group):
            hi, lo = left(row_buf[p])
            his.append(hi)
            los.append(lo)
        hi = jnp.concatenate(his, axis=1)
        lo = jnp.concatenate(los, axis=1)
        span = slice(lead * width, (lead + group) * width)
        main = main + bdot(jnp.concatenate([hi, lo], axis=0), rhs_hi[span, :])
        rest = rest + bdot(hi, rhs_lo[span, :])
    half = 2 * cols + PAD
    z = AMPLITUDE * (main[:half] + main[half:] + rest)
    z_real = z[:cols, :width] - z[cols : 2 * cols, width:]
    z_imag = z[:cols, width:] + z[cols : 2 * cols, :width]
    shift = z[2 * cols : 2 * cols + 1, :width]

    y_real, y_imag = y_local[:cols], y_local[cols:]
    total_shift = shift + det_ref[:, pl.ds(my_start, width)]
    z_real = z_real + total_shift * y_real + 0.5 * y_imag
    z_imag = z_imag + total_shift * y_imag - 0.5 * y_real

    top = n_grp - 1
    if n_grp > 2:
        with jax.named_scope("wgrp"):

            @pl.when(mine < top)
            def _():
                arrived(grp_buf.at[0 : top - 1], grp_recv.at[0])

            @pl.when(mine == top)
            def _():
                arrived(grp_buf.at[0:top], grp_recv.at[0])

    elif n_grp == 2:

        @pl.when(mine == top)
        def _():
            arrived(grp_buf.at[0:top], grp_recv.at[0])

    blocks = [grp_buf[g] for g in range(top)]
    full = jnp.concatenate(
        [jnp.concatenate([block[:cols], block[cols:]], axis=1) for block in blocks], axis=0
    )
    f_hi, f_lo = split(full)
    v = bdot(l_hi, f_hi) + bdot(l_lo, f_hi) + bdot(l_hi, f_lo)
    z_imag = z_imag - (v[:cols, width:] - v[cols:, :width])
    z_real = z_real - (v[:cols, :width] + v[cols:, width:])

    for i, rate in enumerate((z_imag, -z_real)):
        next_ref[i] = olds[0, i] + 0.5 * TIME_STEP * rate
        accum_ref[i] = olds[1, i] + TIME_STEP / 3.0 * rate

    with jax.named_scope("drain"):
        arrived(row_buf.at[0 : n_row - 1], send_sem.at[0])
        arrived(grp_buf.at[0 : n_grp - 1], send_sem.at[1])


def finish(n_grp, next_ref, accum_ref, grp_buf, coef, grp_recv):
    cols, width = coef.shape[0], coef.shape[2]
    mine, top = lax.axis_index("grp"), n_grp - 1

    with jax.named_scope("wtop"):

        @pl.when(mine < top)
        def _():
            pltpu.make_async_copy(grp_buf.at[0], grp_buf.at[0], grp_recv.at[1]).wait()

    sums = [[jnp.zeros((cols, width), jnp.float32)] * 4 for _ in range(2)]
    for j in range(cols):
        fr = grp_buf[top, j : j + 1]
        fi = grp_buf[top, cols + j : cols + j + 1]
        wr, wi = coef[j, :cols], coef[j, cols:]
        k = 2 * (j % 2)
        sums[0][k] = sums[0][k] + wr * fr
        sums[0][k + 1] = sums[0][k + 1] + wi * fi
        sums[1][k] = sums[1][k] + wr * fi
        sums[1][k + 1] = sums[1][k + 1] + wi * fr
    v_real = (sums[0][0] + sums[0][1]) + (sums[0][2] + sums[0][3])
    v_imag = (sums[1][0] + sums[1][2]) - (sums[1][1] + sums[1][3])
    for i, rate in enumerate((-v_imag, v_real)):
        next_ref[i] = next_ref[i] + 0.5 * TIME_STEP * rate
        accum_ref[i] = accum_ref[i] + TIME_STEP / 3.0 * rate


def kernel(n_row, n_grp, pos_in, det_in, pop_in, sec_in, base_in, accum_in, next_ref, accum_ref, olds, pos_ref, det_ref, stage, wide, rhs_hi, rhs_lo, row_buf, grp_buf, coef, row_recv, grp_recv, row_ready, grp_ready):
    def scope(load_sem, send_sem):
        exchange(n_row=n_row, n_grp=n_grp, pos_in=pos_in, det_in=det_in, pop_in=pop_in, sec_in=sec_in, base_in=base_in, accum_in=accum_in, next_ref=next_ref, accum_ref=accum_ref, olds=olds, pos_ref=pos_ref, det_ref=det_ref, stage=stage, wide=wide, rhs_hi=rhs_hi, rhs_lo=rhs_lo, row_buf=row_buf, grp_buf=grp_buf, coef=coef, row_recv=row_recv, grp_recv=grp_recv, row_ready=row_ready, grp_ready=grp_ready, load_sem=load_sem, send_sem=send_sem)

    pl.run_scoped(scope, load_sem=pltpu.SemaphoreType.DMA((4,)), send_sem=pltpu.SemaphoreType.DMA((2,)))
    finish(n_grp, next_ref, accum_ref, grp_buf, coef, grp_recv)


def store(next_ref, accum_ref, next_out, accum_out):
    def scope(sem):
        copies = [
            pltpu.make_async_copy(next_ref, next_out, sem.at[0]),
            pltpu.make_async_copy(accum_ref, accum_out, sem.at[1]),
        ]
        for copy in copies:
            copy.start()
        for copy in copies:
            copy.wait()

    pl.run_scoped(scope, pltpu.SemaphoreType.DMA((2,)))


def local(positions, detuning, populations, base, section, accum):
    n_row, n_grp = lax.axis_size("row"), lax.axis_size("grp")
    cols, width = section.shape[1], section.shape[2]
    total = positions.shape[1]
    block = section.shape
    results = pl.pallas_call(
        functools.partial(kernel, n_row, n_grp),
        out_shape=(pltpu.VMEM(block, jnp.float32), pltpu.VMEM(block, jnp.float32)),
        in_specs=[pl.BlockSpec(memory_space=pl.ANY)] * 6,
        out_specs=(pl.BlockSpec(memory_space=pltpu.VMEM), pl.BlockSpec(memory_space=pltpu.VMEM)),
        scratch_shapes=[
            pltpu.VMEM((2, *block), jnp.float32),
            pltpu.VMEM((3, total), jnp.float32),
            pltpu.VMEM((1, total), jnp.float32),
            pltpu.VMEM((2 * cols + 1, width), jnp.float32),
            pltpu.VMEM((2, 3, TILE, TILE), jnp.float32),
            pltpu.VMEM((total, 2 * width), jnp.bfloat16),
            pltpu.VMEM((total, 2 * width), jnp.bfloat16),
            pltpu.VMEM((n_row, 2 * cols + 1, width), jnp.float32),
            pltpu.VMEM((n_grp, 2 * cols, width), jnp.float32),
            pltpu.VMEM((cols, 2 * cols, width), jnp.float32),
            pltpu.SemaphoreType.DMA((2,)),
            pltpu.SemaphoreType.DMA((2,)),
            pltpu.SemaphoreType.REGULAR((3,)),
            pltpu.SemaphoreType.REGULAR((2,)),
        ],
        compiler_params=pltpu.CompilerParams(collective_id=0, has_side_effects=True),
    )(positions, detuning.reshape(1, total), populations.reshape(1, width), section.reshape(2 * cols, width), base, accum)
    return pl.pallas_call(
        store,
        out_shape=(jax.ShapeDtypeStruct(block, jnp.float32),) * 2,
        in_specs=[pl.BlockSpec(memory_space=pltpu.VMEM)] * 2,
        out_specs=(pl.BlockSpec(memory_space=pltpu.HBM),) * 2,
    )(*[pltpu.with_memory_space_constraint(r, pltpu.VMEM) for r in results])


def solution(mesh):
    return jax.shard_map(
        local,
        mesh=mesh,
        in_specs=(
            P(),
            P(),
            P("row"),
            P(None, "grp", "row"),
            P(None, "grp", "row"),
            P(None, "grp", "row"),
        ),
        out_specs=(P(None, "grp", "row"), P(None, "grp", "row")),
        check_vma=False,
    )
```

```python
import functools
import math

import jax
import jax.numpy as jnp
from jax import lax
from jax.experimental import pallas as pl
from jax.experimental.pallas import tpu as pltpu
from jax.sharding import PartitionSpec as P

TIME_STEP = 0.2
PAD = 16
TILE = 128
AMPLITUDE = -0.75
PAUSE = 1

HALF_SIN = (4.442882834149929, -7.308241154546326, 3.606288958225646, -0.8457635961475002, 0.10920575363724722)
HALF_COS = (1.4142134965650124, -6.97885098823893, 5.739461170681154, -1.8835629872981716, 0.31069819180355424)
MESH = pl.DeviceIdType.MESH


def horner(coeffs, t):
    total = coeffs[-1] * t + coeffs[-2]
    for value in coeffs[-3::-1]:
        total = total * t + value
    return total


def coupling(cols, rows, diag):
    dx = cols[0] - rows[0]
    dy = cols[1] - rows[1]
    dz = cols[2] - rows[2]
    dz_sq = dz * dz
    dist_sq = dx * dx + dy * dy + dz_sq
    if diag is not None:
        dist_sq = jnp.where(diag, 1.0, dist_sq)
    inv = lax.rsqrt(dist_sq)
    dist = dist_sq * inv
    frac = dist - jnp.round(dist)
    t = frac * frac
    half_sin = frac * horner(HALF_SIN, t)
    half_cos = horner(HALF_COS, t)
    sine = half_sin * half_cos
    cosine = 1.0 - half_sin * half_sin
    u = inv * (0.5 / math.pi)
    aligned = dz_sq * (inv * inv)
    amp_imag = (u * u) * (1.0 - 3.0 * aligned)
    amp_real = u * ((1.0 - aligned) - amp_imag)
    h_real = amp_real * cosine - amp_imag * sine
    h_imag = amp_real * sine + amp_imag * cosine
    if diag is not None:
        h_real = jnp.where(diag, 0.0, h_real)
        h_imag = jnp.where(diag, 0.0, h_imag)
    return h_real, h_imag


def split(x):
    hi = x.astype(jnp.bfloat16)
    return hi, (x - hi.astype(jnp.float32)).astype(jnp.bfloat16)


def bdot(a, b):
    return jnp.dot(a, b, preferred_element_type=jnp.float32)


def exchange(
    n_row,
    n_grp,
    pos_in,
    det_in,
    pop_in,
    sec_in,
    base_in,
    accum_in,
    next_ref,
    accum_ref,
    olds,
    pos_ref,
    det_ref,
    stage,
    wide,
    rhs_hi,
    rhs_lo,
    row_buf,
    grp_buf,
    coef,
    send_sem,
    row_recv,
    grp_recv,
    row_ready,
    grp_ready,
    load_sem,
):
    cols, width = sec_in.shape[0] // 2, sec_in.shape[1]
    me = lax.axis_index("row")
    mine = lax.axis_index("grp")
    slab = cols * n_grp
    barrier = pltpu.get_barrier_semaphore()

    last = n_row - 2
    pair = me // 2
    odd = lax.rem(me, 2)
    partner = me + 1 - 2 * odd
    in_first = me < 2
    in_last = me >= last
    between = jnp.logical_not(in_first | in_last)
    even = odd == 0
    low = jnp.minimum(mine, 1)
    ahead = in_first & even & (mine > 0)
    GO, LATE, WORD = 0, 1, 2
    NEXT, REST = 0, 1

    def to_row(sem, lo, hi):
        def body(p, carry):
            pl.semaphore_signal(sem, inc=1, device_id={"row": p}, device_id_type=MESH)
            return carry

        lax.fori_loop(lo, hi, body, 0)

    def to_grp(sem, lo, hi):
        def body(p, carry):
            pl.semaphore_signal(sem, inc=1, device_id={"grp": p}, device_id_type=MESH)
            return carry

        lax.fori_loop(lo, hi, body, 0)

    slab_part = stage.at[0 : 2 * cols]

    def send_row(lo, hi):
        def body(p, carry):
            pltpu.make_async_remote_copy(
                stage,
                row_buf.at[me],
                send_sem.at[0],
                row_recv.at[jnp.where(me < last, 0, 1)],
                device_id={"row": p},
                device_id_type=MESH,
            ).start()
            return carry

        lax.fori_loop(lo, hi, body, 0)

    def send_grp(lo, hi, source):
        def body(p, carry):
            pltpu.make_async_remote_copy(
                source,
                grp_buf.at[mine],
                send_sem.at[1],
                grp_recv.at[jnp.where(mine < n_grp - 1, 0, 1)],
                device_id={"grp": p},
                device_id_type=MESH,
            ).start()
            return carry

        lax.fori_loop(lo, hi, body, 0)

    def arrived(part, sem):
        pltpu.make_async_copy(part, part, sem).wait()

    @pl.when(ahead)
    def _():
        pl.semaphore_wait(barrier, 1)
        send_grp(0, 1, sec_in)

    section_loads = [
        pltpu.make_async_copy(src, dst, load_sem.at[0])
        for src, dst in (
            (sec_in, stage.at[0 : 2 * cols]),
            (pop_in, stage.at[2 * cols : 2 * cols + 1]),
        )
    ]
    pos_load = pltpu.make_async_copy(pos_in, pos_ref, load_sem.at[1])
    det_load = pltpu.make_async_copy(det_in, det_ref, load_sem.at[2])
    old_loads = [
        pltpu.make_async_copy(src, olds.at[i], load_sem.at[3]) for i, src in enumerate((base_in, accum_in))
    ]
    for load in (*section_loads, pos_load, det_load, *old_loads):
        load.start()

    @pl.when(even & (mine > 0))
    def _():
        def body(p, carry):
            pl.semaphore_signal(barrier, inc=1, device_id={"row": partner, "grp": p}, device_id_type=MESH)
            return carry

        lax.fori_loop(mine + 1, n_grp, body, 0)

    @pl.when(jnp.logical_not(even & (mine > 0)))
    def _():
        to_grp(barrier, mine + 1, n_grp)

    @pl.when(even)
    def _():
        pl.semaphore_signal(barrier, inc=1, device_id={"row": partner}, device_id_type=MESH)

    after = jnp.where(in_first, 2, jnp.where(in_last, n_row, last))
    to_row(barrier, after, n_row)

    before = jnp.where(in_first, 0, jnp.where(in_last, last, 2))
    met = before + jnp.where(even, low, 1 + mine + mine - low)

    @pl.when((met > 0) & jnp.logical_not(ahead))
    def _():
        with jax.named_scope("bar"):
            pl.semaphore_wait(barrier, met)

    send_grp(0, jnp.where(even & jnp.logical_not(ahead), low, 0), sec_in)

    def answer_lower(lo, hi):
        to_grp(grp_ready.at[REST], lo, jnp.minimum(hi, mine - 1))
        to_grp(grp_ready.at[NEXT], jnp.maximum(lo, mine - 1), hi)

    answer_lower(0, low)

    @pl.when(between)
    def _():
        to_row(row_ready.at[GO], 0, 2)

    @pl.when(in_last)
    def _():
        to_row(row_ready.at[LATE], 0, last)

    @pl.when(jnp.logical_not(even))
    def _():
        pl.semaphore_signal(row_ready.at[WORD], inc=1, device_id={"row": partner}, device_id_type=MESH)
        answer_lower(low, mine)

    with jax.named_scope("load"):
        pos_load.wait()
        arrived(stage, load_sem.at[0])
    send_row(0, before)

    @pl.when(even)
    def _():
        with jax.named_scope("word"):
            pl.semaphore_wait(row_ready.at[WORD], 1)
        answer_lower(low, mine)
        send_grp(low, mine, slab_part)

    send_row(partner, partner + 1)

    my_start = pl.multiple_of(me * width, width)
    rows = [pos_ref[d : d + 1, pl.ds(my_start, width)] for d in range(3)]
    tiles = width // TILE

    def spread(tile, slot):
        start = pl.multiple_of(tile * TILE, TILE)
        for d in range(3):
            line = pos_ref[d : d + 1, pl.ds(start, TILE)]
            wide[slot, d] = jnp.transpose(jnp.broadcast_to(line, (TILE, TILE)))

    def fill(tile, slot, diag):
        start = pl.multiple_of(tile * TILE, TILE)
        for part in range(tiles):
            lanes = slice(part * TILE, (part + 1) * TILE)
            h_real, h_imag = coupling(
                [wide[slot, d] for d in range(3)],
                [r[:, lanes] for r in rows],
                None if diag is None else diag[:, lanes],
            )
            for base, h in ((0, h_real), (width, h_imag)):
                hi, lo = split(h)
                at = slice(base + part * TILE, base + (part + 1) * TILE)
                rhs_hi[pl.ds(start, TILE), at] = hi
                rhs_lo[pl.ds(start, TILE), at] = lo

    first = me * tiles
    total = n_row * tiles
    lane_ids = lax.broadcasted_iota(jnp.int32, (TILE, width), 1)
    sub_ids = lax.broadcasted_iota(jnp.int32, (TILE, width), 0)

    def tile_at(j):
        return lax.rem(first + j, total)

    with jax.named_scope("couple"):
        def lower_from_odd():
            @pl.when(jnp.logical_not(even))
            def _():
                send_grp(0, mine, slab_part)

        def step(j, carry):
            spread(tile_at(j + 1), lax.rem(j + 1, 2))
            fill(tile_at(j), lax.rem(j, 2), None)
            return carry

        flat = total <= 16
        spread(first, 0)
        for j in range(total if flat else tiles):
            if j == tiles + PAUSE:
                lower_from_odd()
            if j + 1 < total:
                spread(tile_at(j + 1), (j + 1) % 2)
            fill(tile_at(j), j % 2, sub_ids + j * TILE == lane_ids if j < tiles else None)
        if not flat:
            lower_from_odd()
            lax.fori_loop(tiles, total, step, 0)

    @pl.when(in_first & (last > 2))
    def _():
        with jax.named_scope("wmid"):
            pl.semaphore_wait(row_ready.at[GO], last - 2)

        @pl.when(odd == 1)
        def _():
            to_row(row_ready.at[GO], 2, last)

        send_row(2, last)

    @pl.when(between)
    def _():
        with jax.named_scope("wgo"):
            pl.semaphore_wait(row_ready.at[GO], 1)
        send_row(2, 2 * pair)
        send_row(2 * pair + 2, last)

    @pl.when(mine < n_grp - 1)
    def _():
        with jax.named_scope("ansnext"):
            pl.semaphore_wait(grp_ready.at[NEXT], 1)
        send_grp(mine + 1, mine + 2, slab_part)

    @pl.when(jnp.logical_not(in_last))
    def _():
        with jax.named_scope("wlate"):
            pl.semaphore_wait(row_ready.at[LATE], 2)
        send_row(last, n_row)

    @pl.when(mine < n_grp - 2)
    def _():
        with jax.named_scope("ansrest"):
            pl.semaphore_wait(grp_ready.at[REST], n_grp - 2 - mine)
        send_grp(mine + 2, n_grp, slab_part)

    det_load.wait()
    arrived(olds, load_sem.at[3])

    col_start = pl.multiple_of(mine * cols, cols)
    eye = lax.broadcasted_iota(jnp.int32, (cols, TILE), 0) + col_start == lax.broadcasted_iota(
        jnp.int32, (cols, TILE), 1
    )
    slab_rows = [pos_ref[d : d + 1, :TILE] for d in range(3)]
    own_cols = [
        jnp.sum(jnp.where(eye, jnp.broadcast_to(r, (cols, TILE)), 0.0), axis=1, keepdims=True) for r in slab_rows
    ]
    w_real, w_imag = coupling(own_cols, slab_rows, eye)
    w_real = AMPLITUDE * w_real + jnp.where(eye, det_ref[:, :TILE], 0.0)
    w_imag = AMPLITUDE * w_imag + jnp.where(eye, -0.5, 0.0)
    most = slab - cols
    l_hi, l_lo = split(jnp.concatenate([w_real, w_imag], axis=0)[:, :most])
    for j in range(cols):
        for lead, w in ((0, w_real), (cols, w_imag)):
            coef[j, lead : lead + cols] = jnp.broadcast_to(w[:, most + j : most + j + 1], (cols, width))

    y_local = stage[0 : 2 * cols]
    row_buf[me] = stage[...]
    grp_buf[mine] = y_local

    def left(slab_and_pop):
        signed = jnp.broadcast_to(2.0 * slab_and_pop[2 * cols :] - 1.0, (PAD, width))
        return split(jnp.concatenate([slab_and_pop[: 2 * cols], signed], axis=0))

    main = jnp.zeros((4 * cols + 2 * PAD, 2 * width), jnp.float32)
    rest = jnp.zeros((2 * cols + PAD, 2 * width), jnp.float32)
    group = 2
    for lead in range(0, n_row, group):
        his, los = [], []
        for at, count in ((0, last), (last, 2)):
            if lead == at:
                with jax.named_scope(f"wrow{lead}"):

                    @pl.when(in_last == (at == last))
                    def _():
                        arrived(row_buf.at[0 : count - 1], row_recv.at[at // last])

                    @pl.when(in_last != (at == last))
                    def _():
                        arrived(row_buf.at[0:count], row_recv.at[at // last])

        for p in range(lead, lead + group):
            hi, lo = left(row_buf[p])
            his.append(hi)
            los.append(lo)
        hi = jnp.concatenate(his, axis=1)
        lo = jnp.concatenate(los, axis=1)
        span = slice(lead * width, (lead + group) * width)
        main = main + bdot(jnp.concatenate([hi, lo], axis=0), rhs_hi[span, :])
        rest = rest + bdot(hi, rhs_lo[span, :])
    half = 2 * cols + PAD
    z = AMPLITUDE * (main[:half] + main[half:] + rest)
    z_real = z[:cols, :width] - z[cols : 2 * cols, width:]
    z_imag = z[:cols, width:] + z[cols : 2 * cols, :width]
    shift = z[2 * cols : 2 * cols + 1, :width]

    y_real, y_imag = y_local[:cols], y_local[cols:]
    total_shift = shift + det_ref[:, pl.ds(my_start, width)]
    z_real = z_real + total_shift * y_real + 0.5 * y_imag
    z_imag = z_imag + total_shift * y_imag - 0.5 * y_real

    top = n_grp - 1
    if n_grp > 2:
        with jax.named_scope("wgrp"):

            @pl.when(mine < top)
            def _():
                arrived(grp_buf.at[0 : top - 1], grp_recv.at[0])

            @pl.when(mine == top)
            def _():
                arrived(grp_buf.at[0:top], grp_recv.at[0])

    elif n_grp == 2:

        @pl.when(mine == top)
        def _():
            arrived(grp_buf.at[0:top], grp_recv.at[0])

    blocks = [grp_buf[g] for g in range(top)]
    full = jnp.concatenate(
        [jnp.concatenate([block[:cols], block[cols:]], axis=1) for block in blocks], axis=0
    )
    f_hi, f_lo = split(full)
    v = bdot(l_hi, f_hi) + bdot(l_lo, f_hi) + bdot(l_hi, f_lo)
    z_imag = z_imag - (v[:cols, width:] - v[cols:, :width])
    z_real = z_real - (v[:cols, :width] + v[cols:, width:])

    for i, rate in enumerate((z_imag, -z_real)):
        next_ref[i] = olds[0, i] + 0.5 * TIME_STEP * rate
        accum_ref[i] = olds[1, i] + TIME_STEP / 3.0 * rate

    with jax.named_scope("drain"):
        arrived(row_buf.at[0 : n_row - 1], send_sem.at[0])
        arrived(grp_buf.at[0 : n_grp - 1], send_sem.at[1])


def finish(n_grp, next_ref, accum_ref, grp_buf, coef, grp_recv):
    cols, width = coef.shape[0], coef.shape[2]
    mine, top = lax.axis_index("grp"), n_grp - 1

    with jax.named_scope("wtop"):

        @pl.when(mine < top)
        def _():
            pltpu.make_async_copy(grp_buf.at[0], grp_buf.at[0], grp_recv.at[1]).wait()

    sums = [[jnp.zeros((cols, width), jnp.float32)] * 4 for _ in range(2)]
    for j in range(cols):
        fr = grp_buf[top, j : j + 1]
        fi = grp_buf[top, cols + j : cols + j + 1]
        wr, wi = coef[j, :cols], coef[j, cols:]
        k = 2 * (j % 2)
        sums[0][k] = sums[0][k] + wr * fr
        sums[0][k + 1] = sums[0][k + 1] + wi * fi
        sums[1][k] = sums[1][k] + wr * fi
        sums[1][k + 1] = sums[1][k + 1] + wi * fr
    v_real = (sums[0][0] + sums[0][1]) + (sums[0][2] + sums[0][3])
    v_imag = (sums[1][0] + sums[1][2]) - (sums[1][1] + sums[1][3])
    for i, rate in enumerate((-v_imag, v_real)):
        next_ref[i] = next_ref[i] + 0.5 * TIME_STEP * rate
        accum_ref[i] = accum_ref[i] + TIME_STEP / 3.0 * rate


def kernel(n_row, n_grp, pos_in, det_in, pop_in, sec_in, base_in, accum_in, next_ref, accum_ref, olds, pos_ref, det_ref, stage, wide, rhs_hi, rhs_lo, row_buf, grp_buf, coef):
    def scope(row_recv, grp_recv, row_ready, grp_ready, load_sem, send_sem):
        exchange(n_row=n_row, n_grp=n_grp, pos_in=pos_in, det_in=det_in, pop_in=pop_in, sec_in=sec_in, base_in=base_in, accum_in=accum_in, next_ref=next_ref, accum_ref=accum_ref, olds=olds, pos_ref=pos_ref, det_ref=det_ref, stage=stage, wide=wide, rhs_hi=rhs_hi, rhs_lo=rhs_lo, row_buf=row_buf, grp_buf=grp_buf, coef=coef, row_recv=row_recv, grp_recv=grp_recv, row_ready=row_ready, grp_ready=grp_ready, load_sem=load_sem, send_sem=send_sem)
        finish(n_grp, next_ref, accum_ref, grp_buf, coef, grp_recv)

    pl.run_scoped(
        scope,
        row_recv=pltpu.SemaphoreType.DMA((2,)),
        grp_recv=pltpu.SemaphoreType.DMA((2,)),
        row_ready=pltpu.SemaphoreType.REGULAR((3,)),
        grp_ready=pltpu.SemaphoreType.REGULAR((2,)),
        load_sem=pltpu.SemaphoreType.DMA((4,)),
        send_sem=pltpu.SemaphoreType.DMA((2,)),
    )


def store(next_ref, accum_ref, next_out, accum_out):
    def scope(sem):
        copies = [
            pltpu.make_async_copy(next_ref, next_out, sem.at[0]),
            pltpu.make_async_copy(accum_ref, accum_out, sem.at[1]),
        ]
        for copy in copies:
            copy.start()
        for copy in copies:
            copy.wait()

    pl.run_scoped(scope, pltpu.SemaphoreType.DMA((2,)))


def local(positions, detuning, populations, base, section, accum):
    n_row, n_grp = lax.axis_size("row"), lax.axis_size("grp")
    cols, width = section.shape[1], section.shape[2]
    total = positions.shape[1]
    block = section.shape
    results = pl.pallas_call(
        functools.partial(kernel, n_row, n_grp),
        out_shape=(pltpu.VMEM(block, jnp.float32), pltpu.VMEM(block, jnp.float32)),
        in_specs=[pl.BlockSpec(memory_space=pl.ANY)] * 6,
        out_specs=(pl.BlockSpec(memory_space=pltpu.VMEM), pl.BlockSpec(memory_space=pltpu.VMEM)),
        scratch_shapes=[
            pltpu.VMEM((2, *block), jnp.float32),
            pltpu.VMEM((3, total), jnp.float32),
            pltpu.VMEM((1, total), jnp.float32),
            pltpu.VMEM((2 * cols + 1, width), jnp.float32),
            pltpu.VMEM((2, 3, TILE, TILE), jnp.float32),
            pltpu.VMEM((total, 2 * width), jnp.bfloat16),
            pltpu.VMEM((total, 2 * width), jnp.bfloat16),
            pltpu.VMEM((n_row, 2 * cols + 1, width), jnp.float32),
            pltpu.VMEM((n_grp, 2 * cols, width), jnp.float32),
            pltpu.VMEM((cols, 2 * cols, width), jnp.float32),
        ],
        compiler_params=pltpu.CompilerParams(collective_id=0, has_side_effects=True),
    )(positions, detuning.reshape(1, total), populations.reshape(1, width), section.reshape(2 * cols, width), base, accum)
    return pl.pallas_call(
        store,
        out_shape=(jax.ShapeDtypeStruct(block, jnp.float32),) * 2,
        in_specs=[pl.BlockSpec(memory_space=pltpu.VMEM)] * 2,
        out_specs=(pl.BlockSpec(memory_space=pltpu.HBM),) * 2,
    )(*[pltpu.with_memory_space_constraint(r, pltpu.VMEM) for r in results])


def solution(mesh):
    return jax.shard_map(
        local,
        mesh=mesh,
        in_specs=(
            P(),
            P(),
            P("row"),
            P(None, "grp", "row"),
            P(None, "grp", "row"),
            P(None, "grp", "row"),
        ),
        out_specs=(P(None, "grp", "row"), P(None, "grp", "row")),
        check_vma=False,
    )
```

```python
import functools
import math

import jax
import jax.numpy as jnp
from jax import lax
from jax.experimental import pallas as pl
from jax.experimental.pallas import tpu as pltpu
from jax.sharding import PartitionSpec as P

TIME_STEP = 0.2
PAD = 16
TILE = 128
AMPLITUDE = -0.75
PAUSE = 1

HALF_SIN = (4.442882834149929, -7.308241154546326, 3.606288958225646, -0.8457635961475002, 0.10920575363724722)
HALF_COS = (1.4142134965650124, -6.97885098823893, 5.739461170681154, -1.8835629872981716, 0.31069819180355424)
MESH = pl.DeviceIdType.MESH


def horner(coeffs, t):
    total = coeffs[-1] * t + coeffs[-2]
    for value in coeffs[-3::-1]:
        total = total * t + value
    return total


def coupling(cols, rows, diag):
    dx = cols[0] - rows[0]
    dy = cols[1] - rows[1]
    dz = cols[2] - rows[2]
    dz_sq = dz * dz
    dist_sq = dx * dx + dy * dy + dz_sq
    if diag is not None:
        dist_sq = jnp.where(diag, 1.0, dist_sq)
    inv = lax.rsqrt(dist_sq)
    dist = dist_sq * inv
    frac = dist - jnp.round(dist)
    t = frac * frac
    half_sin = frac * horner(HALF_SIN, t)
    half_cos = horner(HALF_COS, t)
    sine = half_sin * half_cos
    cosine = 1.0 - half_sin * half_sin
    u = inv * (0.5 / math.pi)
    aligned = dz_sq * (inv * inv)
    amp_imag = (u * u) * (1.0 - 3.0 * aligned)
    amp_real = u * ((1.0 - aligned) - amp_imag)
    h_real = amp_real * cosine - amp_imag * sine
    h_imag = amp_real * sine + amp_imag * cosine
    if diag is not None:
        h_real = jnp.where(diag, 0.0, h_real)
        h_imag = jnp.where(diag, 0.0, h_imag)
    return h_real, h_imag


def split(x):
    hi = x.astype(jnp.bfloat16)
    return hi, (x - hi.astype(jnp.float32)).astype(jnp.bfloat16)


def bdot(a, b):
    return jnp.dot(a, b, preferred_element_type=jnp.float32)


def exchange(
    n_row,
    n_grp,
    pos_in,
    det_in,
    pop_in,
    sec_in,
    base_in,
    accum_in,
    next_ref,
    accum_ref,
    olds,
    pos_ref,
    det_ref,
    stage,
    wide,
    rhs_hi,
    rhs_lo,
    row_buf,
    grp_buf,
    coef,
    send_sem,
    row_recv,
    grp_recv,
    row_ready,
    grp_ready,
    load_sem,
):
    cols, width = sec_in.shape[0] // 2, sec_in.shape[1]
    me = lax.axis_index("row")
    mine = lax.axis_index("grp")
    slab = cols * n_grp
    barrier = pltpu.get_barrier_semaphore()

    last = n_row - 2
    pair = me // 2
    odd = lax.rem(me, 2)
    partner = me + 1 - 2 * odd
    in_first = me < 2
    in_last = me >= last
    between = jnp.logical_not(in_first | in_last)
    even = odd == 0
    low = jnp.minimum(mine, 1)
    ahead = in_first & even & (mine > 0)
    GO, LATE, WORD = 0, 1, 2
    NEXT, REST = 0, 1

    def to_row(sem, lo, hi):
        def body(p, carry):
            pl.semaphore_signal(sem, inc=1, device_id={"row": p}, device_id_type=MESH)
            return carry

        lax.fori_loop(lo, hi, body, 0)

    def to_grp(sem, lo, hi):
        def body(p, carry):
            pl.semaphore_signal(sem, inc=1, device_id={"grp": p}, device_id_type=MESH)
            return carry

        lax.fori_loop(lo, hi, body, 0)

    slab_part = stage.at[0 : 2 * cols]

    def send_row(lo, hi):
        def body(p, carry):
            pltpu.make_async_remote_copy(
                stage,
                row_buf.at[me],
                send_sem.at[0],
                row_recv.at[jnp.where(me < last, 0, 1)],
                device_id={"row": p},
                device_id_type=MESH,
            ).start()
            return carry

        lax.fori_loop(lo, hi, body, 0)

    def send_grp(lo, hi, source):
        def body(p, carry):
            pltpu.make_async_remote_copy(
                source,
                grp_buf.at[mine],
                send_sem.at[1],
                grp_recv.at[jnp.where(mine < n_grp - 1, 0, 1)],
                device_id={"grp": p},
                device_id_type=MESH,
            ).start()
            return carry

        lax.fori_loop(lo, hi, body, 0)

    def arrived(part, sem):
        pltpu.make_async_copy(part, part, sem).wait()

    @pl.when(ahead)
    def _():
        pl.semaphore_wait(barrier, 1)
        send_grp(0, 1, sec_in)

    section_loads = [
        pltpu.make_async_copy(src, dst, load_sem.at[0])
        for src, dst in (
            (sec_in, stage.at[0 : 2 * cols]),
            (pop_in, stage.at[2 * cols : 2 * cols + 1]),
        )
    ]
    pos_load = pltpu.make_async_copy(pos_in, pos_ref, load_sem.at[1])
    det_load = pltpu.make_async_copy(det_in, det_ref, load_sem.at[2])
    old_loads = [
        pltpu.make_async_copy(src, olds.at[i], load_sem.at[3]) for i, src in enumerate((base_in, accum_in))
    ]
    for load in (*section_loads, pos_load, det_load, *old_loads):
        load.start()

    @pl.when(even & (mine > 0))
    def _():
        def body(p, carry):
            pl.semaphore_signal(barrier, inc=1, device_id={"row": partner, "grp": p}, device_id_type=MESH)
            return carry

        lax.fori_loop(mine + 1, n_grp, body, 0)

    @pl.when(jnp.logical_not(even & (mine > 0)))
    def _():
        to_grp(barrier, mine + 1, n_grp)

    @pl.when(even)
    def _():
        pl.semaphore_signal(barrier, inc=1, device_id={"row": partner}, device_id_type=MESH)

    after = jnp.where(in_first, 2, jnp.where(in_last, n_row, last))
    to_row(barrier, after, n_row)

    before = jnp.where(in_first, 0, jnp.where(in_last, last, 2))
    met = before + jnp.where(even, low, 1 + mine + mine - low)

    @pl.when((met > 0) & jnp.logical_not(ahead))
    def _():
        with jax.named_scope("bar"):
            pl.semaphore_wait(barrier, met)

    send_grp(0, jnp.where(even & jnp.logical_not(ahead), low, 0), sec_in)

    def answer_lower(lo, hi):
        to_grp(grp_ready.at[REST], lo, jnp.minimum(hi, mine - 1))
        to_grp(grp_ready.at[NEXT], jnp.maximum(lo, mine - 1), hi)

    answer_lower(0, low)

    @pl.when(between)
    def _():
        to_row(row_ready.at[GO], 0, 2)

    @pl.when(in_last)
    def _():
        to_row(row_ready.at[LATE], 0, last)

    @pl.when(jnp.logical_not(even))
    def _():
        pl.semaphore_signal(row_ready.at[WORD], inc=1, device_id={"row": partner}, device_id_type=MESH)
        answer_lower(low, mine)

    def hear_between():
        with jax.named_scope("wmid"):
            pl.semaphore_wait(row_ready.at[GO], last - 2)

        @pl.when(odd == 1)
        def _():
            to_row(row_ready.at[GO], 2, last)

    @pl.when(in_first & (mine == 0) & (last > 2))
    def _():
        hear_between()

    with jax.named_scope("load"):
        pos_load.wait()
        arrived(stage, load_sem.at[0])
    send_row(jnp.where(in_first, 2, 0), jnp.where(in_first, jnp.where(mine == 0, last, 2), before))

    @pl.when(even)
    def _():
        with jax.named_scope("word"):
            pl.semaphore_wait(row_ready.at[WORD], 1)
        answer_lower(low, mine)
        send_grp(low, mine, slab_part)

    send_row(partner, partner + 1)

    my_start = pl.multiple_of(me * width, width)
    rows = [pos_ref[d : d + 1, pl.ds(my_start, width)] for d in range(3)]
    tiles = width // TILE

    def spread(tile, slot):
        start = pl.multiple_of(tile * TILE, TILE)
        for d in range(3):
            line = pos_ref[d : d + 1, pl.ds(start, TILE)]
            wide[slot, d] = jnp.transpose(jnp.broadcast_to(line, (TILE, TILE)))

    def fill(tile, slot, diag):
        start = pl.multiple_of(tile * TILE, TILE)
        for part in range(tiles):
            lanes = slice(part * TILE, (part + 1) * TILE)
            h_real, h_imag = coupling(
                [wide[slot, d] for d in range(3)],
                [r[:, lanes] for r in rows],
                None if diag is None else diag[:, lanes],
            )
            for base, h in ((0, h_real), (width, h_imag)):
                hi, lo = split(h)
                at = slice(base + part * TILE, base + (part + 1) * TILE)
                rhs_hi[pl.ds(start, TILE), at] = hi
                rhs_lo[pl.ds(start, TILE), at] = lo

    first = me * tiles
    total = n_row * tiles
    lane_ids = lax.broadcasted_iota(jnp.int32, (TILE, width), 1)
    sub_ids = lax.broadcasted_iota(jnp.int32, (TILE, width), 0)

    def tile_at(j):
        return lax.rem(first + j, total)

    with jax.named_scope("couple"):
        def lower_from_odd():
            @pl.when(jnp.logical_not(even))
            def _():
                send_grp(0, mine, slab_part)

        def step(j, carry):
            spread(tile_at(j + 1), lax.rem(j + 1, 2))
            fill(tile_at(j), lax.rem(j, 2), None)
            return carry

        flat = total <= 16
        spread(first, 0)
        for j in range(total if flat else tiles):
            if j == tiles + PAUSE:
                lower_from_odd()
            if j + 1 < total:
                spread(tile_at(j + 1), (j + 1) % 2)
            fill(tile_at(j), j % 2, sub_ids + j * TILE == lane_ids if j < tiles else None)
        if not flat:
            lower_from_odd()
            lax.fori_loop(tiles, total, step, 0)

    @pl.when(in_first & (mine > 0) & (last > 2))
    def _():
        hear_between()
        send_row(2, last)

    @pl.when(between)
    def _():
        with jax.named_scope("wgo"):
            pl.semaphore_wait(row_ready.at[GO], 1)
        send_row(2, 2 * pair)
        send_row(2 * pair + 2, last)

    @pl.when(mine < n_grp - 1)
    def _():
        with jax.named_scope("ansnext"):
            pl.semaphore_wait(grp_ready.at[NEXT], 1)
        send_grp(mine + 1, mine + 2, slab_part)

    @pl.when(jnp.logical_not(in_last))
    def _():
        with jax.named_scope("wlate"):
            pl.semaphore_wait(row_ready.at[LATE], 2)
        send_row(last, n_row)

    @pl.when(mine < n_grp - 2)
    def _():
        with jax.named_scope("ansrest"):
            pl.semaphore_wait(grp_ready.at[REST], n_grp - 2 - mine)
        send_grp(mine + 2, n_grp, slab_part)

    det_load.wait()
    arrived(olds, load_sem.at[3])

    col_start = pl.multiple_of(mine * cols, cols)
    eye = lax.broadcasted_iota(jnp.int32, (cols, TILE), 0) + col_start == lax.broadcasted_iota(
        jnp.int32, (cols, TILE), 1
    )
    slab_rows = [pos_ref[d : d + 1, :TILE] for d in range(3)]
    own_cols = [
        jnp.sum(jnp.where(eye, jnp.broadcast_to(r, (cols, TILE)), 0.0), axis=1, keepdims=True) for r in slab_rows
    ]
    w_real, w_imag = coupling(own_cols, slab_rows, eye)
    w_real = AMPLITUDE * w_real + jnp.where(eye, det_ref[:, :TILE], 0.0)
    w_imag = AMPLITUDE * w_imag + jnp.where(eye, -0.5, 0.0)
    most = slab - cols
    l_hi, l_lo = split(jnp.concatenate([w_real, w_imag], axis=0)[:, :most])
    for j in range(cols):
        for lead, w in ((0, w_real), (cols, w_imag)):
            coef[j, lead : lead + cols] = jnp.broadcast_to(w[:, most + j : most + j + 1], (cols, width))

    y_local = stage[0 : 2 * cols]
    row_buf[me] = stage[...]
    grp_buf[mine] = y_local

    def left(slab_and_pop):
        signed = jnp.broadcast_to(2.0 * slab_and_pop[2 * cols :] - 1.0, (PAD, width))
        return split(jnp.concatenate([slab_and_pop[: 2 * cols], signed], axis=0))

    main = jnp.zeros((4 * cols + 2 * PAD, 2 * width), jnp.float32)
    rest = jnp.zeros((2 * cols + PAD, 2 * width), jnp.float32)
    group = 2
    for lead in range(0, n_row, group):
        his, los = [], []
        for at, count in ((0, last), (last, 2)):
            if lead == at:
                with jax.named_scope(f"wrow{lead}"):

                    @pl.when(in_last == (at == last))
                    def _():
                        arrived(row_buf.at[0 : count - 1], row_recv.at[at // last])

                    @pl.when(in_last != (at == last))
                    def _():
                        arrived(row_buf.at[0:count], row_recv.at[at // last])

        for p in range(lead, lead + group):
            hi, lo = left(row_buf[p])
            his.append(hi)
            los.append(lo)
        hi = jnp.concatenate(his, axis=1)
        lo = jnp.concatenate(los, axis=1)
        span = slice(lead * width, (lead + group) * width)
        main = main + bdot(jnp.concatenate([hi, lo], axis=0), rhs_hi[span, :])
        rest = rest + bdot(hi, rhs_lo[span, :])
    half = 2 * cols + PAD
    z = AMPLITUDE * (main[:half] + main[half:] + rest)
    z_real = z[:cols, :width] - z[cols : 2 * cols, width:]
    z_imag = z[:cols, width:] + z[cols : 2 * cols, :width]
    shift = z[2 * cols : 2 * cols + 1, :width]

    y_real, y_imag = y_local[:cols], y_local[cols:]
    total_shift = shift + det_ref[:, pl.ds(my_start, width)]
    z_real = z_real + total_shift * y_real + 0.5 * y_imag
    z_imag = z_imag + total_shift * y_imag - 0.5 * y_real

    top = n_grp - 1
    if n_grp > 2:
        with jax.named_scope("wgrp"):

            @pl.when(mine < top)
            def _():
                arrived(grp_buf.at[0 : top - 1], grp_recv.at[0])

            @pl.when(mine == top)
            def _():
                arrived(grp_buf.at[0:top], grp_recv.at[0])

    elif n_grp == 2:

        @pl.when(mine == top)
        def _():
            arrived(grp_buf.at[0:top], grp_recv.at[0])

    blocks = [grp_buf[g] for g in range(top)]
    full = jnp.concatenate(
        [jnp.concatenate([block[:cols], block[cols:]], axis=1) for block in blocks], axis=0
    )
    f_hi, f_lo = split(full)
    v = bdot(l_hi, f_hi) + bdot(l_lo, f_hi) + bdot(l_hi, f_lo)
    z_imag = z_imag - (v[:cols, width:] - v[cols:, :width])
    z_real = z_real - (v[:cols, :width] + v[cols:, width:])

    for i, rate in enumerate((z_imag, -z_real)):
        next_ref[i] = olds[0, i] + 0.5 * TIME_STEP * rate
        accum_ref[i] = olds[1, i] + TIME_STEP / 3.0 * rate

    with jax.named_scope("drain"):
        arrived(row_buf.at[0 : n_row - 1], send_sem.at[0])
        arrived(grp_buf.at[0 : n_grp - 1], send_sem.at[1])


def finish(n_grp, next_ref, accum_ref, grp_buf, coef, grp_recv):
    cols, width = coef.shape[0], coef.shape[2]
    mine, top = lax.axis_index("grp"), n_grp - 1

    with jax.named_scope("wtop"):

        @pl.when(mine < top)
        def _():
            pltpu.make_async_copy(grp_buf.at[0], grp_buf.at[0], grp_recv.at[1]).wait()

    sums = [[jnp.zeros((cols, width), jnp.float32)] * 4 for _ in range(2)]
    for j in range(cols):
        fr = grp_buf[top, j : j + 1]
        fi = grp_buf[top, cols + j : cols + j + 1]
        wr, wi = coef[j, :cols], coef[j, cols:]
        k = 2 * (j % 2)
        sums[0][k] = sums[0][k] + wr * fr
        sums[0][k + 1] = sums[0][k + 1] + wi * fi
        sums[1][k] = sums[1][k] + wr * fi
        sums[1][k + 1] = sums[1][k + 1] + wi * fr
    v_real = (sums[0][0] + sums[0][1]) + (sums[0][2] + sums[0][3])
    v_imag = (sums[1][0] + sums[1][2]) - (sums[1][1] + sums[1][3])
    for i, rate in enumerate((-v_imag, v_real)):
        next_ref[i] = next_ref[i] + 0.5 * TIME_STEP * rate
        accum_ref[i] = accum_ref[i] + TIME_STEP / 3.0 * rate


def kernel(n_row, n_grp, pos_in, det_in, pop_in, sec_in, base_in, accum_in, next_ref, accum_ref, olds, pos_ref, det_ref, stage, wide, rhs_hi, rhs_lo, row_buf, grp_buf, coef):
    def scope(row_recv, grp_recv, row_ready, grp_ready, load_sem, send_sem):
        exchange(n_row=n_row, n_grp=n_grp, pos_in=pos_in, det_in=det_in, pop_in=pop_in, sec_in=sec_in, base_in=base_in, accum_in=accum_in, next_ref=next_ref, accum_ref=accum_ref, olds=olds, pos_ref=pos_ref, det_ref=det_ref, stage=stage, wide=wide, rhs_hi=rhs_hi, rhs_lo=rhs_lo, row_buf=row_buf, grp_buf=grp_buf, coef=coef, row_recv=row_recv, grp_recv=grp_recv, row_ready=row_ready, grp_ready=grp_ready, load_sem=load_sem, send_sem=send_sem)
        finish(n_grp, next_ref, accum_ref, grp_buf, coef, grp_recv)

    pl.run_scoped(
        scope,
        row_recv=pltpu.SemaphoreType.DMA((2,)),
        grp_recv=pltpu.SemaphoreType.DMA((2,)),
        row_ready=pltpu.SemaphoreType.REGULAR((3,)),
        grp_ready=pltpu.SemaphoreType.REGULAR((2,)),
        load_sem=pltpu.SemaphoreType.DMA((4,)),
        send_sem=pltpu.SemaphoreType.DMA((2,)),
    )


def store(next_ref, accum_ref, next_out, accum_out):
    def scope(sem):
        copies = [
            pltpu.make_async_copy(next_ref, next_out, sem.at[0]),
            pltpu.make_async_copy(accum_ref, accum_out, sem.at[1]),
        ]
        for copy in copies:
            copy.start()
        for copy in copies:
            copy.wait()

    pl.run_scoped(scope, pltpu.SemaphoreType.DMA((2,)))


def local(positions, detuning, populations, base, section, accum):
    n_row, n_grp = lax.axis_size("row"), lax.axis_size("grp")
    cols, width = section.shape[1], section.shape[2]
    total = positions.shape[1]
    block = section.shape
    results = pl.pallas_call(
        functools.partial(kernel, n_row, n_grp),
        out_shape=(pltpu.VMEM(block, jnp.float32), pltpu.VMEM(block, jnp.float32)),
        in_specs=[pl.BlockSpec(memory_space=pl.ANY)] * 6,
        out_specs=(pl.BlockSpec(memory_space=pltpu.VMEM), pl.BlockSpec(memory_space=pltpu.VMEM)),
        scratch_shapes=[
            pltpu.VMEM((2, *block), jnp.float32),
            pltpu.VMEM((3, total), jnp.float32),
            pltpu.VMEM((1, total), jnp.float32),
            pltpu.VMEM((2 * cols + 1, width), jnp.float32),
            pltpu.VMEM((2, 3, TILE, TILE), jnp.float32),
            pltpu.VMEM((total, 2 * width), jnp.bfloat16),
            pltpu.VMEM((total, 2 * width), jnp.bfloat16),
            pltpu.VMEM((n_row, 2 * cols + 1, width), jnp.float32),
            pltpu.VMEM((n_grp, 2 * cols, width), jnp.float32),
            pltpu.VMEM((cols, 2 * cols, width), jnp.float32),
        ],
        compiler_params=pltpu.CompilerParams(collective_id=0, has_side_effects=True),
    )(positions, detuning.reshape(1, total), populations.reshape(1, width), section.reshape(2 * cols, width), base, accum)
    return pl.pallas_call(
        store,
        out_shape=(jax.ShapeDtypeStruct(block, jnp.float32),) * 2,
        in_specs=[pl.BlockSpec(memory_space=pltpu.VMEM)] * 2,
        out_specs=(pl.BlockSpec(memory_space=pltpu.HBM),) * 2,
    )(*[pltpu.with_memory_space_constraint(r, pltpu.VMEM) for r in results])


def solution(mesh):
    return jax.shard_map(
        local,
        mesh=mesh,
        in_specs=(
            P(),
            P(),
            P("row"),
            P(None, "grp", "row"),
            P(None, "grp", "row"),
            P(None, "grp", "row"),
        ),
        out_specs=(P(None, "grp", "row"), P(None, "grp", "row")),
        check_vma=False,
    )
```

```python
import functools
import math

import jax
import jax.numpy as jnp
from jax import lax
from jax.experimental import pallas as pl
from jax.experimental.pallas import tpu as pltpu
from jax.sharding import PartitionSpec as P

TIME_STEP = 0.2
PAD = 16
TILE = 128
AMPLITUDE = -0.75
PAUSE = 1

HALF_SIN = (4.442882834149929, -7.308241154546326, 3.606288958225646, -0.8457635961475002, 0.10920575363724722)
HALF_COS = (1.4142134965650124, -6.97885098823893, 5.739461170681154, -1.8835629872981716, 0.31069819180355424)
MESH = pl.DeviceIdType.MESH


def horner(coeffs, t):
    total = coeffs[-1] * t + coeffs[-2]
    for value in coeffs[-3::-1]:
        total = total * t + value
    return total


def coupling(cols, rows, diag):
    dx = cols[0] - rows[0]
    dy = cols[1] - rows[1]
    dz = cols[2] - rows[2]
    dz_sq = dz * dz
    dist_sq = dx * dx + dy * dy + dz_sq
    if diag is not None:
        dist_sq = jnp.where(diag, 1.0, dist_sq)
    inv = lax.rsqrt(dist_sq)
    dist = dist_sq * inv
    frac = dist - jnp.round(dist)
    t = frac * frac
    half_sin = frac * horner(HALF_SIN, t)
    half_cos = horner(HALF_COS, t)
    sine = half_sin * half_cos
    cosine = 1.0 - half_sin * half_sin
    u = inv * (0.5 / math.pi)
    aligned = dz_sq * (inv * inv)
    amp_imag = (u * u) * (1.0 - 3.0 * aligned)
    amp_real = u * ((1.0 - aligned) - amp_imag)
    h_real = amp_real * cosine - amp_imag * sine
    h_imag = amp_real * sine + amp_imag * cosine
    if diag is not None:
        h_real = jnp.where(diag, 0.0, h_real)
        h_imag = jnp.where(diag, 0.0, h_imag)
    return h_real, h_imag


def split(x):
    hi = x.astype(jnp.bfloat16)
    return hi, (x - hi.astype(jnp.float32)).astype(jnp.bfloat16)


def bdot(a, b):
    return jnp.dot(a, b, preferred_element_type=jnp.float32)


def exchange(
    n_row,
    n_grp,
    pos_in,
    det_in,
    pop_in,
    sec_in,
    base_in,
    accum_in,
    next_ref,
    accum_ref,
    olds,
    pos_ref,
    det_ref,
    stage,
    wide,
    rhs_hi,
    rhs_lo,
    row_buf,
    grp_buf,
    coef,
    send_sem,
    row_recv,
    grp_recv,
    row_ready,
    grp_ready,
    load_sem,
):
    cols, width = sec_in.shape[0] // 2, sec_in.shape[1]
    me = lax.axis_index("row")
    mine = lax.axis_index("grp")
    slab = cols * n_grp
    barrier = pltpu.get_barrier_semaphore()

    last = n_row - 2
    pair = me // 2
    odd = lax.rem(me, 2)
    partner = me + 1 - 2 * odd
    in_first = me < 2
    in_last = me >= last
    between = jnp.logical_not(in_first | in_last)
    even = odd == 0
    low = jnp.minimum(mine, 1)
    ahead = in_first & even & (mine > 0)
    GO, LATE, WORD = 0, 1, 2
    NEXT, REST = 0, 1

    def to_row(sem, lo, hi):
        def body(p, carry):
            pl.semaphore_signal(sem, inc=1, device_id={"row": p}, device_id_type=MESH)
            return carry

        lax.fori_loop(lo, hi, body, 0)

    def to_grp(sem, lo, hi):
        def body(p, carry):
            pl.semaphore_signal(sem, inc=1, device_id={"grp": p}, device_id_type=MESH)
            return carry

        lax.fori_loop(lo, hi, body, 0)

    slab_part = stage.at[0 : 2 * cols]

    def send_row(lo, hi):
        def body(p, carry):
            pltpu.make_async_remote_copy(
                stage,
                row_buf.at[me],
                send_sem.at[0],
                row_recv.at[pair],
                device_id={"row": p},
                device_id_type=MESH,
            ).start()
            return carry

        lax.fori_loop(lo, hi, body, 0)

    def send_grp(lo, hi, source):
        def body(p, carry):
            pltpu.make_async_remote_copy(
                source,
                grp_buf.at[mine],
                send_sem.at[1],
                grp_recv.at[jnp.where(mine < n_grp - 1, 0, 1)],
                device_id={"grp": p},
                device_id_type=MESH,
            ).start()
            return carry

        lax.fori_loop(lo, hi, body, 0)

    def arrived(part, sem):
        pltpu.make_async_copy(part, part, sem).wait()

    @pl.when(ahead)
    def _():
        pl.semaphore_wait(barrier, 1)
        send_grp(0, 1, sec_in)

    section_loads = [
        pltpu.make_async_copy(src, dst, load_sem.at[0])
        for src, dst in (
            (sec_in, stage.at[0 : 2 * cols]),
            (pop_in, stage.at[2 * cols : 2 * cols + 1]),
        )
    ]
    pos_load = pltpu.make_async_copy(pos_in, pos_ref, load_sem.at[1])
    det_load = pltpu.make_async_copy(det_in, det_ref, load_sem.at[2])
    old_loads = [
        pltpu.make_async_copy(src, olds.at[i], load_sem.at[3]) for i, src in enumerate((base_in, accum_in))
    ]
    for load in (*section_loads, pos_load, det_load, *old_loads):
        load.start()

    @pl.when(even & (mine > 0))
    def _():
        def body(p, carry):
            pl.semaphore_signal(barrier, inc=1, device_id={"row": partner, "grp": p}, device_id_type=MESH)
            return carry

        lax.fori_loop(mine + 1, n_grp, body, 0)

    @pl.when(jnp.logical_not(even & (mine > 0)))
    def _():
        to_grp(barrier, mine + 1, n_grp)

    @pl.when(even)
    def _():
        pl.semaphore_signal(barrier, inc=1, device_id={"row": partner}, device_id_type=MESH)

    after = jnp.where(in_first, 2, jnp.where(in_last, n_row, last))
    to_row(barrier, after, n_row)

    before = jnp.where(in_first, 0, jnp.where(in_last, last, 2))
    met = before + jnp.where(even, low, 1 + mine + mine - low)

    @pl.when((met > 0) & jnp.logical_not(ahead))
    def _():
        pl.semaphore_wait(barrier, met)

    send_grp(0, jnp.where(even & jnp.logical_not(ahead), low, 0), sec_in)

    def answer_lower(lo, hi):
        to_grp(grp_ready.at[REST], lo, jnp.minimum(hi, mine - 1))
        to_grp(grp_ready.at[NEXT], jnp.maximum(lo, mine - 1), hi)

    answer_lower(0, low)

    @pl.when(between)
    def _():
        to_row(row_ready.at[GO], 0, 2)

    @pl.when(in_last)
    def _():
        to_row(row_ready.at[LATE], 0, last)

    @pl.when(jnp.logical_not(even))
    def _():
        pl.semaphore_signal(row_ready.at[WORD], inc=1, device_id={"row": partner}, device_id_type=MESH)
        answer_lower(low, mine)

    def hear_between():
        pl.semaphore_wait(row_ready.at[GO], last - 2)

        @pl.when(odd == 1)
        def _():
            to_row(row_ready.at[GO], 2, last)

    @pl.when(in_first & (mine == 0) & (last > 2))
    def _():
        hear_between()

    pos_load.wait()
    arrived(stage, load_sem.at[0])
    send_row(jnp.where(in_first, 2, 0), jnp.where(in_first, jnp.where(mine == 0, last, 2), before))

    @pl.when(even)
    def _():
        pl.semaphore_wait(row_ready.at[WORD], 1)
        answer_lower(low, mine)
        send_grp(low, mine, slab_part)

    send_row(partner, partner + 1)

    my_start = pl.multiple_of(me * width, width)
    rows = [pos_ref[d : d + 1, pl.ds(my_start, width)] for d in range(3)]
    tiles = width // TILE

    def spread(tile, slot):
        start = pl.multiple_of(tile * TILE, TILE)
        for d in range(3):
            line = pos_ref[d : d + 1, pl.ds(start, TILE)]
            wide[slot, d] = jnp.transpose(jnp.broadcast_to(line, (TILE, TILE)))

    def fill(tile, slot, diag):
        start = pl.multiple_of(tile * TILE, TILE)
        for part in range(tiles):
            lanes = slice(part * TILE, (part + 1) * TILE)
            h_real, h_imag = coupling(
                [wide[slot, d] for d in range(3)],
                [r[:, lanes] for r in rows],
                None if diag is None else diag[:, lanes],
            )
            for base, h in ((0, h_real), (width, h_imag)):
                hi, lo = split(h)
                at = slice(base + part * TILE, base + (part + 1) * TILE)
                rhs_hi[pl.ds(start, TILE), at] = hi
                rhs_lo[pl.ds(start, TILE), at] = lo

    first = me * tiles
    total = n_row * tiles
    lane_ids = lax.broadcasted_iota(jnp.int32, (TILE, width), 1)
    sub_ids = lax.broadcasted_iota(jnp.int32, (TILE, width), 0)

    def tile_at(j):
        return lax.rem(first + j, total)

    def lower_from_odd():
        @pl.when(jnp.logical_not(even))
        def _():
            send_grp(0, mine, slab_part)

    def step(j, carry):
        spread(tile_at(j + 1), lax.rem(j + 1, 2))
        fill(tile_at(j), lax.rem(j, 2), None)
        return carry

    flat = total <= 16
    spread(first, 0)
    for j in range(total if flat else tiles):
        if j == tiles + PAUSE:
            lower_from_odd()
        if j + 1 < total:
            spread(tile_at(j + 1), (j + 1) % 2)
        fill(tile_at(j), j % 2, sub_ids + j * TILE == lane_ids if j < tiles else None)
    if not flat:
        lower_from_odd()
        lax.fori_loop(tiles, total, step, 0)

    @pl.when(in_first & (mine > 0) & (last > 2))
    def _():
        hear_between()
        send_row(2, last)

    @pl.when(between)
    def _():
        pl.semaphore_wait(row_ready.at[GO], 1)
        send_row(2, 2 * pair)
        send_row(2 * pair + 2, last)

    @pl.when(mine < n_grp - 1)
    def _():
        pl.semaphore_wait(grp_ready.at[NEXT], 1)
        send_grp(mine + 1, mine + 2, slab_part)

    @pl.when(jnp.logical_not(in_last))
    def _():
        pl.semaphore_wait(row_ready.at[LATE], 2)
        send_row(last, n_row)

    @pl.when(mine < n_grp - 2)
    def _():
        pl.semaphore_wait(grp_ready.at[REST], n_grp - 2 - mine)
        send_grp(mine + 2, n_grp, slab_part)

    det_load.wait()
    arrived(olds, load_sem.at[3])

    col_start = pl.multiple_of(mine * cols, cols)
    eye = lax.broadcasted_iota(jnp.int32, (cols, TILE), 0) + col_start == lax.broadcasted_iota(
        jnp.int32, (cols, TILE), 1
    )
    slab_rows = [pos_ref[d : d + 1, :TILE] for d in range(3)]
    own_cols = [
        jnp.sum(jnp.where(eye, jnp.broadcast_to(r, (cols, TILE)), 0.0), axis=1, keepdims=True) for r in slab_rows
    ]
    w_real, w_imag = coupling(own_cols, slab_rows, eye)
    w_real = AMPLITUDE * w_real + jnp.where(eye, det_ref[:, :TILE], 0.0)
    w_imag = AMPLITUDE * w_imag + jnp.where(eye, -0.5, 0.0)
    most = slab - cols
    l_hi, l_lo = split(jnp.concatenate([w_real, w_imag], axis=0)[:, :most])
    for j in range(cols):
        for lead, w in ((0, w_real), (cols, w_imag)):
            coef[j, lead : lead + cols] = jnp.broadcast_to(w[:, most + j : most + j + 1], (cols, width))

    y_local = stage[0 : 2 * cols]
    row_buf[me] = stage[...]
    grp_buf[mine] = y_local

    def left(slab_and_pop):
        signed = jnp.broadcast_to(2.0 * slab_and_pop[2 * cols :] - 1.0, (PAD, width))
        return split(jnp.concatenate([slab_and_pop[: 2 * cols], signed], axis=0))

    main = jnp.zeros((4 * cols + 2 * PAD, 2 * width), jnp.float32)
    rest = jnp.zeros((2 * cols + PAD, 2 * width), jnp.float32)
    group = 2
    for lead in range(0, n_row, group):
        his, los = [], []

        @pl.when(pair == lead // group)
        def _():
            arrived(row_buf.at[0], row_recv.at[lead // group])

        @pl.when(pair != lead // group)
        def _():
            arrived(row_buf.at[0:group], row_recv.at[lead // group])

        for p in range(lead, lead + group):
            hi, lo = left(row_buf[p])
            his.append(hi)
            los.append(lo)
        hi = jnp.concatenate(his, axis=1)
        lo = jnp.concatenate(los, axis=1)
        span = slice(lead * width, (lead + group) * width)
        main = main + bdot(jnp.concatenate([hi, lo], axis=0), rhs_hi[span, :])
        rest = rest + bdot(hi, rhs_lo[span, :])
    half = 2 * cols + PAD
    z = AMPLITUDE * (main[:half] + main[half:] + rest)
    z_real = z[:cols, :width] - z[cols : 2 * cols, width:]
    z_imag = z[:cols, width:] + z[cols : 2 * cols, :width]
    shift = z[2 * cols : 2 * cols + 1, :width]

    y_real, y_imag = y_local[:cols], y_local[cols:]
    total_shift = shift + det_ref[:, pl.ds(my_start, width)]
    z_real = z_real + total_shift * y_real + 0.5 * y_imag
    z_imag = z_imag + total_shift * y_imag - 0.5 * y_real

    top = n_grp - 1
    if n_grp > 2:

        @pl.when(mine < top)
        def _():
            arrived(grp_buf.at[0 : top - 1], grp_recv.at[0])

        @pl.when(mine == top)
        def _():
            arrived(grp_buf.at[0:top], grp_recv.at[0])

    elif n_grp == 2:

        @pl.when(mine == top)
        def _():
            arrived(grp_buf.at[0:top], grp_recv.at[0])

    blocks = [grp_buf[g] for g in range(top)]
    full = jnp.concatenate(
        [jnp.concatenate([block[:cols], block[cols:]], axis=1) for block in blocks], axis=0
    )
    f_hi, f_lo = split(full)
    v = bdot(l_hi, f_hi) + bdot(l_lo, f_hi) + bdot(l_hi, f_lo)
    z_imag = z_imag - (v[:cols, width:] - v[cols:, :width])
    z_real = z_real - (v[:cols, :width] + v[cols:, width:])

    for i, rate in enumerate((z_imag, -z_real)):
        next_ref[i] = olds[0, i] + 0.5 * TIME_STEP * rate
        accum_ref[i] = olds[1, i] + TIME_STEP / 3.0 * rate

    arrived(row_buf.at[0 : n_row - 1], send_sem.at[0])
    arrived(grp_buf.at[0 : n_grp - 1], send_sem.at[1])


    @pl.when(mine < top)
    def _():
        arrived(grp_buf.at[0], grp_recv.at[1])

    sums = [[jnp.zeros((cols, width), jnp.float32)] * 4 for _ in range(2)]
    for j in range(cols):
        fr = grp_buf[top, j : j + 1]
        fi = grp_buf[top, cols + j : cols + j + 1]
        wr, wi = coef[j, :cols], coef[j, cols:]
        k = 2 * (j % 2)
        sums[0][k] = sums[0][k] + wr * fr
        sums[0][k + 1] = sums[0][k + 1] + wi * fi
        sums[1][k] = sums[1][k] + wr * fi
        sums[1][k + 1] = sums[1][k + 1] + wi * fr
    v_real = (sums[0][0] + sums[0][1]) + (sums[0][2] + sums[0][3])
    v_imag = (sums[1][0] + sums[1][2]) - (sums[1][1] + sums[1][3])
    for i, rate in enumerate((-v_imag, v_real)):
        next_ref[i] = next_ref[i] + 0.5 * TIME_STEP * rate
        accum_ref[i] = accum_ref[i] + TIME_STEP / 3.0 * rate


def kernel(n_row, n_grp, *refs):
    pl.run_scoped(
        functools.partial(exchange, n_row, n_grp, *refs),
        send_sem=pltpu.SemaphoreType.DMA((2,)),
        row_recv=pltpu.SemaphoreType.DMA((n_row // 2,)),
        grp_recv=pltpu.SemaphoreType.DMA((2,)),
        row_ready=pltpu.SemaphoreType.REGULAR((3,)),
        grp_ready=pltpu.SemaphoreType.REGULAR((2,)),
        load_sem=pltpu.SemaphoreType.DMA((4,)),
    )


def store(next_ref, accum_ref, next_out, accum_out):
    def scope(sem):
        copies = [
            pltpu.make_async_copy(next_ref, next_out, sem.at[0]),
            pltpu.make_async_copy(accum_ref, accum_out, sem.at[1]),
        ]
        for copy in copies:
            copy.start()
        for copy in copies:
            copy.wait()

    pl.run_scoped(scope, pltpu.SemaphoreType.DMA((2,)))


def local(positions, detuning, populations, base, section, accum):
    n_row, n_grp = lax.axis_size("row"), lax.axis_size("grp")
    cols, width = section.shape[1], section.shape[2]
    total = positions.shape[1]
    block = section.shape
    results = pl.pallas_call(
        functools.partial(kernel, n_row, n_grp),
        out_shape=(pltpu.VMEM(block, jnp.float32), pltpu.VMEM(block, jnp.float32)),
        in_specs=[pl.BlockSpec(memory_space=pl.ANY)] * 6,
        out_specs=(pl.BlockSpec(memory_space=pltpu.VMEM), pl.BlockSpec(memory_space=pltpu.VMEM)),
        scratch_shapes=[
            pltpu.VMEM((2, *block), jnp.float32),
            pltpu.VMEM((3, total), jnp.float32),
            pltpu.VMEM((1, total), jnp.float32),
            pltpu.VMEM((2 * cols + 1, width), jnp.float32),
            pltpu.VMEM((2, 3, TILE, TILE), jnp.float32),
            pltpu.VMEM((total, 2 * width), jnp.bfloat16),
            pltpu.VMEM((total, 2 * width), jnp.bfloat16),
            pltpu.VMEM((n_row, 2 * cols + 1, width), jnp.float32),
            pltpu.VMEM((n_grp, 2 * cols, width), jnp.float32),
            pltpu.VMEM((cols, 2 * cols, width), jnp.float32),
        ],
        compiler_params=pltpu.CompilerParams(collective_id=0, has_side_effects=True),
    )(positions, detuning.reshape(1, total), populations.reshape(1, width), section.reshape(2 * cols, width), base, accum)
    return pl.pallas_call(
        store,
        out_shape=(jax.ShapeDtypeStruct(block, jnp.float32),) * 2,
        in_specs=[pl.BlockSpec(memory_space=pltpu.VMEM)] * 2,
        out_specs=(pl.BlockSpec(memory_space=pltpu.HBM),) * 2,
    )(*[pltpu.with_memory_space_constraint(r, pltpu.VMEM) for r in results])


def solution(mesh):
    return jax.shard_map(
        local,
        mesh=mesh,
        in_specs=(
            P(),
            P(),
            P("row"),
            P(None, "grp", "row"),
            P(None, "grp", "row"),
            P(None, "grp", "row"),
        ),
        out_specs=(P(None, "grp", "row"), P(None, "grp", "row")),
        check_vma=False,
    )
```

```python
import functools
import math

import jax
import jax.numpy as jnp
from jax import lax
from jax.experimental import pallas as pl
from jax.experimental.pallas import tpu as pltpu
from jax.sharding import PartitionSpec as P

TIME_STEP = 0.2
PAD = 16
TILE = 128
AMPLITUDE = -0.75
PAUSE = 1

HALF_SIN = (4.442882834149929, -7.308241154546326, 3.606288958225646, -0.8457635961475002, 0.10920575363724722)
HALF_COS = (1.4142134965650124, -6.97885098823893, 5.739461170681154, -1.8835629872981716, 0.31069819180355424)
MESH = pl.DeviceIdType.MESH


def horner(coeffs, t):
    total = coeffs[-1] * t + coeffs[-2]
    for value in coeffs[-3::-1]:
        total = total * t + value
    return total


def coupling(cols, rows, diag):
    dx = cols[0] - rows[0]
    dy = cols[1] - rows[1]
    dz = cols[2] - rows[2]
    dz_sq = dz * dz
    dist_sq = dx * dx + dy * dy + dz_sq
    if diag is not None:
        dist_sq = jnp.where(diag, 1.0, dist_sq)
    inv = lax.rsqrt(dist_sq)
    dist = dist_sq * inv
    frac = dist - jnp.round(dist)
    t = frac * frac
    half_sin = frac * horner(HALF_SIN, t)
    half_cos = horner(HALF_COS, t)
    sine = half_sin * half_cos
    cosine = 1.0 - half_sin * half_sin
    u = inv * (0.5 / math.pi)
    aligned = dz_sq * (inv * inv)
    amp_imag = (u * u) * (1.0 - 3.0 * aligned)
    amp_real = u * ((1.0 - aligned) - amp_imag)
    h_real = amp_real * cosine - amp_imag * sine
    h_imag = amp_real * sine + amp_imag * cosine
    if diag is not None:
        h_real = jnp.where(diag, 0.0, h_real)
        h_imag = jnp.where(diag, 0.0, h_imag)
    return h_real, h_imag


def split(x):
    hi = x.astype(jnp.bfloat16)
    return hi, (x - hi.astype(jnp.float32)).astype(jnp.bfloat16)


def bdot(a, b):
    return jnp.dot(a, b, preferred_element_type=jnp.float32)


def exchange(
    n_row,
    n_grp,
    pos_in,
    det_in,
    pop_in,
    sec_in,
    base_in,
    accum_in,
    next_ref,
    accum_ref,
    olds,
    pos_ref,
    det_ref,
    stage,
    wide,
    rhs_hi,
    rhs_lo,
    row_buf,
    grp_buf,
    coef,
    send_sem,
    row_recv,
    grp_recv,
    row_ready,
    grp_ready,
    load_sem,
):
    cols, width = sec_in.shape[0] // 2, sec_in.shape[1]
    me = lax.axis_index("row")
    mine = lax.axis_index("grp")
    slab = cols * n_grp
    barrier = pltpu.get_barrier_semaphore()

    def grp_copy(p, source):
        return pltpu.make_async_remote_copy(
            source,
            grp_buf.at[mine],
            send_sem.at[1],
            grp_recv.at[jnp.where(mine < n_grp - 1, 0, 1)],
            device_id={"grp": p},
            device_id_type=MESH,
        )

    ahead = (me == 0) & (mine > 0)

    @pl.when(ahead)
    def _():
        pl.semaphore_wait(barrier, 1)
        grp_copy(0, sec_in).start()

    last = n_row - 2
    pair = me // 2
    odd = lax.rem(me, 2)
    partner = me + 1 - 2 * odd
    in_first = me < 2
    in_last = me >= last
    between = jnp.logical_not(in_first | in_last)
    even = odd == 0
    low = jnp.minimum(mine, 1)
    GO, LATE, WORD = 0, 1, 2
    NEXT, REST = 0, 1

    def to_row(sem, lo, hi):
        def body(p, carry):
            pl.semaphore_signal(sem, inc=1, device_id={"row": p}, device_id_type=MESH)
            return carry

        lax.fori_loop(lo, hi, body, 0)

    def to_grp(sem, lo, hi):
        def body(p, carry):
            pl.semaphore_signal(sem, inc=1, device_id={"grp": p}, device_id_type=MESH)
            return carry

        lax.fori_loop(lo, hi, body, 0)

    slab_part = stage.at[0 : 2 * cols]

    def send_row(lo, hi):
        def body(p, carry):
            pltpu.make_async_remote_copy(
                stage,
                row_buf.at[me],
                send_sem.at[0],
                row_recv.at[pair],
                device_id={"row": p},
                device_id_type=MESH,
            ).start()
            return carry

        lax.fori_loop(lo, hi, body, 0)

    def send_grp(lo, hi, source):
        def body(p, carry):
            grp_copy(p, source).start()
            return carry

        lax.fori_loop(lo, hi, body, 0)

    def arrived(part, sem):
        pltpu.make_async_copy(part, part, sem).wait()

    section_loads = [
        pltpu.make_async_copy(src, dst, load_sem.at[0])
        for src, dst in (
            (sec_in, stage.at[0 : 2 * cols]),
            (pop_in, stage.at[2 * cols : 2 * cols + 1]),
        )
    ]
    pos_load = pltpu.make_async_copy(pos_in, pos_ref, load_sem.at[1])
    det_load = pltpu.make_async_copy(det_in, det_ref, load_sem.at[2])
    old_loads = [
        pltpu.make_async_copy(src, olds.at[i], load_sem.at[3]) for i, src in enumerate((base_in, accum_in))
    ]
    for load in (*section_loads, pos_load, det_load, *old_loads):
        load.start()

    @pl.when(even & (mine > 0))
    def _():
        def body(p, carry):
            pl.semaphore_signal(barrier, inc=1, device_id={"row": partner, "grp": p}, device_id_type=MESH)
            return carry

        lax.fori_loop(mine + 1, n_grp, body, 0)

    @pl.when(jnp.logical_not(even & (mine > 0)))
    def _():
        to_grp(barrier, mine + 1, n_grp)

    @pl.when(even)
    def _():
        pl.semaphore_signal(barrier, inc=1, device_id={"row": partner}, device_id_type=MESH)

    after = jnp.where(in_first, 2, jnp.where(in_last, n_row, last))
    to_row(barrier, after, n_row)

    before = jnp.where(in_first, 0, jnp.where(in_last, last, 2))
    met = before + jnp.where(even, low, 1 + mine + mine - low)

    @pl.when((met > 0) & jnp.logical_not(ahead))
    def _():
        pl.semaphore_wait(barrier, met)

    send_grp(0, jnp.where(even & jnp.logical_not(ahead), low, 0), sec_in)

    def answer_lower(lo, hi):
        to_grp(grp_ready.at[REST], lo, jnp.minimum(hi, mine - 1))
        to_grp(grp_ready.at[NEXT], jnp.maximum(lo, mine - 1), hi)

    answer_lower(0, low)

    @pl.when(between)
    def _():
        to_row(row_ready.at[GO], 0, 2)

    @pl.when(in_last)
    def _():
        to_row(row_ready.at[LATE], 0, last)

    @pl.when(jnp.logical_not(even))
    def _():
        pl.semaphore_signal(row_ready.at[WORD], inc=1, device_id={"row": partner}, device_id_type=MESH)
        answer_lower(low, mine)

    def hear_between():
        pl.semaphore_wait(row_ready.at[GO], last - 2)

        @pl.when(odd == 1)
        def _():
            to_row(row_ready.at[GO], 2, last)

    @pl.when(in_first & (mine == 0) & (last > 2))
    def _():
        hear_between()

    pos_load.wait()
    arrived(stage, load_sem.at[0])
    send_row(jnp.where(in_first, 2, 0), jnp.where(in_first, jnp.where(mine == 0, last, 2), before))

    @pl.when(even)
    def _():
        pl.semaphore_wait(row_ready.at[WORD], 1)
        answer_lower(low, mine)
        send_grp(low, mine, slab_part)

    send_row(partner, partner + 1)

    my_start = pl.multiple_of(me * width, width)
    rows = [pos_ref[d : d + 1, pl.ds(my_start, width)] for d in range(3)]
    tiles = width // TILE

    def spread(tile, slot):
        start = pl.multiple_of(tile * TILE, TILE)
        for d in range(3):
            line = pos_ref[d : d + 1, pl.ds(start, TILE)]
            wide[slot, d] = jnp.transpose(jnp.broadcast_to(line, (TILE, TILE)))

    def fill(tile, slot, diag):
        start = pl.multiple_of(tile * TILE, TILE)
        for part in range(tiles):
            lanes = slice(part * TILE, (part + 1) * TILE)
            h_real, h_imag = coupling(
                [wide[slot, d] for d in range(3)],
                [r[:, lanes] for r in rows],
                None if diag is None else diag[:, lanes],
            )
            for base, h in ((0, h_real), (width, h_imag)):
                hi, lo = split(h)
                at = slice(base + part * TILE, base + (part + 1) * TILE)
                rhs_hi[pl.ds(start, TILE), at] = hi
                rhs_lo[pl.ds(start, TILE), at] = lo

    first = me * tiles
    total = n_row * tiles
    lane_ids = lax.broadcasted_iota(jnp.int32, (TILE, width), 1)
    sub_ids = lax.broadcasted_iota(jnp.int32, (TILE, width), 0)

    def tile_at(j):
        return lax.rem(first + j, total)

    def lower_from_odd():
        @pl.when(jnp.logical_not(even))
        def _():
            send_grp(0, mine, slab_part)

    def step(j, carry):
        spread(tile_at(j + 1), lax.rem(j + 1, 2))
        fill(tile_at(j), lax.rem(j, 2), None)
        return carry

    flat = total <= 16
    spread(first, 0)
    for j in range(total if flat else tiles):
        if j == tiles + PAUSE:
            lower_from_odd()
        if j + 1 < total:
            spread(tile_at(j + 1), (j + 1) % 2)
        fill(tile_at(j), j % 2, sub_ids + j * TILE == lane_ids if j < tiles else None)
    if not flat:
        lower_from_odd()
        lax.fori_loop(tiles, total, step, 0)

    @pl.when(in_first & (mine > 0) & (last > 2))
    def _():
        hear_between()
        send_row(2, last)

    @pl.when(between)
    def _():
        pl.semaphore_wait(row_ready.at[GO], 1)
        send_row(2, 2 * pair)
        send_row(2 * pair + 2, last)

    @pl.when(mine < n_grp - 1)
    def _():
        pl.semaphore_wait(grp_ready.at[NEXT], 1)
        send_grp(mine + 1, mine + 2, slab_part)

    @pl.when(jnp.logical_not(in_last))
    def _():
        pl.semaphore_wait(row_ready.at[LATE], 2)
        send_row(last, n_row)

    @pl.when(mine < n_grp - 2)
    def _():
        pl.semaphore_wait(grp_ready.at[REST], n_grp - 2 - mine)
        send_grp(mine + 2, n_grp, slab_part)

    det_load.wait()
    arrived(olds, load_sem.at[3])

    col_start = pl.multiple_of(mine * cols, cols)
    eye = lax.broadcasted_iota(jnp.int32, (cols, TILE), 0) + col_start == lax.broadcasted_iota(
        jnp.int32, (cols, TILE), 1
    )
    slab_rows = [pos_ref[d : d + 1, :TILE] for d in range(3)]
    own_cols = [
        jnp.sum(jnp.where(eye, jnp.broadcast_to(r, (cols, TILE)), 0.0), axis=1, keepdims=True) for r in slab_rows
    ]
    w_real, w_imag = coupling(own_cols, slab_rows, eye)
    w_real = AMPLITUDE * w_real + jnp.where(eye, det_ref[:, :TILE], 0.0)
    w_imag = AMPLITUDE * w_imag + jnp.where(eye, -0.5, 0.0)
    most = slab - cols
    l_hi, l_lo = split(jnp.concatenate([w_real, w_imag], axis=0)[:, :most])
    for j in range(cols):
        for lead, w in ((0, w_real), (cols, w_imag)):
            coef[j, lead : lead + cols] = jnp.broadcast_to(w[:, most + j : most + j + 1], (cols, width))

    y_local = stage[0 : 2 * cols]
    row_buf[me] = stage[...]
    grp_buf[mine] = y_local

    def left(slab_and_pop):
        signed = jnp.broadcast_to(2.0 * slab_and_pop[2 * cols :] - 1.0, (PAD, width))
        return split(jnp.concatenate([slab_and_pop[: 2 * cols], signed], axis=0))

    main = jnp.zeros((4 * cols + 2 * PAD, 2 * width), jnp.float32)
    rest = jnp.zeros((2 * cols + PAD, 2 * width), jnp.float32)
    group = 2
    for lead in range(0, n_row, group):
        his, los = [], []

        @pl.when(pair == lead // group)
        def _():
            arrived(row_buf.at[0], row_recv.at[lead // group])

        @pl.when(pair != lead // group)
        def _():
            arrived(row_buf.at[0:group], row_recv.at[lead // group])

        for p in range(lead, lead + group):
            hi, lo = left(row_buf[p])
            his.append(hi)
            los.append(lo)
        hi = jnp.concatenate(his, axis=1)
        lo = jnp.concatenate(los, axis=1)
        span = slice(lead * width, (lead + group) * width)
        main = main + bdot(jnp.concatenate([hi, lo], axis=0), rhs_hi[span, :])
        rest = rest + bdot(hi, rhs_lo[span, :])
    half = 2 * cols + PAD
    z = AMPLITUDE * (main[:half] + main[half:] + rest)
    z_real = z[:cols, :width] - z[cols : 2 * cols, width:]
    z_imag = z[:cols, width:] + z[cols : 2 * cols, :width]
    shift = z[2 * cols : 2 * cols + 1, :width]

    y_real, y_imag = y_local[:cols], y_local[cols:]
    total_shift = shift + det_ref[:, pl.ds(my_start, width)]
    z_real = z_real + total_shift * y_real + 0.5 * y_imag
    z_imag = z_imag + total_shift * y_imag - 0.5 * y_real

    top = n_grp - 1
    if n_grp > 2:

        @pl.when(mine < top)
        def _():
            arrived(grp_buf.at[0 : top - 1], grp_recv.at[0])

        @pl.when(mine == top)
        def _():
            arrived(grp_buf.at[0:top], grp_recv.at[0])

    elif n_grp == 2:

        @pl.when(mine == top)
        def _():
            arrived(grp_buf.at[0:top], grp_recv.at[0])

    blocks = [grp_buf[g] for g in range(top)]
    full = jnp.concatenate(
        [jnp.concatenate([block[:cols], block[cols:]], axis=1) for block in blocks], axis=0
    )
    f_hi, f_lo = split(full)
    v = bdot(l_hi, f_hi) + bdot(l_lo, f_hi) + bdot(l_hi, f_lo)
    z_imag = z_imag - (v[:cols, width:] - v[cols:, :width])
    z_real = z_real - (v[:cols, :width] + v[cols:, width:])

    for i, rate in enumerate((z_imag, -z_real)):
        next_ref[i] = olds[0, i] + 0.5 * TIME_STEP * rate
        accum_ref[i] = olds[1, i] + TIME_STEP / 3.0 * rate

    arrived(row_buf.at[0 : n_row - 1], send_sem.at[0])
    arrived(grp_buf.at[0 : n_grp - 1], send_sem.at[1])


    @pl.when(mine < top)
    def _():
        arrived(grp_buf.at[0], grp_recv.at[1])

    sums = [[jnp.zeros((cols, width), jnp.float32)] * 4 for _ in range(2)]
    for j in range(cols):
        fr = grp_buf[top, j : j + 1]
        fi = grp_buf[top, cols + j : cols + j + 1]
        wr, wi = coef[j, :cols], coef[j, cols:]
        k = 2 * (j % 2)
        sums[0][k] = sums[0][k] + wr * fr
        sums[0][k + 1] = sums[0][k + 1] + wi * fi
        sums[1][k] = sums[1][k] + wr * fi
        sums[1][k + 1] = sums[1][k + 1] + wi * fr
    v_real = (sums[0][0] + sums[0][1]) + (sums[0][2] + sums[0][3])
    v_imag = (sums[1][0] + sums[1][2]) - (sums[1][1] + sums[1][3])
    for i, rate in enumerate((-v_imag, v_real)):
        next_ref[i] = next_ref[i] + 0.5 * TIME_STEP * rate
        accum_ref[i] = accum_ref[i] + TIME_STEP / 3.0 * rate


def kernel(n_row, n_grp, *refs):
    pl.run_scoped(
        functools.partial(exchange, n_row, n_grp, *refs),
        send_sem=pltpu.SemaphoreType.DMA((2,)),
        row_recv=pltpu.SemaphoreType.DMA((n_row // 2,)),
        grp_recv=pltpu.SemaphoreType.DMA((2,)),
        row_ready=pltpu.SemaphoreType.REGULAR((3,)),
        grp_ready=pltpu.SemaphoreType.REGULAR((2,)),
        load_sem=pltpu.SemaphoreType.DMA((4,)),
    )


def store(next_ref, accum_ref, next_out, accum_out):
    def scope(sem):
        copies = [
            pltpu.make_async_copy(next_ref, next_out, sem.at[0]),
            pltpu.make_async_copy(accum_ref, accum_out, sem.at[1]),
        ]
        for copy in copies:
            copy.start()
        for copy in copies:
            copy.wait()

    pl.run_scoped(scope, pltpu.SemaphoreType.DMA((2,)))


def local(positions, detuning, populations, base, section, accum):
    n_row, n_grp = lax.axis_size("row"), lax.axis_size("grp")
    cols, width = section.shape[1], section.shape[2]
    total = positions.shape[1]
    block = section.shape
    results = pl.pallas_call(
        functools.partial(kernel, n_row, n_grp),
        out_shape=(pltpu.VMEM(block, jnp.float32), pltpu.VMEM(block, jnp.float32)),
        in_specs=[pl.BlockSpec(memory_space=pl.ANY)] * 6,
        out_specs=(pl.BlockSpec(memory_space=pltpu.VMEM), pl.BlockSpec(memory_space=pltpu.VMEM)),
        scratch_shapes=[
            pltpu.VMEM((2, *block), jnp.float32),
            pltpu.VMEM((3, total), jnp.float32),
            pltpu.VMEM((1, total), jnp.float32),
            pltpu.VMEM((2 * cols + 1, width), jnp.float32),
            pltpu.VMEM((2, 3, TILE, TILE), jnp.float32),
            pltpu.VMEM((total, 2 * width), jnp.bfloat16),
            pltpu.VMEM((total, 2 * width), jnp.bfloat16),
            pltpu.VMEM((n_row, 2 * cols + 1, width), jnp.float32),
            pltpu.VMEM((n_grp, 2 * cols, width), jnp.float32),
            pltpu.VMEM((cols, 2 * cols, width), jnp.float32),
        ],
        compiler_params=pltpu.CompilerParams(collective_id=0, has_side_effects=True),
    )(positions, detuning.reshape(1, total), populations.reshape(1, width), section.reshape(2 * cols, width), base, accum)
    return pl.pallas_call(
        store,
        out_shape=(jax.ShapeDtypeStruct(block, jnp.float32),) * 2,
        in_specs=[pl.BlockSpec(memory_space=pltpu.VMEM)] * 2,
        out_specs=(pl.BlockSpec(memory_space=pltpu.HBM),) * 2,
    )(*[pltpu.with_memory_space_constraint(r, pltpu.VMEM) for r in results])


def solution(mesh):
    return jax.shard_map(
        local,
        mesh=mesh,
        in_specs=(
            P(),
            P(),
            P("row"),
            P(None, "grp", "row"),
            P(None, "grp", "row"),
            P(None, "grp", "row"),
        ),
        out_specs=(P(None, "grp", "row"), P(None, "grp", "row")),
        check_vma=False,
    )
```

```python
import functools
import math

import jax
import jax.numpy as jnp
from jax import lax
from jax.experimental import pallas as pl
from jax.experimental.pallas import tpu as pltpu
from jax.sharding import PartitionSpec as P

TIME_STEP = 0.2
PAD = 16
TILE = 128
AMPLITUDE = -0.75
PAUSE = 1
PIECES = 4

HALF_SIN = (4.442882834149929, -7.308241154546326, 3.606288958225646, -0.8457635961475002, 0.10920575363724722)
HALF_COS = (1.4142134965650124, -6.97885098823893, 5.739461170681154, -1.8835629872981716, 0.31069819180355424)
MESH = pl.DeviceIdType.MESH


def horner(coeffs, t):
    total = coeffs[-1] * t + coeffs[-2]
    for value in coeffs[-3::-1]:
        total = total * t + value
    return total


def coupling(cols, rows, diag):
    dx = cols[0] - rows[0]
    dy = cols[1] - rows[1]
    dz = cols[2] - rows[2]
    dz_sq = dz * dz
    dist_sq = dx * dx + dy * dy + dz_sq
    if diag is not None:
        dist_sq = jnp.where(diag, 1.0, dist_sq)
    inv = lax.rsqrt(dist_sq)
    dist = dist_sq * inv
    frac = dist - jnp.round(dist)
    t = frac * frac
    half_sin = frac * horner(HALF_SIN, t)
    half_cos = horner(HALF_COS, t)
    sine = half_sin * half_cos
    cosine = 1.0 - half_sin * half_sin
    u = inv * (0.5 / math.pi)
    aligned = dz_sq * (inv * inv)
    amp_imag = (u * u) * (1.0 - 3.0 * aligned)
    amp_real = u * ((1.0 - aligned) - amp_imag)
    h_real = amp_real * cosine - amp_imag * sine
    h_imag = amp_real * sine + amp_imag * cosine
    if diag is not None:
        h_real = jnp.where(diag, 0.0, h_real)
        h_imag = jnp.where(diag, 0.0, h_imag)
    return h_real, h_imag


def split(x):
    hi = x.astype(jnp.bfloat16)
    return hi, (x - hi.astype(jnp.float32)).astype(jnp.bfloat16)


def bdot(a, b):
    return jnp.dot(a, b, preferred_element_type=jnp.float32)


def exchange(
    n_row,
    n_grp,
    pos_in,
    det_in,
    pop_in,
    sec_in,
    base_in,
    accum_in,
    next_ref,
    accum_ref,
    olds,
    pos_ref,
    det_ref,
    stage,
    wide,
    rhs_hi,
    rhs_lo,
    row_buf,
    grp_buf,
    coef,
    send_sem,
    row_recv,
    grp_recv,
    row_ready,
    grp_ready,
    load_sem,
):
    cols, width = sec_in.shape[0] // 2, sec_in.shape[1]
    me = lax.axis_index("row")
    mine = lax.axis_index("grp")
    slab = cols * n_grp
    barrier = pltpu.get_barrier_semaphore()

    top = n_grp - 1
    piece = 2 * cols // PIECES

    def send_pieces(p, source):
        for q in range(PIECES):
            part = slice(q * piece, (q + 1) * piece)
            pltpu.make_async_remote_copy(
                source.at[part],
                grp_buf.at[mine, part],
                send_sem.at[1],
                grp_recv.at[jnp.where(mine < top, 0, 1 + q)],
                device_id={"grp": p},
                device_id_type=MESH,
            ).start()

    ahead = (me == 0) & (mine > 0)

    @pl.when(ahead)
    def _():
        pl.semaphore_wait(barrier, 1)
        send_pieces(0, sec_in)

    last = n_row - 2
    pair = me // 2
    odd = lax.rem(me, 2)
    partner = me + 1 - 2 * odd
    in_first = me < 2
    in_last = me >= last
    between = jnp.logical_not(in_first | in_last)
    even = odd == 0
    low = jnp.minimum(mine, 1)
    GO, LATE, WORD = 0, 1, 2
    NEXT, REST = 0, 1

    def to_row(sem, lo, hi):
        def body(p, carry):
            pl.semaphore_signal(sem, inc=1, device_id={"row": p}, device_id_type=MESH)
            return carry

        lax.fori_loop(lo, hi, body, 0)

    def to_grp(sem, lo, hi):
        def body(p, carry):
            pl.semaphore_signal(sem, inc=1, device_id={"grp": p}, device_id_type=MESH)
            return carry

        lax.fori_loop(lo, hi, body, 0)

    slab_part = stage.at[0 : 2 * cols]

    def send_row(lo, hi):
        def body(p, carry):
            pltpu.make_async_remote_copy(
                stage,
                row_buf.at[me],
                send_sem.at[0],
                row_recv.at[pair],
                device_id={"row": p},
                device_id_type=MESH,
            ).start()
            return carry

        lax.fori_loop(lo, hi, body, 0)

    def send_grp(lo, hi, source):
        def body(p, carry):
            send_pieces(p, source)
            return carry

        lax.fori_loop(lo, hi, body, 0)

    def arrived(part, sem):
        pltpu.make_async_copy(part, part, sem).wait()

    section_loads = [
        pltpu.make_async_copy(src, dst, load_sem.at[0])
        for src, dst in (
            (sec_in, stage.at[0 : 2 * cols]),
            (pop_in, stage.at[2 * cols : 2 * cols + 1]),
        )
    ]
    pos_load = pltpu.make_async_copy(pos_in, pos_ref, load_sem.at[1])
    det_load = pltpu.make_async_copy(det_in, det_ref, load_sem.at[2])
    old_loads = [
        pltpu.make_async_copy(src, olds.at[i], load_sem.at[3]) for i, src in enumerate((base_in, accum_in))
    ]

    def start_loads():
        for load in (*section_loads, pos_load, det_load, *old_loads):
            load.start()

    @pl.when(jnp.logical_not(ahead))
    def _():
        start_loads()

    @pl.when(even & (mine > 0))
    def _():
        def body(p, carry):
            pl.semaphore_signal(barrier, inc=1, device_id={"row": partner, "grp": p}, device_id_type=MESH)
            return carry

        lax.fori_loop(mine + 1, n_grp, body, 0)

    @pl.when(jnp.logical_not(even & (mine > 0)))
    def _():
        to_grp(barrier, mine + 1, n_grp)

    @pl.when(even)
    def _():
        pl.semaphore_signal(barrier, inc=1, device_id={"row": partner}, device_id_type=MESH)

    after = jnp.where(in_first, 2, jnp.where(in_last, n_row, last))
    to_row(barrier, after, n_row)

    @pl.when(ahead)
    def _():
        start_loads()

    before = jnp.where(in_first, 0, jnp.where(in_last, last, 2))
    met = before + jnp.where(even, low, 1 + mine + mine - low)

    @pl.when((met > 0) & jnp.logical_not(ahead))
    def _():
        pl.semaphore_wait(barrier, met)

    send_grp(0, jnp.where(even & jnp.logical_not(ahead), low, 0), sec_in)

    def answer_lower(lo, hi):
        to_grp(grp_ready.at[REST], lo, jnp.minimum(hi, mine - 1))
        to_grp(grp_ready.at[NEXT], jnp.maximum(lo, mine - 1), hi)

    answer_lower(0, low)

    @pl.when(between)
    def _():
        to_row(row_ready.at[GO], 0, 2)

    @pl.when(in_last)
    def _():
        to_row(row_ready.at[LATE], 0, last)

    @pl.when(jnp.logical_not(even))
    def _():
        pl.semaphore_signal(row_ready.at[WORD], inc=1, device_id={"row": partner}, device_id_type=MESH)
        answer_lower(low, mine)

    def hear_between():
        pl.semaphore_wait(row_ready.at[GO], last - 2)

        @pl.when(odd == 1)
        def _():
            to_row(row_ready.at[GO], 2, last)

    @pl.when(in_first & (mine == 0) & (last > 2))
    def _():
        hear_between()

    pos_load.wait()
    arrived(stage, load_sem.at[0])
    send_row(jnp.where(in_first, 2, 0), jnp.where(in_first, jnp.where(mine == 0, last, 2), before))

    @pl.when(even)
    def _():
        pl.semaphore_wait(row_ready.at[WORD], 1)
        answer_lower(low, mine)
        send_grp(low, mine, slab_part)

    send_row(partner, partner + 1)

    my_start = pl.multiple_of(me * width, width)
    rows = [pos_ref[d : d + 1, pl.ds(my_start, width)] for d in range(3)]
    tiles = width // TILE

    def spread(tile, slot):
        start = pl.multiple_of(tile * TILE, TILE)
        for d in range(3):
            line = pos_ref[d : d + 1, pl.ds(start, TILE)]
            wide[slot, d] = jnp.transpose(jnp.broadcast_to(line, (TILE, TILE)))

    def fill(tile, slot, diag):
        start = pl.multiple_of(tile * TILE, TILE)
        for part in range(tiles):
            lanes = slice(part * TILE, (part + 1) * TILE)
            h_real, h_imag = coupling(
                [wide[slot, d] for d in range(3)],
                [r[:, lanes] for r in rows],
                None if diag is None else diag[:, lanes],
            )
            for base, h in ((0, h_real), (width, h_imag)):
                hi, lo = split(h)
                at = slice(base + part * TILE, base + (part + 1) * TILE)
                rhs_hi[pl.ds(start, TILE), at] = hi
                rhs_lo[pl.ds(start, TILE), at] = lo

    first = me * tiles
    total = n_row * tiles
    lane_ids = lax.broadcasted_iota(jnp.int32, (TILE, width), 1)
    sub_ids = lax.broadcasted_iota(jnp.int32, (TILE, width), 0)

    def tile_at(j):
        return lax.rem(first + j, total)

    def lower_from_odd():
        @pl.when(jnp.logical_not(even))
        def _():
            send_grp(0, mine, slab_part)

    def step(j, carry):
        spread(tile_at(j + 1), lax.rem(j + 1, 2))
        fill(tile_at(j), lax.rem(j, 2), None)
        return carry

    flat = total <= 16
    spread(first, 0)
    for j in range(total if flat else tiles):
        if j == tiles + PAUSE:
            lower_from_odd()
        if j + 1 < total:
            spread(tile_at(j + 1), (j + 1) % 2)
        fill(tile_at(j), j % 2, sub_ids + j * TILE == lane_ids if j < tiles else None)
    if not flat:
        lower_from_odd()
        lax.fori_loop(tiles, total, step, 0)

    @pl.when(in_first & (mine > 0) & (last > 2))
    def _():
        hear_between()
        send_row(2, last)

    @pl.when(between)
    def _():
        pl.semaphore_wait(row_ready.at[GO], 1)
        send_row(2, 2 * pair)
        send_row(2 * pair + 2, last)

    @pl.when(mine < n_grp - 1)
    def _():
        pl.semaphore_wait(grp_ready.at[NEXT], 1)
        send_grp(mine + 1, mine + 2, slab_part)

    @pl.when(jnp.logical_not(in_last))
    def _():
        pl.semaphore_wait(row_ready.at[LATE], 2)
        send_row(last, n_row)

    @pl.when(mine < n_grp - 2)
    def _():
        pl.semaphore_wait(grp_ready.at[REST], n_grp - 2 - mine)
        send_grp(mine + 2, n_grp, slab_part)

    det_load.wait()
    arrived(olds, load_sem.at[3])

    col_start = pl.multiple_of(mine * cols, cols)
    eye = lax.broadcasted_iota(jnp.int32, (cols, TILE), 0) + col_start == lax.broadcasted_iota(
        jnp.int32, (cols, TILE), 1
    )
    slab_rows = [pos_ref[d : d + 1, :TILE] for d in range(3)]
    own_cols = [
        jnp.sum(jnp.where(eye, jnp.broadcast_to(r, (cols, TILE)), 0.0), axis=1, keepdims=True) for r in slab_rows
    ]
    w_real, w_imag = coupling(own_cols, slab_rows, eye)
    w_real = AMPLITUDE * w_real + jnp.where(eye, det_ref[:, :TILE], 0.0)
    w_imag = AMPLITUDE * w_imag + jnp.where(eye, -0.5, 0.0)
    most = slab - cols
    l_hi, l_lo = split(jnp.concatenate([w_real, w_imag], axis=0)[:, :most])
    for j in range(cols):
        for lead, w in ((0, w_real), (cols, w_imag)):
            coef[j, lead : lead + cols] = jnp.broadcast_to(w[:, most + j : most + j + 1], (cols, width))

    y_local = stage[0 : 2 * cols]
    row_buf[me] = stage[...]
    grp_buf[mine] = y_local

    def left(slab_and_pop):
        signed = jnp.broadcast_to(2.0 * slab_and_pop[2 * cols :] - 1.0, (PAD, width))
        return split(jnp.concatenate([slab_and_pop[: 2 * cols], signed], axis=0))

    main = jnp.zeros((4 * cols + 2 * PAD, 2 * width), jnp.float32)
    rest = jnp.zeros((2 * cols + PAD, 2 * width), jnp.float32)
    group = 2
    for lead in range(0, n_row, group):
        his, los = [], []

        @pl.when(pair == lead // group)
        def _():
            arrived(row_buf.at[0], row_recv.at[lead // group])

        @pl.when(pair != lead // group)
        def _():
            arrived(row_buf.at[0:group], row_recv.at[lead // group])

        for p in range(lead, lead + group):
            hi, lo = left(row_buf[p])
            his.append(hi)
            los.append(lo)
        hi = jnp.concatenate(his, axis=1)
        lo = jnp.concatenate(los, axis=1)
        span = slice(lead * width, (lead + group) * width)
        main = main + bdot(jnp.concatenate([hi, lo], axis=0), rhs_hi[span, :])
        rest = rest + bdot(hi, rhs_lo[span, :])
    half = 2 * cols + PAD
    z = AMPLITUDE * (main[:half] + main[half:] + rest)
    z_real = z[:cols, :width] - z[cols : 2 * cols, width:]
    z_imag = z[:cols, width:] + z[cols : 2 * cols, :width]
    shift = z[2 * cols : 2 * cols + 1, :width]

    y_real, y_imag = y_local[:cols], y_local[cols:]
    total_shift = shift + det_ref[:, pl.ds(my_start, width)]
    z_real = z_real + total_shift * y_real + 0.5 * y_imag
    z_imag = z_imag + total_shift * y_imag - 0.5 * y_real

    if n_grp > 2:

        @pl.when(mine < top)
        def _():
            arrived(grp_buf.at[0 : top - 1], grp_recv.at[0])

        @pl.when(mine == top)
        def _():
            arrived(grp_buf.at[0:top], grp_recv.at[0])

    elif n_grp == 2:

        @pl.when(mine == top)
        def _():
            arrived(grp_buf.at[0:top], grp_recv.at[0])

    blocks = [grp_buf[g] for g in range(top)]
    full = jnp.concatenate(
        [jnp.concatenate([block[:cols], block[cols:]], axis=1) for block in blocks], axis=0
    )
    f_hi, f_lo = split(full)
    v = bdot(l_hi, f_hi) + bdot(l_lo, f_hi) + bdot(l_hi, f_lo)
    z_imag = z_imag - (v[:cols, width:] - v[cols:, :width])
    z_real = z_real - (v[:cols, :width] + v[cols:, width:])

    for i, rate in enumerate((z_imag, -z_real)):
        next_ref[i] = olds[0, i] + 0.5 * TIME_STEP * rate
        accum_ref[i] = olds[1, i] + TIME_STEP / 3.0 * rate

    arrived(row_buf.at[0 : n_row - 1], send_sem.at[0])
    arrived(grp_buf.at[0 : n_grp - 1], send_sem.at[1])

    v_real = v_imag = jnp.zeros((cols, width), jnp.float32)
    for q in range(PIECES):

        @pl.when(mine < top)
        def _():
            arrived(grp_buf.at[0, 0:piece], grp_recv.at[1 + q])

        for row in range(q * piece, (q + 1) * piece):
            j = row % cols
            f = grp_buf[top, row : row + 1]
            wr, wi = coef[j, :cols], coef[j, cols:]
            if row < cols:
                v_real = v_real + wr * f
                v_imag = v_imag - wi * f
            else:
                v_real = v_real + wi * f
                v_imag = v_imag + wr * f
    for i, rate in enumerate((-v_imag, v_real)):
        next_ref[i] = next_ref[i] + 0.5 * TIME_STEP * rate
        accum_ref[i] = accum_ref[i] + TIME_STEP / 3.0 * rate


def kernel(n_row, n_grp, *refs):
    pl.run_scoped(
        functools.partial(exchange, n_row, n_grp, *refs),
        send_sem=pltpu.SemaphoreType.DMA((2,)),
        row_recv=pltpu.SemaphoreType.DMA((n_row // 2,)),
        grp_recv=pltpu.SemaphoreType.DMA((1 + PIECES,)),
        row_ready=pltpu.SemaphoreType.REGULAR((3,)),
        grp_ready=pltpu.SemaphoreType.REGULAR((2,)),
        load_sem=pltpu.SemaphoreType.DMA((4,)),
    )


def store(next_ref, accum_ref, next_out, accum_out):
    def scope(sem):
        copies = [
            pltpu.make_async_copy(next_ref, next_out, sem.at[0]),
            pltpu.make_async_copy(accum_ref, accum_out, sem.at[1]),
        ]
        for copy in copies:
            copy.start()
        for copy in copies:
            copy.wait()

    pl.run_scoped(scope, pltpu.SemaphoreType.DMA((2,)))


def local(positions, detuning, populations, base, section, accum):
    n_row, n_grp = lax.axis_size("row"), lax.axis_size("grp")
    cols, width = section.shape[1], section.shape[2]
    total = positions.shape[1]
    block = section.shape
    results = pl.pallas_call(
        functools.partial(kernel, n_row, n_grp),
        out_shape=(pltpu.VMEM(block, jnp.float32), pltpu.VMEM(block, jnp.float32)),
        in_specs=[pl.BlockSpec(memory_space=pl.ANY)] * 6,
        out_specs=(pl.BlockSpec(memory_space=pltpu.VMEM), pl.BlockSpec(memory_space=pltpu.VMEM)),
        scratch_shapes=[
            pltpu.VMEM((2, *block), jnp.float32),
            pltpu.VMEM((3, total), jnp.float32),
            pltpu.VMEM((1, total), jnp.float32),
            pltpu.VMEM((2 * cols + 1, width), jnp.float32),
            pltpu.VMEM((2, 3, TILE, TILE), jnp.float32),
            pltpu.VMEM((total, 2 * width), jnp.bfloat16),
            pltpu.VMEM((total, 2 * width), jnp.bfloat16),
            pltpu.VMEM((n_row, 2 * cols + 1, width), jnp.float32),
            pltpu.VMEM((n_grp, 2 * cols, width), jnp.float32),
            pltpu.VMEM((cols, 2 * cols, width), jnp.float32),
        ],
        compiler_params=pltpu.CompilerParams(collective_id=0, has_side_effects=True),
    )(positions, detuning.reshape(1, total), populations.reshape(1, width), section.reshape(2 * cols, width), base, accum)
    return pl.pallas_call(
        store,
        out_shape=(jax.ShapeDtypeStruct(block, jnp.float32),) * 2,
        in_specs=[pl.BlockSpec(memory_space=pltpu.VMEM)] * 2,
        out_specs=(pl.BlockSpec(memory_space=pltpu.HBM),) * 2,
    )(*[pltpu.with_memory_space_constraint(r, pltpu.VMEM) for r in results])


def solution(mesh):
    return jax.shard_map(
        local,
        mesh=mesh,
        in_specs=(
            P(),
            P(),
            P("row"),
            P(None, "grp", "row"),
            P(None, "grp", "row"),
            P(None, "grp", "row"),
        ),
        out_specs=(P(None, "grp", "row"), P(None, "grp", "row")),
        check_vma=False,
    )
```

```python
import functools
import math

import jax
import jax.numpy as jnp
from jax import lax
from jax.experimental import pallas as pl
from jax.experimental.pallas import tpu as pltpu
from jax.sharding import PartitionSpec as P

TIME_STEP = 0.2
PAD = 16
TILE = 128
AMPLITUDE = -0.75
PAUSE = 3
PIECES = 4

HALF_SIN = (4.442882834149929, -7.308241154546326, 3.606288958225646, -0.8457635961475002, 0.10920575363724722)
HALF_COS = (1.4142134965650124, -6.97885098823893, 5.739461170681154, -1.8835629872981716, 0.31069819180355424)
MESH = pl.DeviceIdType.MESH


def horner(coeffs, t):
    total = coeffs[-1] * t + coeffs[-2]
    for value in coeffs[-3::-1]:
        total = total * t + value
    return total


def coupling(cols, rows, diag):
    dx = cols[0] - rows[0]
    dy = cols[1] - rows[1]
    dz = cols[2] - rows[2]
    dz_sq = dz * dz
    dist_sq = dx * dx + dy * dy + dz_sq
    if diag is not None:
        dist_sq = jnp.where(diag, 1.0, dist_sq)
    inv = lax.rsqrt(dist_sq)
    dist = dist_sq * inv
    frac = dist - jnp.round(dist)
    t = frac * frac
    half_sin = frac * horner(HALF_SIN, t)
    half_cos = horner(HALF_COS, t)
    sine = half_sin * half_cos
    cosine = 1.0 - half_sin * half_sin
    u = inv * (0.5 / math.pi)
    aligned = dz_sq * (inv * inv)
    amp_imag = (u * u) * (1.0 - 3.0 * aligned)
    amp_real = u * ((1.0 - aligned) - amp_imag)
    h_real = amp_real * cosine - amp_imag * sine
    h_imag = amp_real * sine + amp_imag * cosine
    if diag is not None:
        h_real = jnp.where(diag, 0.0, h_real)
        h_imag = jnp.where(diag, 0.0, h_imag)
    return h_real, h_imag


def split(x):
    hi = x.astype(jnp.bfloat16)
    return hi, (x - hi.astype(jnp.float32)).astype(jnp.bfloat16)


def bdot(a, b):
    return jnp.dot(a, b, preferred_element_type=jnp.float32)


def exchange(
    n_row,
    n_grp,
    pos_in,
    det_in,
    pop_in,
    sec_in,
    base_in,
    accum_in,
    next_ref,
    accum_ref,
    olds,
    pos_ref,
    det_ref,
    stage,
    wide,
    rhs_hi,
    rhs_lo,
    row_buf,
    grp_buf,
    coef,
    send_sem,
    row_recv,
    grp_recv,
    row_ready,
    grp_ready,
    load_sem,
):
    cols, width = sec_in.shape[0] // 2, sec_in.shape[1]
    me = lax.axis_index("row")
    mine = lax.axis_index("grp")
    slab = cols * n_grp
    barrier = pltpu.get_barrier_semaphore()

    top = n_grp - 1
    piece = 2 * cols // PIECES

    def send_pieces(p, source):
        for q in range(PIECES):
            part = slice(q * piece, (q + 1) * piece)
            pltpu.make_async_remote_copy(
                source.at[part],
                grp_buf.at[mine, part],
                send_sem.at[1],
                grp_recv.at[jnp.where(mine < top, 0, 1 + q)],
                device_id={"grp": p},
                device_id_type=MESH,
            ).start()

    ahead = (me == 0) & (mine > 0)

    @pl.when(ahead)
    def _():
        pl.semaphore_wait(barrier, 1)
        send_pieces(0, sec_in)

    last = n_row - 2
    pair = me // 2
    odd = lax.rem(me, 2)
    partner = me + 1 - 2 * odd
    in_first = me < 2
    in_last = me >= last
    between = jnp.logical_not(in_first | in_last)
    even = odd == 0
    low = jnp.minimum(mine, 1)
    GO, LATE, WORD = 0, 1, 2
    NEXT, REST = 0, 1

    def to_row(sem, lo, hi):
        def body(p, carry):
            pl.semaphore_signal(sem, inc=1, device_id={"row": p}, device_id_type=MESH)
            return carry

        lax.fori_loop(lo, hi, body, 0)

    def to_grp(sem, lo, hi):
        def body(p, carry):
            pl.semaphore_signal(sem, inc=1, device_id={"grp": p}, device_id_type=MESH)
            return carry

        lax.fori_loop(lo, hi, body, 0)

    slab_part = stage.at[0 : 2 * cols]

    def send_row(lo, hi):
        def body(p, carry):
            pltpu.make_async_remote_copy(
                stage,
                row_buf.at[me],
                send_sem.at[0],
                row_recv.at[pair],
                device_id={"row": p},
                device_id_type=MESH,
            ).start()
            return carry

        lax.fori_loop(lo, hi, body, 0)

    def send_grp(lo, hi, source):
        def body(p, carry):
            send_pieces(p, source)
            return carry

        lax.fori_loop(lo, hi, body, 0)

    def arrived(part, sem):
        pltpu.make_async_copy(part, part, sem).wait()

    section_loads = [
        pltpu.make_async_copy(src, dst, load_sem.at[0])
        for src, dst in (
            (sec_in, stage.at[0 : 2 * cols]),
            (pop_in, stage.at[2 * cols : 2 * cols + 1]),
        )
    ]
    pos_load = pltpu.make_async_copy(pos_in, pos_ref, load_sem.at[1])
    det_load = pltpu.make_async_copy(det_in, det_ref, load_sem.at[2])
    old_loads = [
        pltpu.make_async_copy(src, olds.at[i], load_sem.at[3]) for i, src in enumerate((base_in, accum_in))
    ]

    def start_loads():
        for load in (*section_loads, pos_load, det_load, *old_loads):
            load.start()

    @pl.when(jnp.logical_not(ahead))
    def _():
        start_loads()

    @pl.when(even & (mine > 0))
    def _():
        def body(p, carry):
            pl.semaphore_signal(barrier, inc=1, device_id={"row": partner, "grp": p}, device_id_type=MESH)
            return carry

        lax.fori_loop(mine + 1, n_grp, body, 0)

    @pl.when(jnp.logical_not(even & (mine > 0)))
    def _():
        to_grp(barrier, mine + 1, n_grp)

    @pl.when(even)
    def _():
        pl.semaphore_signal(barrier, inc=1, device_id={"row": partner}, device_id_type=MESH)

    after = jnp.where(in_first, 2, jnp.where(in_last, n_row, last))
    to_row(barrier, after, n_row)

    @pl.when(ahead)
    def _():
        start_loads()

    before = jnp.where(in_first, 0, jnp.where(in_last, last, 2))
    met = before + jnp.where(even, low, 1 + mine + mine - low)

    @pl.when((met > 0) & jnp.logical_not(ahead))
    def _():
        pl.semaphore_wait(barrier, met)

    send_grp(0, jnp.where(even & jnp.logical_not(ahead), low, 0), sec_in)

    def answer_lower(lo, hi):
        to_grp(grp_ready.at[REST], lo, jnp.minimum(hi, mine - 1))
        to_grp(grp_ready.at[NEXT], jnp.maximum(lo, mine - 1), hi)

    answer_lower(0, low)

    @pl.when(between)
    def _():
        to_row(row_ready.at[GO], 0, 2)

    @pl.when(in_last)
    def _():
        to_row(row_ready.at[LATE], 0, last)

    @pl.when(jnp.logical_not(even))
    def _():
        pl.semaphore_signal(row_ready.at[WORD], inc=1, device_id={"row": partner}, device_id_type=MESH)
        answer_lower(low, mine)

    def hear_between():
        pl.semaphore_wait(row_ready.at[GO], last - 2)

        @pl.when(odd == 1)
        def _():
            to_row(row_ready.at[GO], 2, last)

    @pl.when(in_first & (mine == 0) & (last > 2))
    def _():
        hear_between()

    pos_load.wait()
    arrived(stage, load_sem.at[0])
    send_row(jnp.where(in_first, 2, 0), jnp.where(in_first, jnp.where(mine == 0, last, 2), before))

    @pl.when(even)
    def _():
        pl.semaphore_wait(row_ready.at[WORD], 1)
        answer_lower(low, mine)
        send_grp(low, jnp.where(ahead, low, mine), slab_part)

    send_row(partner, partner + 1)

    my_start = pl.multiple_of(me * width, width)
    rows = [pos_ref[d : d + 1, pl.ds(my_start, width)] for d in range(3)]
    tiles = width // TILE

    def spread(tile, slot):
        start = pl.multiple_of(tile * TILE, TILE)
        for d in range(3):
            line = pos_ref[d : d + 1, pl.ds(start, TILE)]
            wide[slot, d] = jnp.transpose(jnp.broadcast_to(line, (TILE, TILE)))

    def fill(tile, slot, diag):
        start = pl.multiple_of(tile * TILE, TILE)
        for part in range(tiles):
            lanes = slice(part * TILE, (part + 1) * TILE)
            h_real, h_imag = coupling(
                [wide[slot, d] for d in range(3)],
                [r[:, lanes] for r in rows],
                None if diag is None else diag[:, lanes],
            )
            for base, h in ((0, h_real), (width, h_imag)):
                hi, lo = split(h)
                at = slice(base + part * TILE, base + (part + 1) * TILE)
                rhs_hi[pl.ds(start, TILE), at] = hi
                rhs_lo[pl.ds(start, TILE), at] = lo

    first = me * tiles
    total = n_row * tiles
    lane_ids = lax.broadcasted_iota(jnp.int32, (TILE, width), 1)
    sub_ids = lax.broadcasted_iota(jnp.int32, (TILE, width), 0)

    def tile_at(j):
        return lax.rem(first + j, total)

    def lower_from_odd():
        @pl.when(jnp.logical_not(even))
        def _():
            send_grp(0, mine, slab_part)

    def step(j, carry):
        spread(tile_at(j + 1), lax.rem(j + 1, 2))
        fill(tile_at(j), lax.rem(j, 2), None)
        return carry

    flat = total <= 16
    spread(first, 0)
    for j in range(total if flat else tiles):
        if j == tiles + PAUSE:
            lower_from_odd()
        if j + 1 < total:
            spread(tile_at(j + 1), (j + 1) % 2)
        fill(tile_at(j), j % 2, sub_ids + j * TILE == lane_ids if j < tiles else None)
    if not flat:
        lower_from_odd()
        lax.fori_loop(tiles, total, step, 0)

    @pl.when(ahead)
    def _():
        send_grp(1, mine, slab_part)

    @pl.when(in_first & (mine > 0) & (last > 2))
    def _():
        hear_between()
        send_row(2, last)

    @pl.when(between)
    def _():
        pl.semaphore_wait(row_ready.at[GO], 1)
        send_row(2, 2 * pair)
        send_row(2 * pair + 2, last)

    @pl.when(mine < n_grp - 1)
    def _():
        pl.semaphore_wait(grp_ready.at[NEXT], 1)
        send_grp(mine + 1, mine + 2, slab_part)

    @pl.when(jnp.logical_not(in_last))
    def _():
        pl.semaphore_wait(row_ready.at[LATE], 2)
        send_row(last, n_row)

    @pl.when(mine < n_grp - 2)
    def _():
        pl.semaphore_wait(grp_ready.at[REST], n_grp - 2 - mine)
        send_grp(mine + 2, n_grp, slab_part)

    det_load.wait()
    arrived(olds, load_sem.at[3])

    col_start = pl.multiple_of(mine * cols, cols)
    eye = lax.broadcasted_iota(jnp.int32, (cols, TILE), 0) + col_start == lax.broadcasted_iota(
        jnp.int32, (cols, TILE), 1
    )
    slab_rows = [pos_ref[d : d + 1, :TILE] for d in range(3)]
    own_cols = [
        jnp.sum(jnp.where(eye, jnp.broadcast_to(r, (cols, TILE)), 0.0), axis=1, keepdims=True) for r in slab_rows
    ]
    w_real, w_imag = coupling(own_cols, slab_rows, eye)
    w_real = AMPLITUDE * w_real + jnp.where(eye, det_ref[:, :TILE], 0.0)
    w_imag = AMPLITUDE * w_imag + jnp.where(eye, -0.5, 0.0)
    most = slab - cols
    l_hi, l_lo = split(jnp.concatenate([w_real, w_imag], axis=0)[:, :most])
    for j in range(cols):
        for lead, w in ((0, w_real), (cols, w_imag)):
            coef[j, lead : lead + cols] = jnp.broadcast_to(w[:, most + j : most + j + 1], (cols, width))

    y_local = stage[0 : 2 * cols]
    row_buf[me] = stage[...]
    grp_buf[mine] = y_local

    def left(slab_and_pop):
        signed = jnp.broadcast_to(2.0 * slab_and_pop[2 * cols :] - 1.0, (PAD, width))
        return split(jnp.concatenate([slab_and_pop[: 2 * cols], signed], axis=0))

    def lower_planes():
        if n_grp > 2:

            @pl.when(mine < top)
            def _():
                arrived(grp_buf.at[0 : top - 1], grp_recv.at[0])

            @pl.when(mine == top)
            def _():
                arrived(grp_buf.at[0:top], grp_recv.at[0])

        elif n_grp == 2:

            @pl.when(mine == top)
            def _():
                arrived(grp_buf.at[0:top], grp_recv.at[0])

        blocks = [grp_buf[g] for g in range(top)]
        full = jnp.concatenate(
            [jnp.concatenate([block[:cols], block[cols:]], axis=1) for block in blocks], axis=0
        )
        f_hi, f_lo = split(full)
        v = bdot(l_hi, f_hi) + bdot(l_lo, f_hi) + bdot(l_hi, f_lo)
        v_imag = v[:cols, width:] - v[cols:, :width]
        v_real = v[:cols, :width] + v[cols:, width:]
        return v_real, v_imag

    main = jnp.zeros((4 * cols + 2 * PAD, 2 * width), jnp.float32)
    rest = jnp.zeros((2 * cols + PAD, 2 * width), jnp.float32)
    group = 2
    for lead in range(0, n_row, group):
        if lead == last:
            v_real, v_imag = lower_planes()
        his, los = [], []

        @pl.when(pair == lead // group)
        def _():
            arrived(row_buf.at[0], row_recv.at[lead // group])

        @pl.when(pair != lead // group)
        def _():
            arrived(row_buf.at[0:group], row_recv.at[lead // group])

        for p in range(lead, lead + group):
            hi, lo = left(row_buf[p])
            his.append(hi)
            los.append(lo)
        hi = jnp.concatenate(his, axis=1)
        lo = jnp.concatenate(los, axis=1)
        span = slice(lead * width, (lead + group) * width)
        main = main + bdot(jnp.concatenate([hi, lo], axis=0), rhs_hi[span, :])
        rest = rest + bdot(hi, rhs_lo[span, :])
    half = 2 * cols + PAD
    z = AMPLITUDE * (main[:half] + main[half:] + rest)
    z_real = z[:cols, :width] - z[cols : 2 * cols, width:]
    z_imag = z[:cols, width:] + z[cols : 2 * cols, :width]
    shift = z[2 * cols : 2 * cols + 1, :width]

    y_real, y_imag = y_local[:cols], y_local[cols:]
    total_shift = shift + det_ref[:, pl.ds(my_start, width)]
    z_real = z_real + total_shift * y_real + 0.5 * y_imag
    z_imag = z_imag + total_shift * y_imag - 0.5 * y_real

    z_imag = z_imag - v_imag
    z_real = z_real - v_real

    for i, rate in enumerate((z_imag, -z_real)):
        next_ref[i] = olds[0, i] + 0.5 * TIME_STEP * rate
        accum_ref[i] = olds[1, i] + TIME_STEP / 3.0 * rate

    arrived(row_buf.at[0 : n_row - 1], send_sem.at[0])
    arrived(grp_buf.at[0 : n_grp - 1], send_sem.at[1])

    v_real = v_imag = jnp.zeros((cols, width), jnp.float32)
    for q in range(PIECES):

        @pl.when(mine < top)
        def _():
            arrived(grp_buf.at[0, 0:piece], grp_recv.at[1 + q])

        for row in range(q * piece, (q + 1) * piece):
            j = row % cols
            f = grp_buf[top, row : row + 1]
            wr, wi = coef[j, :cols], coef[j, cols:]
            if row < cols:
                v_real = v_real + wr * f
                v_imag = v_imag - wi * f
            else:
                v_real = v_real + wi * f
                v_imag = v_imag + wr * f
    for i, rate in enumerate((-v_imag, v_real)):
        next_ref[i] = next_ref[i] + 0.5 * TIME_STEP * rate
        accum_ref[i] = accum_ref[i] + TIME_STEP / 3.0 * rate


def kernel(n_row, n_grp, *refs):
    pl.run_scoped(
        functools.partial(exchange, n_row, n_grp, *refs),
        send_sem=pltpu.SemaphoreType.DMA((2,)),
        row_recv=pltpu.SemaphoreType.DMA((n_row // 2,)),
        grp_recv=pltpu.SemaphoreType.DMA((1 + PIECES,)),
        row_ready=pltpu.SemaphoreType.REGULAR((3,)),
        grp_ready=pltpu.SemaphoreType.REGULAR((2,)),
        load_sem=pltpu.SemaphoreType.DMA((4,)),
    )


def store(next_ref, accum_ref, next_out, accum_out):
    def scope(sem):
        copies = [
            pltpu.make_async_copy(next_ref, next_out, sem.at[0]),
            pltpu.make_async_copy(accum_ref, accum_out, sem.at[1]),
        ]
        for copy in copies:
            copy.start()
        for copy in copies:
            copy.wait()

    pl.run_scoped(scope, pltpu.SemaphoreType.DMA((2,)))


def local(positions, detuning, populations, base, section, accum):
    n_row, n_grp = lax.axis_size("row"), lax.axis_size("grp")
    cols, width = section.shape[1], section.shape[2]
    total = positions.shape[1]
    block = section.shape
    results = pl.pallas_call(
        functools.partial(kernel, n_row, n_grp),
        out_shape=(pltpu.VMEM(block, jnp.float32), pltpu.VMEM(block, jnp.float32)),
        in_specs=[pl.BlockSpec(memory_space=pl.ANY)] * 6,
        out_specs=(pl.BlockSpec(memory_space=pltpu.VMEM), pl.BlockSpec(memory_space=pltpu.VMEM)),
        scratch_shapes=[
            pltpu.VMEM((2, *block), jnp.float32),
            pltpu.VMEM((3, total), jnp.float32),
            pltpu.VMEM((1, total), jnp.float32),
            pltpu.VMEM((2 * cols + 1, width), jnp.float32),
            pltpu.VMEM((2, 3, TILE, TILE), jnp.float32),
            pltpu.VMEM((total, 2 * width), jnp.bfloat16),
            pltpu.VMEM((total, 2 * width), jnp.bfloat16),
            pltpu.VMEM((n_row, 2 * cols + 1, width), jnp.float32),
            pltpu.VMEM((n_grp, 2 * cols, width), jnp.float32),
            pltpu.VMEM((cols, 2 * cols, width), jnp.float32),
        ],
        compiler_params=pltpu.CompilerParams(collective_id=0, has_side_effects=True),
    )(positions, detuning.reshape(1, total), populations.reshape(1, width), section.reshape(2 * cols, width), base, accum)
    return pl.pallas_call(
        store,
        out_shape=(jax.ShapeDtypeStruct(block, jnp.float32),) * 2,
        in_specs=[pl.BlockSpec(memory_space=pltpu.VMEM)] * 2,
        out_specs=(pl.BlockSpec(memory_space=pltpu.HBM),) * 2,
    )(*[pltpu.with_memory_space_constraint(r, pltpu.VMEM) for r in results])


def solution(mesh):
    return jax.shard_map(
        local,
        mesh=mesh,
        in_specs=(
            P(),
            P(),
            P("row"),
            P(None, "grp", "row"),
            P(None, "grp", "row"),
            P(None, "grp", "row"),
        ),
        out_specs=(P(None, "grp", "row"), P(None, "grp", "row")),
        check_vma=False,
    )
```

```python
import functools
import math

import jax
import jax.numpy as jnp
from jax import lax
from jax.experimental import pallas as pl
from jax.experimental.pallas import tpu as pltpu
from jax.sharding import PartitionSpec as P

TIME_STEP = 0.2
PAD = 16
TILE = 128
AMPLITUDE = -0.75
PAUSE = 3
PIECES = 4

HALF_SIN = (4.442882834149929, -7.308241154546326, 3.606288958225646, -0.8457635961475002, 0.10920575363724722)
HALF_COS = (1.4142134965650124, -6.97885098823893, 5.739461170681154, -1.8835629872981716, 0.31069819180355424)
MESH = pl.DeviceIdType.MESH


def horner(coeffs, t):
    total = coeffs[-1] * t + coeffs[-2]
    for value in coeffs[-3::-1]:
        total = total * t + value
    return total


def coupling(cols, rows, diag):
    dx = cols[0] - rows[0]
    dy = cols[1] - rows[1]
    dz = cols[2] - rows[2]
    dz_sq = dz * dz
    dist_sq = dx * dx + dy * dy + dz_sq
    if diag is not None:
        dist_sq = jnp.where(diag, 1.0, dist_sq)
    inv = lax.rsqrt(dist_sq)
    dist = dist_sq * inv
    frac = dist - jnp.round(dist)
    t = frac * frac
    half_sin = frac * horner(HALF_SIN, t)
    half_cos = horner(HALF_COS, t)
    sine = half_sin * half_cos
    cosine = 1.0 - half_sin * half_sin
    u = inv * (0.5 / math.pi)
    aligned = dz_sq * (inv * inv)
    amp_imag = (u * u) * (1.0 - 3.0 * aligned)
    amp_real = u * ((1.0 - aligned) - amp_imag)
    h_real = amp_real * cosine - amp_imag * sine
    h_imag = amp_real * sine + amp_imag * cosine
    if diag is not None:
        h_real = jnp.where(diag, 0.0, h_real)
        h_imag = jnp.where(diag, 0.0, h_imag)
    return h_real, h_imag


def split(x):
    hi = x.astype(jnp.bfloat16)
    return hi, (x - hi.astype(jnp.float32)).astype(jnp.bfloat16)


def bdot(a, b):
    return jnp.dot(a, b, preferred_element_type=jnp.float32)


def exchange(
    n_row,
    n_grp,
    pos_in,
    det_in,
    pop_in,
    sec_in,
    base_in,
    accum_in,
    next_ref,
    accum_ref,
    olds,
    pos_ref,
    det_ref,
    stage,
    wide,
    rhs_hi,
    rhs_lo,
    row_buf,
    grp_buf,
    coef,
    send_sem,
    row_recv,
    grp_recv,
    row_ready,
    grp_ready,
    load_sem,
):
    cols, width = sec_in.shape[0] // 2, sec_in.shape[1]
    me = lax.axis_index("row")
    mine = lax.axis_index("grp")
    slab = cols * n_grp
    barrier = pltpu.get_barrier_semaphore()

    top = n_grp - 1
    piece = 2 * cols // PIECES

    def send_pieces(p, source):
        for q in range(PIECES):
            part = slice(q * piece, (q + 1) * piece)
            pltpu.make_async_remote_copy(
                source.at[part],
                grp_buf.at[mine, part],
                send_sem.at[1],
                grp_recv.at[jnp.where(mine < top, 0, 1 + q)],
                device_id={"grp": p},
                device_id_type=MESH,
            ).start()

    ahead = (me == 0) & (mine > 0)

    @pl.when(ahead)
    def _():
        pl.semaphore_wait(barrier, 1)
        send_pieces(0, sec_in)

    last = n_row - 2
    pair = me // 2
    odd = lax.rem(me, 2)
    partner = me + 1 - 2 * odd
    in_first = me < 2
    in_last = me >= last
    between = jnp.logical_not(in_first | in_last)
    even = odd == 0
    low = jnp.minimum(mine, 1)
    GO, LATE, WORD = 0, 1, 2
    NEXT, REST = 0, 1

    def to_row(sem, lo, hi):
        def body(p, carry):
            pl.semaphore_signal(sem, inc=1, device_id={"row": p}, device_id_type=MESH)
            return carry

        lax.fori_loop(lo, hi, body, 0)

    def to_grp(sem, lo, hi):
        def body(p, carry):
            pl.semaphore_signal(sem, inc=1, device_id={"grp": p}, device_id_type=MESH)
            return carry

        lax.fori_loop(lo, hi, body, 0)

    slab_part = stage.at[0 : 2 * cols]

    def send_row(lo, hi):
        def body(p, carry):
            pltpu.make_async_remote_copy(
                stage,
                row_buf.at[me],
                send_sem.at[0],
                row_recv.at[pair],
                device_id={"row": p},
                device_id_type=MESH,
            ).start()
            return carry

        lax.fori_loop(lo, hi, body, 0)

    def send_grp(lo, hi, source):
        def body(p, carry):
            send_pieces(p, source)
            return carry

        lax.fori_loop(lo, hi, body, 0)

    def arrived(part, sem):
        pltpu.make_async_copy(part, part, sem).wait()

    section_loads = [
        pltpu.make_async_copy(src, dst, load_sem.at[0])
        for src, dst in (
            (sec_in, stage.at[0 : 2 * cols]),
            (pop_in, stage.at[2 * cols : 2 * cols + 1]),
        )
    ]
    pos_load = pltpu.make_async_copy(pos_in, pos_ref, load_sem.at[1])
    det_load = pltpu.make_async_copy(det_in, det_ref, load_sem.at[2])
    old_loads = [
        pltpu.make_async_copy(src, olds.at[i], load_sem.at[3]) for i, src in enumerate((base_in, accum_in))
    ]

    def start_loads():
        for load in (*section_loads, pos_load, det_load, *old_loads):
            load.start()

    @pl.when(jnp.logical_not(ahead))
    def _():
        start_loads()

    @pl.when(even & (mine > 0))
    def _():
        def body(p, carry):
            pl.semaphore_signal(barrier, inc=1, device_id={"row": partner, "grp": p}, device_id_type=MESH)
            return carry

        lax.fori_loop(mine + 1, n_grp, body, 0)

    @pl.when(jnp.logical_not(even & (mine > 0)))
    def _():
        to_grp(barrier, mine + 1, n_grp)

    @pl.when(even)
    def _():
        pl.semaphore_signal(barrier, inc=1, device_id={"row": partner}, device_id_type=MESH)

    after = jnp.where(in_first, 2, jnp.where(in_last, n_row, last))
    to_row(barrier, after, n_row)

    @pl.when(ahead)
    def _():
        start_loads()

    before = jnp.where(in_first, 0, jnp.where(in_last, last, 2))
    met = before + jnp.where(even, low, 1 + mine + mine - low)

    @pl.when((met > 0) & jnp.logical_not(ahead))
    def _():
        pl.semaphore_wait(barrier, met)

    send_grp(0, jnp.where(even & jnp.logical_not(ahead), low, 0), sec_in)

    def answer_lower(lo, hi):
        to_grp(grp_ready.at[REST], lo, jnp.minimum(hi, mine - 1))
        to_grp(grp_ready.at[NEXT], jnp.maximum(lo, mine - 1), hi)

    answer_lower(0, low)

    @pl.when(between)
    def _():
        to_row(row_ready.at[GO], 0, 2)

    @pl.when(in_last)
    def _():
        to_row(row_ready.at[LATE], 0, last)

    @pl.when(jnp.logical_not(even))
    def _():
        pl.semaphore_signal(row_ready.at[WORD], inc=1, device_id={"row": partner}, device_id_type=MESH)
        answer_lower(low, mine)

    def hear_between():
        pl.semaphore_wait(row_ready.at[GO], last - 2)

        @pl.when(odd == 1)
        def _():
            to_row(row_ready.at[GO], 2, last)

    @pl.when(in_first & (mine == 0) & (last > 2))
    def _():
        hear_between()

    pos_load.wait()
    arrived(stage, load_sem.at[0])
    send_row(jnp.where(in_first, 2, 0), jnp.where(in_first, jnp.where(mine == 0, last, 2), before))

    @pl.when(even)
    def _():
        pl.semaphore_wait(row_ready.at[WORD], 1)
        answer_lower(low, mine)
        send_grp(low, jnp.where(ahead, low, mine), slab_part)

    send_row(partner, partner + 1)

    @pl.when(jnp.logical_not(even) & (mine < top))
    def _():
        send_grp(0, mine, slab_part)

    my_start = pl.multiple_of(me * width, width)
    rows = [pos_ref[d : d + 1, pl.ds(my_start, width)] for d in range(3)]
    tiles = width // TILE

    def spread(tile, slot):
        start = pl.multiple_of(tile * TILE, TILE)
        for d in range(3):
            line = pos_ref[d : d + 1, pl.ds(start, TILE)]
            wide[slot, d] = jnp.transpose(jnp.broadcast_to(line, (TILE, TILE)))

    def fill(tile, slot, diag):
        start = pl.multiple_of(tile * TILE, TILE)
        for part in range(tiles):
            lanes = slice(part * TILE, (part + 1) * TILE)
            h_real, h_imag = coupling(
                [wide[slot, d] for d in range(3)],
                [r[:, lanes] for r in rows],
                None if diag is None else diag[:, lanes],
            )
            for base, h in ((0, h_real), (width, h_imag)):
                hi, lo = split(h)
                at = slice(base + part * TILE, base + (part + 1) * TILE)
                rhs_hi[pl.ds(start, TILE), at] = hi
                rhs_lo[pl.ds(start, TILE), at] = lo

    first = me * tiles
    total = n_row * tiles
    lane_ids = lax.broadcasted_iota(jnp.int32, (TILE, width), 1)
    sub_ids = lax.broadcasted_iota(jnp.int32, (TILE, width), 0)

    def tile_at(j):
        return lax.rem(first + j, total)

    def lower_from_odd():
        @pl.when(jnp.logical_not(even) & (mine == top))
        def _():
            send_grp(0, mine, slab_part)

    def step(j, carry):
        spread(tile_at(j + 1), lax.rem(j + 1, 2))
        fill(tile_at(j), lax.rem(j, 2), None)
        return carry

    flat = total <= 16
    spread(first, 0)
    for j in range(total if flat else tiles):
        if j == tiles + PAUSE:
            lower_from_odd()
        if j + 1 < total:
            spread(tile_at(j + 1), (j + 1) % 2)
        fill(tile_at(j), j % 2, sub_ids + j * TILE == lane_ids if j < tiles else None)
    if not flat:
        lower_from_odd()
        lax.fori_loop(tiles, total, step, 0)

    @pl.when(ahead)
    def _():
        send_grp(1, mine, slab_part)

    @pl.when(in_first & (mine > 0) & (last > 2))
    def _():
        hear_between()
        send_row(2, last)

    @pl.when(between)
    def _():
        pl.semaphore_wait(row_ready.at[GO], 1)
        send_row(2, 2 * pair)
        send_row(2 * pair + 2, last)

    @pl.when(mine < n_grp - 1)
    def _():
        pl.semaphore_wait(grp_ready.at[NEXT], 1)
        send_grp(mine + 1, mine + 2, slab_part)

    @pl.when(jnp.logical_not(in_last))
    def _():
        pl.semaphore_wait(row_ready.at[LATE], 2)
        send_row(last, n_row)

    @pl.when(mine < n_grp - 2)
    def _():
        pl.semaphore_wait(grp_ready.at[REST], n_grp - 2 - mine)
        send_grp(mine + 2, n_grp, slab_part)

    det_load.wait()
    arrived(olds, load_sem.at[3])

    col_start = pl.multiple_of(mine * cols, cols)
    eye = lax.broadcasted_iota(jnp.int32, (cols, TILE), 0) + col_start == lax.broadcasted_iota(
        jnp.int32, (cols, TILE), 1
    )
    slab_rows = [pos_ref[d : d + 1, :TILE] for d in range(3)]
    own_cols = [
        jnp.sum(jnp.where(eye, jnp.broadcast_to(r, (cols, TILE)), 0.0), axis=1, keepdims=True) for r in slab_rows
    ]
    w_real, w_imag = coupling(own_cols, slab_rows, eye)
    w_real = AMPLITUDE * w_real + jnp.where(eye, det_ref[:, :TILE], 0.0)
    w_imag = AMPLITUDE * w_imag + jnp.where(eye, -0.5, 0.0)
    most = slab - cols
    l_hi, l_lo = split(jnp.concatenate([w_real, w_imag], axis=0)[:, :most])
    for j in range(cols):
        for lead, w in ((0, w_real), (cols, w_imag)):
            coef[j, lead : lead + cols] = jnp.broadcast_to(w[:, most + j : most + j + 1], (cols, width))

    y_local = stage[0 : 2 * cols]
    row_buf[me] = stage[...]
    grp_buf[mine] = y_local

    def left(slab_and_pop):
        signed = jnp.broadcast_to(2.0 * slab_and_pop[2 * cols :] - 1.0, (PAD, width))
        return split(jnp.concatenate([slab_and_pop[: 2 * cols], signed], axis=0))

    def lower_planes():
        if n_grp > 2:

            @pl.when(mine < top)
            def _():
                arrived(grp_buf.at[0 : top - 1], grp_recv.at[0])

            @pl.when(mine == top)
            def _():
                arrived(grp_buf.at[0:top], grp_recv.at[0])

        elif n_grp == 2:

            @pl.when(mine == top)
            def _():
                arrived(grp_buf.at[0:top], grp_recv.at[0])

        blocks = [grp_buf[g] for g in range(top)]
        full = jnp.concatenate(
            [jnp.concatenate([block[:cols], block[cols:]], axis=1) for block in blocks], axis=0
        )
        f_hi, f_lo = split(full)
        v = bdot(l_hi, f_hi) + bdot(l_lo, f_hi) + bdot(l_hi, f_lo)
        v_imag = v[:cols, width:] - v[cols:, :width]
        v_real = v[:cols, :width] + v[cols:, width:]
        return v_real, v_imag

    main = jnp.zeros((4 * cols + 2 * PAD, 2 * width), jnp.float32)
    rest = jnp.zeros((2 * cols + PAD, 2 * width), jnp.float32)
    group = 2
    for lead in range(0, n_row, group):
        if lead == last:
            v_real, v_imag = lower_planes()
        his, los = [], []

        @pl.when(pair == lead // group)
        def _():
            arrived(row_buf.at[0], row_recv.at[lead // group])

        @pl.when(pair != lead // group)
        def _():
            arrived(row_buf.at[0:group], row_recv.at[lead // group])

        for p in range(lead, lead + group):
            hi, lo = left(row_buf[p])
            his.append(hi)
            los.append(lo)
        hi = jnp.concatenate(his, axis=1)
        lo = jnp.concatenate(los, axis=1)
        span = slice(lead * width, (lead + group) * width)
        main = main + bdot(jnp.concatenate([hi, lo], axis=0), rhs_hi[span, :])
        rest = rest + bdot(hi, rhs_lo[span, :])
    half = 2 * cols + PAD
    z = AMPLITUDE * (main[:half] + main[half:] + rest)
    z_real = z[:cols, :width] - z[cols : 2 * cols, width:]
    z_imag = z[:cols, width:] + z[cols : 2 * cols, :width]
    shift = z[2 * cols : 2 * cols + 1, :width]

    y_real, y_imag = y_local[:cols], y_local[cols:]
    total_shift = shift + det_ref[:, pl.ds(my_start, width)]
    z_real = z_real + total_shift * y_real + 0.5 * y_imag
    z_imag = z_imag + total_shift * y_imag - 0.5 * y_real

    z_imag = z_imag - v_imag
    z_real = z_real - v_real

    for i, rate in enumerate((z_imag, -z_real)):
        next_ref[i] = olds[0, i] + 0.5 * TIME_STEP * rate
        accum_ref[i] = olds[1, i] + TIME_STEP / 3.0 * rate

    arrived(row_buf.at[0 : n_row - 1], send_sem.at[0])
    arrived(grp_buf.at[0 : n_grp - 1], send_sem.at[1])

    v_real = v_imag = jnp.zeros((cols, width), jnp.float32)
    for q in range(PIECES):

        @pl.when(mine < top)
        def _():
            arrived(grp_buf.at[0, 0:piece], grp_recv.at[1 + q])

        for row in range(q * piece, (q + 1) * piece):
            j = row % cols
            f = grp_buf[top, row : row + 1]
            wr, wi = coef[j, :cols], coef[j, cols:]
            if row < cols:
                v_real = v_real + wr * f
                v_imag = v_imag - wi * f
            else:
                v_real = v_real + wi * f
                v_imag = v_imag + wr * f
    for i, rate in enumerate((-v_imag, v_real)):
        next_ref[i] = next_ref[i] + 0.5 * TIME_STEP * rate
        accum_ref[i] = accum_ref[i] + TIME_STEP / 3.0 * rate


def kernel(n_row, n_grp, *refs):
    pl.run_scoped(
        functools.partial(exchange, n_row, n_grp, *refs),
        send_sem=pltpu.SemaphoreType.DMA((2,)),
        row_recv=pltpu.SemaphoreType.DMA((n_row // 2,)),
        grp_recv=pltpu.SemaphoreType.DMA((1 + PIECES,)),
        row_ready=pltpu.SemaphoreType.REGULAR((3,)),
        grp_ready=pltpu.SemaphoreType.REGULAR((2,)),
        load_sem=pltpu.SemaphoreType.DMA((4,)),
    )


def store(next_ref, accum_ref, next_out, accum_out):
    def scope(sem):
        copies = [
            pltpu.make_async_copy(next_ref, next_out, sem.at[0]),
            pltpu.make_async_copy(accum_ref, accum_out, sem.at[1]),
        ]
        for copy in copies:
            copy.start()
        for copy in copies:
            copy.wait()

    pl.run_scoped(scope, pltpu.SemaphoreType.DMA((2,)))


def local(positions, detuning, populations, base, section, accum):
    n_row, n_grp = lax.axis_size("row"), lax.axis_size("grp")
    cols, width = section.shape[1], section.shape[2]
    total = positions.shape[1]
    block = section.shape
    results = pl.pallas_call(
        functools.partial(kernel, n_row, n_grp),
        out_shape=(pltpu.VMEM(block, jnp.float32), pltpu.VMEM(block, jnp.float32)),
        in_specs=[pl.BlockSpec(memory_space=pl.ANY)] * 6,
        out_specs=(pl.BlockSpec(memory_space=pltpu.VMEM), pl.BlockSpec(memory_space=pltpu.VMEM)),
        scratch_shapes=[
            pltpu.VMEM((2, *block), jnp.float32),
            pltpu.VMEM((3, total), jnp.float32),
            pltpu.VMEM((1, total), jnp.float32),
            pltpu.VMEM((2 * cols + 1, width), jnp.float32),
            pltpu.VMEM((2, 3, TILE, TILE), jnp.float32),
            pltpu.VMEM((total, 2 * width), jnp.bfloat16),
            pltpu.VMEM((total, 2 * width), jnp.bfloat16),
            pltpu.VMEM((n_row, 2 * cols + 1, width), jnp.float32),
            pltpu.VMEM((n_grp, 2 * cols, width), jnp.float32),
            pltpu.VMEM((cols, 2 * cols, width), jnp.float32),
        ],
        compiler_params=pltpu.CompilerParams(collective_id=0, has_side_effects=True),
    )(positions, detuning.reshape(1, total), populations.reshape(1, width), section.reshape(2 * cols, width), base, accum)
    return pl.pallas_call(
        store,
        out_shape=(jax.ShapeDtypeStruct(block, jnp.float32),) * 2,
        in_specs=[pl.BlockSpec(memory_space=pltpu.VMEM)] * 2,
        out_specs=(pl.BlockSpec(memory_space=pltpu.HBM),) * 2,
    )(*[pltpu.with_memory_space_constraint(r, pltpu.VMEM) for r in results])


def solution(mesh):
    return jax.shard_map(
        local,
        mesh=mesh,
        in_specs=(
            P(),
            P(),
            P("row"),
            P(None, "grp", "row"),
            P(None, "grp", "row"),
            P(None, "grp", "row"),
        ),
        out_specs=(P(None, "grp", "row"), P(None, "grp", "row")),
        check_vma=False,
    )
```

```python
import functools
import math

import jax
import jax.numpy as jnp
from jax import lax
from jax.experimental import pallas as pl
from jax.experimental.pallas import tpu as pltpu
from jax.sharding import PartitionSpec as P

TIME_STEP = 0.2
PAD = 16
TILE = 128
AMPLITUDE = -0.75
PAUSE = 3
PIECES = 4

HALF_SIN = (4.442882834149929, -7.308241154546326, 3.606288958225646, -0.8457635961475002, 0.10920575363724722)
HALF_COS = (1.4142134965650124, -6.97885098823893, 5.739461170681154, -1.8835629872981716, 0.31069819180355424)
MESH = pl.DeviceIdType.MESH


def horner(coeffs, t):
    total = coeffs[-1] * t + coeffs[-2]
    for value in coeffs[-3::-1]:
        total = total * t + value
    return total


def coupling(cols, rows, diag):
    dx = cols[0] - rows[0]
    dy = cols[1] - rows[1]
    dz = cols[2] - rows[2]
    dz_sq = dz * dz
    dist_sq = dx * dx + dy * dy + dz_sq
    if diag is not None:
        dist_sq = jnp.where(diag, 1.0, dist_sq)
    inv = lax.rsqrt(dist_sq)
    dist = dist_sq * inv
    frac = dist - jnp.round(dist)
    t = frac * frac
    half_sin = frac * horner(HALF_SIN, t)
    half_cos = horner(HALF_COS, t)
    sine = half_sin * half_cos
    cosine = 1.0 - half_sin * half_sin
    u = inv * (0.5 / math.pi)
    aligned = dz_sq * (inv * inv)
    amp_imag = (u * u) * (1.0 - 3.0 * aligned)
    amp_real = u * ((1.0 - aligned) - amp_imag)
    h_real = amp_real * cosine - amp_imag * sine
    h_imag = amp_real * sine + amp_imag * cosine
    if diag is not None:
        h_real = jnp.where(diag, 0.0, h_real)
        h_imag = jnp.where(diag, 0.0, h_imag)
    return h_real, h_imag


def split(x):
    hi = x.astype(jnp.bfloat16)
    return hi, (x - hi.astype(jnp.float32)).astype(jnp.bfloat16)


def bdot(a, b):
    return jnp.dot(a, b, preferred_element_type=jnp.float32)


def exchange(
    n_row,
    n_grp,
    pos_in,
    det_in,
    pop_in,
    sec_in,
    base_in,
    accum_in,
    next_ref,
    accum_ref,
    olds,
    pos_ref,
    det_ref,
    stage,
    wide,
    rhs_hi,
    rhs_lo,
    row_buf,
    grp_buf,
    coef,
    send_sem,
    row_recv,
    grp_recv,
    row_ready,
    grp_ready,
    load_sem,
):
    cols, width = sec_in.shape[0] // 2, sec_in.shape[1]
    me = lax.axis_index("row")
    mine = lax.axis_index("grp")
    slab = cols * n_grp
    barrier = pltpu.get_barrier_semaphore()

    top = n_grp - 1
    piece = 2 * cols // PIECES

    def send_pieces(p, source):
        for q in range(PIECES):
            part = slice(q * piece, (q + 1) * piece)
            pltpu.make_async_remote_copy(
                source.at[part],
                grp_buf.at[mine, part],
                send_sem.at[1],
                grp_recv.at[jnp.where(mine < top, 0, 1 + q)],
                device_id={"grp": p},
                device_id_type=MESH,
            ).start()

    ahead = (me == 0) & (mine > 0)

    @pl.when(ahead)
    def _():
        pl.semaphore_wait(barrier, 1)
        send_pieces(0, sec_in)

    last = n_row - 2
    pair = me // 2
    odd = lax.rem(me, 2)
    partner = me + 1 - 2 * odd
    in_first = me < 2
    in_last = me >= last
    between = jnp.logical_not(in_first | in_last)
    even = odd == 0
    low = jnp.minimum(mine, 1)
    GO, LATE, WORD = 0, 1, 2
    NEXT, REST = 0, 1

    def to_row(sem, lo, hi):
        def body(p, carry):
            pl.semaphore_signal(sem, inc=1, device_id={"row": p}, device_id_type=MESH)
            return carry

        lax.fori_loop(lo, hi, body, 0)

    def to_grp(sem, lo, hi):
        def body(p, carry):
            pl.semaphore_signal(sem, inc=1, device_id={"grp": p}, device_id_type=MESH)
            return carry

        lax.fori_loop(lo, hi, body, 0)

    slab_part = stage.at[0 : 2 * cols]

    def send_row(lo, hi):
        def body(p, carry):
            pltpu.make_async_remote_copy(
                stage,
                row_buf.at[me],
                send_sem.at[0],
                row_recv.at[pair],
                device_id={"row": p},
                device_id_type=MESH,
            ).start()
            return carry

        lax.fori_loop(lo, hi, body, 0)

    def send_grp(lo, hi, source):
        def body(p, carry):
            send_pieces(p, source)
            return carry

        lax.fori_loop(lo, hi, body, 0)

    def arrived(part, sem):
        pltpu.make_async_copy(part, part, sem).wait()

    section_loads = [
        pltpu.make_async_copy(src, dst, load_sem.at[0])
        for src, dst in (
            (sec_in, stage.at[0 : 2 * cols]),
            (pop_in, stage.at[2 * cols : 2 * cols + 1]),
        )
    ]
    pos_load = pltpu.make_async_copy(pos_in, pos_ref, load_sem.at[1])
    det_load = pltpu.make_async_copy(det_in, det_ref, load_sem.at[2])
    old_loads = [
        pltpu.make_async_copy(src, olds.at[i], load_sem.at[3]) for i, src in enumerate((base_in, accum_in))
    ]

    def start_loads():
        for load in (*section_loads, pos_load, det_load, *old_loads):
            load.start()

    @pl.when(jnp.logical_not(ahead))
    def _():
        start_loads()

    @pl.when(even & (mine > 0))
    def _():
        def body(p, carry):
            pl.semaphore_signal(barrier, inc=1, device_id={"row": partner, "grp": p}, device_id_type=MESH)
            return carry

        lax.fori_loop(mine + 1, n_grp, body, 0)

    @pl.when(jnp.logical_not(even & (mine > 0)))
    def _():
        to_grp(barrier, mine + 1, n_grp)

    @pl.when(even)
    def _():
        pl.semaphore_signal(barrier, inc=1, device_id={"row": partner}, device_id_type=MESH)

    after = jnp.where(in_first, 2, jnp.where(in_last, n_row, last))
    to_row(barrier, after, n_row)

    @pl.when(ahead)
    def _():
        start_loads()

    before = jnp.where(in_first, 0, jnp.where(in_last, last, 2))
    met = before + jnp.where(even, low, 1 + mine + mine - low)

    @pl.when((met > 0) & jnp.logical_not(ahead))
    def _():
        pl.semaphore_wait(barrier, met)

    send_grp(0, jnp.where(even & jnp.logical_not(ahead), low, 0), sec_in)

    def answer_lower(lo, hi):
        to_grp(grp_ready.at[REST], lo, jnp.minimum(hi, mine - 1))
        to_grp(grp_ready.at[NEXT], jnp.maximum(lo, mine - 1), hi)

    answer_lower(0, low)

    @pl.when(between)
    def _():
        to_row(row_ready.at[GO], 0, 2)

    @pl.when(in_last)
    def _():
        to_row(row_ready.at[LATE], 0, last)

    @pl.when(jnp.logical_not(even))
    def _():
        pl.semaphore_signal(row_ready.at[WORD], inc=1, device_id={"row": partner}, device_id_type=MESH)
        answer_lower(low, mine)

    def hear_between():
        pl.semaphore_wait(row_ready.at[GO], last - 2)

        @pl.when(odd == 1)
        def _():
            to_row(row_ready.at[GO], 2, last)

    @pl.when(in_first & (mine == 0) & (last > 2))
    def _():
        hear_between()

    pos_load.wait()
    arrived(stage, load_sem.at[0])
    send_row(jnp.where(in_first, 2, 0), jnp.where(in_first, jnp.where(mine == 0, last, 2), before))

    @pl.when(even)
    def _():
        pl.semaphore_wait(row_ready.at[WORD], 1)
        answer_lower(low, mine)
        send_grp(low, jnp.where(ahead, low, mine), slab_part)

    send_row(partner, partner + 1)

    @pl.when(jnp.logical_not(even) & (mine < top))
    def _():
        send_grp(0, mine, slab_part)

    my_start = pl.multiple_of(me * width, width)
    rows = [pos_ref[d : d + 1, pl.ds(my_start, width)] for d in range(3)]
    tiles = width // TILE

    def spread(tile, slot):
        start = pl.multiple_of(tile * TILE, TILE)
        for d in range(3):
            line = pos_ref[d : d + 1, pl.ds(start, TILE)]
            wide[slot, d] = jnp.transpose(jnp.broadcast_to(line, (TILE, TILE)))

    def fill(tile, slot, diag):
        start = pl.multiple_of(tile * TILE, TILE)
        for part in range(tiles):
            lanes = slice(part * TILE, (part + 1) * TILE)
            h_real, h_imag = coupling(
                [wide[slot, d] for d in range(3)],
                [r[:, lanes] for r in rows],
                None if diag is None else diag[:, lanes],
            )
            for base, h in ((0, h_real), (width, h_imag)):
                hi, lo = split(h)
                at = slice(base + part * TILE, base + (part + 1) * TILE)
                rhs_hi[pl.ds(start, TILE), at] = hi
                rhs_lo[pl.ds(start, TILE), at] = lo

    first = me * tiles
    total = n_row * tiles
    lane_ids = lax.broadcasted_iota(jnp.int32, (TILE, width), 1)
    sub_ids = lax.broadcasted_iota(jnp.int32, (TILE, width), 0)

    def tile_at(j):
        return lax.rem(first + j, total)

    def lower_from_odd():
        @pl.when(jnp.logical_not(even) & (mine == top))
        def _():
            send_grp(0, mine, slab_part)

    def step(j, carry):
        spread(tile_at(j + 1), lax.rem(j + 1, 2))
        fill(tile_at(j), lax.rem(j, 2), None)
        return carry

    flat = total <= 16
    spread(first, 0)
    for j in range(total if flat else tiles):
        if j == tiles + PAUSE:
            lower_from_odd()
        if j + 1 < total:
            spread(tile_at(j + 1), (j + 1) % 2)
        fill(tile_at(j), j % 2, sub_ids + j * TILE == lane_ids if j < tiles else None)
    if not flat:
        lower_from_odd()
        lax.fori_loop(tiles, total, step, 0)

    @pl.when(ahead)
    def _():
        send_grp(1, mine, slab_part)

    @pl.when(in_first & (mine > 0) & (last > 2))
    def _():
        hear_between()
        send_row(2, last)

    @pl.when(between)
    def _():
        pl.semaphore_wait(row_ready.at[GO], 1)
        send_row(2, 2 * pair)
        send_row(2 * pair + 2, last)

    @pl.when(mine < n_grp - 1)
    def _():
        pl.semaphore_wait(grp_ready.at[NEXT], 1)
        send_grp(mine + 1, mine + 2, slab_part)

    @pl.when(jnp.logical_not(in_last))
    def _():
        pl.semaphore_wait(row_ready.at[LATE], 2)
        send_row(last, n_row)

    @pl.when(mine < n_grp - 2)
    def _():
        pl.semaphore_wait(grp_ready.at[REST], n_grp - 2 - mine)
        send_grp(mine + 2, n_grp, slab_part)

    det_load.wait()
    arrived(olds, load_sem.at[3])

    col_start = pl.multiple_of(mine * cols, cols)
    eye = lax.broadcasted_iota(jnp.int32, (cols, TILE), 0) + col_start == lax.broadcasted_iota(
        jnp.int32, (cols, TILE), 1
    )
    slab_rows = [pos_ref[d : d + 1, :TILE] for d in range(3)]
    own_cols = [
        jnp.sum(jnp.where(eye, jnp.broadcast_to(r, (cols, TILE)), 0.0), axis=1, keepdims=True) for r in slab_rows
    ]
    w_real, w_imag = coupling(own_cols, slab_rows, eye)
    w_real = AMPLITUDE * w_real + jnp.where(eye, det_ref[:, :TILE], 0.0)
    w_imag = AMPLITUDE * w_imag + jnp.where(eye, -0.5, 0.0)
    most = slab - cols
    l_hi, l_lo = split(jnp.concatenate([w_real, w_imag], axis=0)[:, :most])
    for j in range(cols):
        for lead, w in ((0, w_real), (cols, w_imag)):
            coef[j, lead : lead + cols] = jnp.broadcast_to(w[:, most + j : most + j + 1], (cols, width))

    y_local = stage[0 : 2 * cols]
    row_buf[me] = stage[...]
    grp_buf[mine] = y_local

    def left(slab_and_pop):
        signed = jnp.broadcast_to(2.0 * slab_and_pop[2 * cols :] - 1.0, (PAD, width))
        return split(jnp.concatenate([slab_and_pop[: 2 * cols], signed], axis=0))

    def lower_planes():
        if n_grp > 2:

            @pl.when(mine < top)
            def _():
                arrived(grp_buf.at[0 : top - 1], grp_recv.at[0])

            @pl.when(mine == top)
            def _():
                arrived(grp_buf.at[0:top], grp_recv.at[0])

        elif n_grp == 2:

            @pl.when(mine == top)
            def _():
                arrived(grp_buf.at[0:top], grp_recv.at[0])

        blocks = [grp_buf[g] for g in range(top)]
        full = jnp.concatenate(
            [jnp.concatenate([block[:cols], block[cols:]], axis=1) for block in blocks], axis=0
        )
        f_hi, f_lo = split(full)
        v = bdot(l_hi, f_hi) + bdot(l_lo, f_hi) + bdot(l_hi, f_lo)
        v_imag = v[:cols, width:] - v[cols:, :width]
        v_real = v[:cols, :width] + v[cols:, width:]
        return v_real, v_imag

    main = jnp.zeros((4 * cols + 2 * PAD, 2 * width), jnp.float32)
    rest = jnp.zeros((2 * cols + PAD, 2 * width), jnp.float32)
    group = 2
    for lead in range(0, n_row, group):
        if lead == last:
            v_real, v_imag = lower_planes()
        his, los = [], []

        @pl.when(pair == lead // group)
        def _():
            arrived(row_buf.at[0], row_recv.at[lead // group])

        @pl.when(pair != lead // group)
        def _():
            arrived(row_buf.at[0:group], row_recv.at[lead // group])

        for p in range(lead, lead + group):
            hi, lo = left(row_buf[p])
            his.append(hi)
            los.append(lo)
        hi = jnp.concatenate(his, axis=1)
        lo = jnp.concatenate(los, axis=1)
        span = slice(lead * width, (lead + group) * width)
        main = main + bdot(jnp.concatenate([hi, lo], axis=0), rhs_hi[span, :])
        rest = rest + bdot(hi, rhs_lo[span, :])
    half = 2 * cols + PAD
    z = AMPLITUDE * (main[:half] + main[half:] + rest)
    z_real = z[:cols, :width] - z[cols : 2 * cols, width:]
    z_imag = z[:cols, width:] + z[cols : 2 * cols, :width]
    shift = z[2 * cols : 2 * cols + 1, :width]

    y_real, y_imag = y_local[:cols], y_local[cols:]
    total_shift = shift + det_ref[:, pl.ds(my_start, width)]
    z_real = z_real + total_shift * y_real + 0.5 * y_imag
    z_imag = z_imag + total_shift * y_imag - 0.5 * y_real

    z_imag = z_imag - v_imag
    z_real = z_real - v_real

    for i, rate in enumerate((z_imag, -z_real)):
        next_ref[i] = olds[0, i] + 0.5 * TIME_STEP * rate
        accum_ref[i] = olds[1, i] + TIME_STEP / 3.0 * rate


    v_real = v_imag = jnp.zeros((cols, width), jnp.float32)
    for q in range(PIECES):
        if q == PIECES - 1:
            arrived(row_buf.at[0 : n_row - 1], send_sem.at[0])
            arrived(grp_buf.at[0 : n_grp - 1], send_sem.at[1])

        @pl.when(mine < top)
        def _():
            arrived(grp_buf.at[0, 0:piece], grp_recv.at[1 + q])

        for row in range(q * piece, (q + 1) * piece):
            j = row % cols
            f = grp_buf[top, row : row + 1]
            wr, wi = coef[j, :cols], coef[j, cols:]
            if row < cols:
                v_real = v_real + wr * f
                v_imag = v_imag - wi * f
            else:
                v_real = v_real + wi * f
                v_imag = v_imag + wr * f
    for i, rate in enumerate((-v_imag, v_real)):
        next_ref[i] = next_ref[i] + 0.5 * TIME_STEP * rate
        accum_ref[i] = accum_ref[i] + TIME_STEP / 3.0 * rate


def kernel(n_row, n_grp, *refs):
    pl.run_scoped(
        functools.partial(exchange, n_row, n_grp, *refs),
        send_sem=pltpu.SemaphoreType.DMA((2,)),
        row_recv=pltpu.SemaphoreType.DMA((n_row // 2,)),
        grp_recv=pltpu.SemaphoreType.DMA((1 + PIECES,)),
        row_ready=pltpu.SemaphoreType.REGULAR((3,)),
        grp_ready=pltpu.SemaphoreType.REGULAR((2,)),
        load_sem=pltpu.SemaphoreType.DMA((4,)),
    )


def store(next_ref, accum_ref, next_out, accum_out):
    def scope(sem):
        copies = [
            pltpu.make_async_copy(next_ref, next_out, sem.at[0]),
            pltpu.make_async_copy(accum_ref, accum_out, sem.at[1]),
        ]
        for copy in copies:
            copy.start()
        for copy in copies:
            copy.wait()

    pl.run_scoped(scope, pltpu.SemaphoreType.DMA((2,)))


def local(positions, detuning, populations, base, section, accum):
    n_row, n_grp = lax.axis_size("row"), lax.axis_size("grp")
    cols, width = section.shape[1], section.shape[2]
    total = positions.shape[1]
    block = section.shape
    results = pl.pallas_call(
        functools.partial(kernel, n_row, n_grp),
        out_shape=(pltpu.VMEM(block, jnp.float32), pltpu.VMEM(block, jnp.float32)),
        in_specs=[pl.BlockSpec(memory_space=pl.ANY)] * 6,
        out_specs=(pl.BlockSpec(memory_space=pltpu.VMEM), pl.BlockSpec(memory_space=pltpu.VMEM)),
        scratch_shapes=[
            pltpu.VMEM((2, *block), jnp.float32),
            pltpu.VMEM((3, total), jnp.float32),
            pltpu.VMEM((1, total), jnp.float32),
            pltpu.VMEM((2 * cols + 1, width), jnp.float32),
            pltpu.VMEM((2, 3, TILE, TILE), jnp.float32),
            pltpu.VMEM((total, 2 * width), jnp.bfloat16),
            pltpu.VMEM((total, 2 * width), jnp.bfloat16),
            pltpu.VMEM((n_row, 2 * cols + 1, width), jnp.float32),
            pltpu.VMEM((n_grp, 2 * cols, width), jnp.float32),
            pltpu.VMEM((cols, 2 * cols, width), jnp.float32),
        ],
        compiler_params=pltpu.CompilerParams(collective_id=0, has_side_effects=True),
    )(positions, detuning.reshape(1, total), populations.reshape(1, width), section.reshape(2 * cols, width), base, accum)
    return pl.pallas_call(
        store,
        out_shape=(jax.ShapeDtypeStruct(block, jnp.float32),) * 2,
        in_specs=[pl.BlockSpec(memory_space=pltpu.VMEM)] * 2,
        out_specs=(pl.BlockSpec(memory_space=pltpu.HBM),) * 2,
    )(*[pltpu.with_memory_space_constraint(r, pltpu.VMEM) for r in results])


def solution(mesh):
    return jax.shard_map(
        local,
        mesh=mesh,
        in_specs=(
            P(),
            P(),
            P("row"),
            P(None, "grp", "row"),
            P(None, "grp", "row"),
            P(None, "grp", "row"),
        ),
        out_specs=(P(None, "grp", "row"), P(None, "grp", "row")),
        check_vma=False,
    )
```
